256 devices in a mesh: item: 16 (over x, y), user: 8 (over z), edge: 2 (over core).
Axes of the slice: x: 4, y: 4, z: 8, core: 2. Of those that a mesh axis runs over, the one named last changes fastest.
Arguments:
- item_emb: bfloat16 [65536, 256], P('item'), may hold values from -6 to 6
- user_emb: bfloat16 [49152, 256], P('user'), may hold values from -6 to 6
- block_item: int32 [16, 8, 2, 96], P('item', 'user', 'edge'), may hold values from 0 to 31
- block_user: int32 [16, 8, 2, 96], P('item', 'user', 'edge'), may hold values from 0 to 47
- block_rows: int32 [16, 8, 2, 96, 128], P('item', 'user', 'edge'), may hold values from 0 to 127
- block_count: int32 [16, 8, 2], P('item', 'user', 'edge'), may hold values from 1 to 96, as said below
- user_weight: bfloat16 [256, 256], replicated, may hold values from -7 to 7
- up_weight: bfloat16 [256, 1024], replicated, may hold values from -0.375 to 0.375
- down_weight: bfloat16 [1024, 256], replicated, may hold values from -0.1875 to 0.1875
Outputs:
- new_items: bfloat16 [65536, 256], P(('item', 'user', 'edge'))
The draws below stay inside these ranges and needn't reach their ends.
Inputs may be any that keep to these rules, and one draw needn't show every extreme that they name: `block_count`: some list has exactly 96 live slots in every draw; entries of slots that are not live are ignored.
All inputs are finite; a program needn't handle non-finite values.
Results may differ from the reference program's by a relative error of at most 0.0045.
Values may be sent and summed in bfloat16 or wider, within the bound.
A program may use at most 64 MiB of HBM per device.

```python
import jax
import jax.numpy as jnp
from jax import lax

E = 256
HID = 1024
TILE = 128
IT_SH = 32
US_SH = 48
MAXB = 96
GI = 16
GU = 8
GE = 2
ITEMS = 65536
USERS = 49152
USER_DEGREE = 40


def draw_block_count(key, part):
    first, second = jax.random.split(jax.random.fold_in(key, 17))
    lowest = max(1, MAXB // 4)
    counts = jax.random.randint(first, (GI * GU * GE,), lowest, MAXB + 1, dtype=jnp.int32)
    chosen = jax.random.randint(second, (), 0, GI * GU * GE, dtype=jnp.int32)
    counts = jnp.where(jnp.arange(GI * GU * GE, dtype=jnp.int32) == chosen, MAXB, counts)
    return counts.reshape(GI, GU, GE)


def plant(values, key, low, high):
    place = [jax.random.randint(jax.random.fold_in(key, axis), (), 0, length) for axis, length in enumerate(values.shape)]
    widest = values.shape.index(max(values.shape))
    neighbour = place[:widest] + [(place[widest] + 1) % values.shape[widest]] + place[widest + 1:]
    return values.at[tuple(place)].set(low).at[tuple(neighbour)].set(high)


def block_levels(key, shape, pieces, low, top_value):
    def one(axis_at, shards_of):
        steps = jax.random.uniform(jax.random.fold_in(jax.random.fold_in(key, 6), axis_at), (shards_of,), jnp.float32, low / len(pieces), top_value / len(pieces))
        return jnp.repeat(jnp.exp(steps), shape[axis_at] // shards_of).reshape((-1,) + (1,) * (len(shape) - axis_at - 1))

    loudness = one(*pieces[0])
    for cut in pieces[1:]:
        loudness = loudness * one(*cut)
    return loudness


def centred(own_key, extent, deviation, most, pieces=(), kind=jnp.bfloat16):
    loudness = block_levels(own_key, extent, pieces, -0.22, 0.18) if pieces else 1.0
    entries = jax.random.normal(own_key, extent, jnp.float32) * deviation * loudness
    return jnp.minimum(jnp.maximum(entries, -most), most).astype(kind)


def setup_inputs(seed: int = 0) -> dict:
    keys = jax.random.split(jax.random.key(seed), 10)
    return {
        "item_emb": centred(keys[0], (ITEMS, E), 1.0, 6.0, ((0, 16),)),
        "user_emb": centred(keys[1], (USERS, E), 1.0, 6.0, ((0, 8),)),
        "block_item": plant(jax.random.randint(keys[2], (GI, GU, GE, MAXB), 0, IT_SH), jax.random.fold_in(keys[2], 1), 0, IT_SH - 1).astype(jnp.int32),
        "block_user": plant(jax.random.randint(keys[3], (GI, GU, GE, MAXB), 0, US_SH), jax.random.fold_in(keys[3], 1), 0, US_SH - 1).astype(jnp.int32),
        "block_rows": plant(jax.random.randint(keys[4], (GI, GU, GE, MAXB, TILE), 0, TILE), jax.random.fold_in(keys[4], 1), 0, TILE - 1).astype(jnp.int32),
        "block_count": draw_block_count(jax.random.fold_in(keys[9], 71), 0),
        "user_weight": centred(keys[6], (E, E), (3.0 * USER_DEGREE ** 0.5 * E ** -0.5), 7.0),
        "up_weight": centred(keys[7], (E, HID), E ** -0.5, 0.375),
        "down_weight": centred(keys[8], (HID, E), HID ** -0.5, 0.1875),
    }


def reference(item_emb, user_emb, block_item, block_user, block_rows, block_count, user_weight, up_weight, down_weight):
    item_span = IT_SH * TILE
    user_span = US_SH * TILE
    lists = GI * GU * GE
    slot_items = block_item.reshape(lists, MAXB)
    slot_users = block_user.reshape(lists, MAXB)
    slot_links = block_rows.reshape(lists, MAXB, TILE)
    counts = block_count.reshape(lists)
    numbers = jnp.arange(lists, dtype=jnp.int32)
    inside = jnp.arange(TILE, dtype=jnp.int32)
    positions = jnp.arange(MAXB, dtype=jnp.int32)

    def edges_of(which, items_at, users_at, links, live_count):
        owner_item = which // (GU * GE)
        owner_user = (which // GE) % GU
        source_rows = owner_item * item_span + items_at[:, None] * TILE + inside[None, :]
        target_rows = owner_user * user_span + users_at[:, None] * TILE + links
        alive = jnp.broadcast_to((positions < live_count)[:, None], (MAXB, TILE)).astype(jnp.float32)
        return source_rows.reshape(-1).astype(jnp.int32), target_rows.reshape(-1).astype(jnp.int32), alive.reshape(-1)

    def first_hop(carry, packed):
        summed, degree = carry
        source_rows, target_rows, alive = edges_of(*packed)
        values = item_emb[source_rows].astype(jnp.float32) * alive[:, None]
        return (summed.at[target_rows].add(values), degree.at[target_rows].add(alive)), None

    start = (jnp.zeros((USERS, E), jnp.float32), jnp.zeros((USERS,), jnp.float32))
    (user_sum, user_degree), _ = lax.scan(first_hop, start, (numbers, slot_items, slot_users, slot_links, counts))
    user_mean = (user_sum / jnp.maximum(user_degree, 1.0)[:, None]).astype(jnp.bfloat16)
    user_new = (user_emb.astype(jnp.float32) + jax.nn.silu(jnp.dot(user_mean, user_weight, preferred_element_type=jnp.float32))).astype(jnp.bfloat16)

    def second_hop(carry, packed):
        summed, degree = carry
        source_rows, target_rows, alive = edges_of(*packed)
        values = user_new[target_rows].astype(jnp.float32) * alive[:, None]
        return (summed.at[source_rows].add(values), degree.at[source_rows].add(alive)), None

    start = (jnp.zeros((ITEMS, E), jnp.float32), jnp.zeros((ITEMS,), jnp.float32))
    (item_sum, item_degree), _ = lax.scan(second_hop, start, (numbers, slot_items, slot_users, slot_links, counts))
    merged = item_emb.astype(jnp.float32) + item_sum / jnp.maximum(item_degree, 1.0)[:, None]
    hidden = jax.nn.silu(jnp.dot(merged.astype(jnp.bfloat16), up_weight, preferred_element_type=jnp.float32)).astype(jnp.bfloat16)
    return (merged + jnp.dot(hidden, down_weight, preferred_element_type=jnp.float32)).astype(jnp.bfloat16)
```

```python
import functools

import jax
import jax.numpy as jnp
from jax import lax
from jax.experimental import pallas as pl
from jax.experimental.pallas import tpu as pltpu
from jax.sharding import PartitionSpec as P

TILE = 128
MESH = pl.DeviceIdType.MESH
F32 = jnp.float32
BF16 = jnp.bfloat16
GROUP = 4
VM = pltpu.VMEM


def rows_at(offset, count, unit):
    return pl.ds(pl.multiple_of(offset, unit), count)


def mask_links(count_ref, links_ref, masked_ref):
    slot = lax.broadcasted_iota(jnp.int32, links_ref.shape, 0)
    masked_ref[...] = jnp.where(slot < count_ref[0], links_ref[...], -1)


def hop1_kernel(bi_ref, bu_ref, count_ref, links_ref, bi_row, bu_row, items_ref, part_ref, cnt_ref, hits_ref, acc, masked):
    slots = links_ref.shape[0]
    user_tiles = acc.shape[0]
    mask_links(count_ref, links_ref, masked)
    acc[...] = jnp.zeros_like(acc)

    inside = lax.broadcasted_iota(jnp.int32, (TILE, TILE), 0)

    def blocks(group, carry):
        made = []
        for k in range(GROUP):
            b = group * GROUP + k
            live = b < count_ref[0]
            it = jnp.where(live, bi_ref[b], 0)
            ut = jnp.where(live, bu_ref[b], 0)
            onehot = (masked[pl.ds(b, 1), :] == inside).astype(F32).astype(BF16)
            rows = items_ref[rows_at(it * TILE, TILE, TILE), :]
            made.append((ut, jnp.dot(onehot, rows, preferred_element_type=F32)))
        for ut, contrib in made:
            acc[ut] += contrib
        return carry

    lax.fori_loop(0, (count_ref[0] + GROUP - 1) // GROUP, blocks, 0)

    lane = lax.broadcasted_iota(jnp.int32, (slots, TILE), 1)
    column_hits = jnp.zeros((slots, TILE), F32)
    links = masked[...]
    for r in range(TILE):
        column_hits += (links[:, r : r + 1] == lane).astype(F32)
    column_hits = column_hits.astype(BF16)
    triples = user_tiles // 3
    which = lax.broadcasted_iota(jnp.int32, (triples, slots), 0) * 3
    at = bu_row[...]
    a, b, c = (
        jnp.dot((which + k == at).astype(F32).astype(BF16), column_hits, preferred_element_type=F32)
        for k in range(3)
    )
    lanes = lax.broadcasted_iota(jnp.int32, (triples, TILE), 1)
    cnt_ref[0] = a
    cnt_ref[1] = jnp.where(lanes < 32, pltpu.roll(a, 32, 1), pltpu.roll(b, 32, 1))
    cnt_ref[2] = jnp.where(lanes < 64, pltpu.roll(b, 64, 1), pltpu.roll(c, 64, 1))
    cnt_ref[3] = pltpu.roll(c, 96, 1)

    slot = lax.broadcasted_iota(jnp.int32, (TILE, slots), 1)
    tile = lax.broadcasted_iota(jnp.int32, (TILE, slots), 0)
    chosen = ((tile == bi_row[...]) & (slot < count_ref[0])).astype(F32).astype(BF16)
    ones = jnp.ones((8, slots), BF16)
    hits_ref[...] = lax.dot_general(ones, chosen, (((1,), (1,)), ((), ())), preferred_element_type=F32)

    def store(t, carry):
        part_ref[rows_at(t * TILE, TILE, TILE), :] = acc[t].astype(BF16)
        return carry

    lax.fori_loop(0, user_tiles, store, 0)


def hop2_kernel(bi_ref, bu_ref, count_ref, links_ref, users_ref, part_ref, acc, masked):
    mask_links(count_ref, links_ref, masked)
    acc[...] = jnp.zeros_like(acc)
    inside = lax.broadcasted_iota(jnp.int32, (TILE, TILE), 0)

    def blocks(group, carry):
        made = []
        for k in range(GROUP):
            b = group * GROUP + k
            live = b < count_ref[0]
            it = jnp.where(live, bi_ref[b], 0)
            ut = jnp.where(live, bu_ref[b], 0)
            onehot = (masked[pl.ds(b, 1), :] == inside).astype(F32).astype(BF16)
            rows = users_ref[rows_at(ut * TILE, TILE, TILE), :]
            contrib = lax.dot_general(onehot, rows, (((0,), (0,)), ((), ())), preferred_element_type=F32)
            made.append((it, contrib))
        for it, contrib in made:
            acc[it] += contrib
        return carry

    lax.fori_loop(0, (count_ref[0] + GROUP - 1) // GROUP, blocks, 0)

    def store(t, carry):
        part_ref[rows_at(t * TILE, TILE, TILE), :] = acc[t].astype(BF16)
        return carry

    lax.fori_loop(0, acc.shape[0], store, 0)


class Wires:
    def __init__(self, send_sem, recv_sem):
        self.send_sem, self.recv_sem, self.made = send_sem, recv_sem, []

    def start(self, src, dst, device):
        at = len(self.made)
        copy = pltpu.make_async_remote_copy(
            src_ref=src,
            dst_ref=dst,
            send_sem=self.send_sem.at[at],
            recv_sem=self.recv_sem.at[at],
            device_id=device,
            device_id_type=MESH,
        )
        copy.start()
        self.made.append(copy)
        return copy

    def finish(self):
        for copy in self.made:
            copy.wait_send()


def enter(peers):
    barrier = pltpu.get_barrier_semaphore()
    for peer in peers:
        pl.semaphore_signal(barrier, inc=1, device_id=peer, device_id_type=MESH)
    pl.semaphore_wait(barrier, len(peers))


def up(x):
    return x.astype(F32)


SIDE = 4
PLANE_COPIES = 111


def plane_kernel(
    part, cnt, emb, weight, users, from_core, sums, opposite, final, total, opposite2, final2, small, total_cnt, got_cnt,
    own_rows, local_sem, send_sem, recv_sem,
):
    item, e = lax.axis_index("item"), lax.axis_index("edge")
    x, y = item // SIDE, item % SIDE
    seg = part.shape[0] // (2 * 2 * SIDE * SIDE)
    block = SIDE * seg
    half, half2 = block // 2, seg // 2

    def step(value, by):
        return lax.rem(value + (by + SIDE), SIDE)

    def along_x(by):
        return {"item": step(x, by) * SIDE + y}

    def along_y(by):
        return {"item": x * SIDE + step(y, by)}

    other = {"edge": 1 - e}
    p1, p2 = (x, y), (y, x)
    ring1, ring2 = (along_x, along_y), (along_y, along_x)

    def block_at(core, h, k1):
        return ((core * 2 + h) * SIDE + step(p1[h], k1)) * block

    def seg_at(core, h, k1, k2):
        return block_at(core, h, k1) + step(p2[h], k2) * seg

    own_copies = []
    for h in range(2):
        copy = pltpu.make_async_copy(
            emb.at[rows_at(seg_at(e, h, 0, 0), seg, seg)], own_rows.at[h], local_sem.at[h]
        )
        copy.start()
        own_copies.append(copy)

    enter([along_x(1), along_x(-1), along_y(1), along_y(-1), other])
    w = Wires(send_sem, recv_sem)

    core_cnt = w.start(cnt, got_cnt.at[0], other)
    core_sums = {}
    for k in (2, 1, 3, 0):
        for h in range(2):
            core_sums[h, k] = w.start(
                part.at[rows_at(block_at(1 - e, h, k), block, seg)], from_core.at[h, k], other
            )

    def mine(h, k, start, size):
        return up(part[rows_at(block_at(e, h, k) + start, size, half2), :]) + up(from_core[h, k, pl.ds(start, size), :])

    to_far = {}
    for h in range(2):
        core_sums[h, 2].wait_recv()
        sums[h, 2] = mine(h, 2, 0, block).astype(BF16)
        to_far[h, 1] = w.start(sums.at[h, 2, pl.ds(0, half)], opposite.at[h, 0], ring1[h](1))
        to_far[h, -1] = w.start(sums.at[h, 2, pl.ds(half, half)], opposite.at[h, 1], ring1[h](-1))
    near = {}
    for h in range(2):
        core_sums[h, 1].wait_recv()
        sums[h, 1, pl.ds(half, half)] = mine(h, 1, half, half).astype(BF16)
        near[h, 1, 0] = w.start(sums.at[h, 1, pl.ds(half, half)], final.at[h, 0, pl.ds(half, half)], ring1[h](1))
        core_sums[h, 3].wait_recv()
        sums[h, 3, pl.ds(0, half)] = mine(h, 3, 0, half).astype(BF16)
        near[h, -1, 0] = w.start(sums.at[h, 3, pl.ds(0, half)], final.at[h, 1, pl.ds(0, half)], ring1[h](-1))
    core_cnt.wait_recv()
    total_cnt[0] = cnt[...] + got_cnt[0]
    cnt_x = [w.start(total_cnt.at[0], got_cnt.at[1], along_x(1)), w.start(total_cnt.at[0], got_cnt.at[2], along_x(-1))]
    for h in range(2):
        to_far[h, 1].wait_recv()
        sums[h, 1, pl.ds(0, half)] = (mine(h, 1, 0, half) + up(opposite[h, 0])).astype(BF16)
        near[h, 1, 1] = w.start(sums.at[h, 1, pl.ds(0, half)], final.at[h, 0, pl.ds(0, half)], ring1[h](1))
        to_far[h, -1].wait_recv()
        sums[h, 3, pl.ds(half, half)] = (mine(h, 3, half, half) + up(opposite[h, 1])).astype(BF16)
        near[h, -1, 1] = w.start(sums.at[h, 3, pl.ds(half, half)], final.at[h, 1, pl.ds(half, half)], ring1[h](-1))
    cnt_x[0].wait_recv()
    cnt_x.append(w.start(got_cnt.at[1], got_cnt.at[3], along_x(1)))
    for h in range(2):
        core_sums[h, 0].wait_recv()
        near[h, 1, 0].wait_recv()
        near[h, -1, 0].wait_recv()
        total[h, pl.ds(0, half)] = mine(h, 0, 0, half) + up(final[h, 1, pl.ds(0, half)])
        total[h, pl.ds(half, half)] = mine(h, 0, half, half) + up(final[h, 0, pl.ds(half, half)])
    cnt_x[1].wait_recv()
    cnt_x[2].wait_recv()
    total_cnt[1] = total_cnt[0] + got_cnt[1] + got_cnt[2] + got_cnt[3]
    cnt_y = [w.start(total_cnt.at[1], got_cnt.at[4], along_y(1)), w.start(total_cnt.at[1], got_cnt.at[5], along_y(-1))]

    def ready(h, k, start, size):
        return total[h, rows_at(step(p2[h], k) * seg + start, size, half2), :]

    to_far2, near2 = {}, {}
    for h in range(2):
        near[h, 1, 1].wait_recv()
        near[h, -1, 1].wait_recv()
        total[h, pl.ds(0, half)] += up(final[h, 0, pl.ds(0, half)])
        total[h, pl.ds(half, half)] += up(final[h, 1, pl.ds(half, half)])
        small[h, 0] = ready(h, 2, 0, seg).astype(BF16)
        to_far2[h, 1] = w.start(small.at[h, 0, pl.ds(0, half2)], opposite2.at[h, 0], ring2[h](1))
        to_far2[h, -1] = w.start(small.at[h, 0, pl.ds(half2, half2)], opposite2.at[h, 1], ring2[h](-1))
        small[h, 1, pl.ds(half2, half2)] = ready(h, 1, half2, half2).astype(BF16)
        near2[h, 1, 0] = w.start(small.at[h, 1, pl.ds(half2, half2)], final2.at[h, 0, pl.ds(half2, half2)], ring2[h](1))
        small[h, 2, pl.ds(0, half2)] = ready(h, -1, 0, half2).astype(BF16)
        near2[h, -1, 0] = w.start(small.at[h, 2, pl.ds(0, half2)], final2.at[h, 1, pl.ds(0, half2)], ring2[h](-1))
    cnt_y[0].wait_recv()
    cnt_y.append(w.start(got_cnt.at[4], got_cnt.at[6], along_y(1)))
    for h in range(2):
        to_far2[h, 1].wait_recv()
        small[h, 1, pl.ds(0, half2)] = (ready(h, 1, 0, half2) + up(opposite2[h, 0])).astype(BF16)
        near2[h, 1, 1] = w.start(small.at[h, 1, pl.ds(0, half2)], final2.at[h, 0, pl.ds(0, half2)], ring2[h](1))
        to_far2[h, -1].wait_recv()
        small[h, 2, pl.ds(half2, half2)] = (ready(h, -1, half2, half2) + up(opposite2[h, 1])).astype(BF16)
        near2[h, -1, 1] = w.start(small.at[h, 2, pl.ds(half2, half2)], final2.at[h, 1, pl.ds(half2, half2)], ring2[h](-1))
    cnt_y[1].wait_recv()
    cnt_y[2].wait_recv()
    total_cnt[2] = total_cnt[1] + got_cnt[4] + got_cnt[5] + got_cnt[6]

    own_diag = lax.broadcasted_iota(jnp.int32, (seg, TILE), 0) == lax.broadcasted_iota(jnp.int32, (seg, TILE), 1)
    for h in range(2):
        degree = total_cnt[2, step(p2[h], 0), pl.ds((e * 2 + h) * SIDE + p1[h], 1), :]
        degree = jnp.sum(jnp.where(own_diag, jnp.broadcast_to(degree, (seg, TILE)), 0.0), axis=1, keepdims=True)
        own_copies[h].wait()
        for s in (1, -1):
            near2[h, s, 0].wait_recv()
            near2[h, s, 1].wait_recv()
        summed = ready(h, 0, 0, seg) + up(final2[h, 0]) + up(final2[h, 1])
        average = (summed / jnp.maximum(degree, 1.0)).astype(BF16)
        v = jnp.dot(average, weight[...], preferred_element_type=F32)
        fresh = up(own_rows[h]) + v / (1.0 + jnp.exp(-v))
        users[rows_at(seg_at(e, h, 0, 0), seg, seg), :] = fresh.astype(BF16)

    def send(h, k1, k2, start, size, device):
        there = users.at[rows_at(seg_at(e, h, k1, k2) + start, size, half2)]
        return w.start(there, there, device)

    c1, c1f, c2, c2f, d = {}, {}, {}, {}, []

    def spread(h, k2):
        for s in (1, -1):
            c2[h, k2, s] = send(h, 0, k2, 0, seg, ring1[h](s))
        d.append(send(h, 0, k2, 0, seg, other))

    def relay(h, k2):
        c2[h, k2, 1].wait_recv()
        c2f[h, k2, 1] = send(h, -1, k2, 0, half2, ring1[h](1))
        d.append(send(h, -1, k2, 0, seg, other))
        c2[h, k2, -1].wait_recv()
        c2f[h, k2, -1] = send(h, 1, k2, half2, half2, ring1[h](-1))
        d.append(send(h, 1, k2, 0, seg, other))

    for h in range(2):
        for s in (1, -1):
            c1[h, s] = send(h, 0, 0, 0, seg, ring2[h](s))
        spread(h, 0)
    for h in range(2):
        c1[h, 1].wait_recv()
        c1f[h, 1] = send(h, 0, -1, 0, half2, ring2[h](1))
        c1[h, -1].wait_recv()
        c1f[h, -1] = send(h, 0, 1, half2, half2, ring2[h](-1))
        spread(h, -1)
        spread(h, 1)
    for h in range(2):
        relay(h, 0)
    for h in range(2):
        c1f[h, 1].wait_recv()
        c1f[h, -1].wait_recv()
        spread(h, 2)
    for k2 in (-1, 1, 2):
        for h in range(2):
            relay(h, k2)
    for k2 in (0, -1, 1, 2):
        for h in range(2):
            c2f[h, k2, 1].wait_recv()
            c2f[h, k2, -1].wait_recv()
            d.append(send(h, 2, k2, 0, seg, other))
    for copy in d:
        copy.wait_recv()
    w.finish()
    assert len(w.made) <= PLANE_COPIES, len(w.made)


DEPTH = 8
COLUMN_COPIES = 8 + 14 + 8


def column_kernel(
    part, hits, items, up_weight, down_weight, out, from_core, sums, got_up, got_down, chip_hits, got_hits, own_rows, up_v,
    down_v, local_sem, send_sem, recv_sem,
):
    u, e = lax.axis_index("user"), lax.axis_index("edge")
    share = out.shape[0]
    half = share // 2

    def step(by):
        return lax.rem(u + (by + DEPTH), DEPTH)

    other = {"edge": 1 - e}
    place = {1: {"user": step(1)}, -1: {"user": step(-1)}}

    def chunk(k, core):
        return (step(k) * 2 + core) * share

    local = [
        pltpu.make_async_copy(items.at[rows_at(chunk(0, e), share, share)], own_rows, local_sem.at[0]),
        pltpu.make_async_copy(up_weight, up_v, local_sem.at[1]),
        pltpu.make_async_copy(down_weight, down_v, local_sem.at[2]),
    ]
    for copy in local:
        copy.start()
    enter([place[1], place[-1], other])
    w = Wires(send_sem, recv_sem)
    core_hits = w.start(hits, got_hits.at[0], other)
    core = {}
    for k in (4, 3, -3, 2, -2, 1, -1, 0):
        core[k] = w.start(part.at[rows_at(chunk(k, 1 - e), share, share)], from_core.at[k % DEPTH], other)

    def mine(k, q):
        return up(part[rows_at(chunk(k, e) + q * half, half, half), :]) + up(from_core[k % DEPTH, pl.ds(q * half, half), :])

    got = {1: got_up, -1: got_down}
    wires = {}
    hit_wires = {}

    landed = set()

    def land(k):
        if k not in landed:
            landed.add(k)
            core[k].wait_recv()

    def pass_on(s, k, q):
        land(4 if k == 4 else s * k)
        value = mine(s * k, q)
        if (s, k + 1, q) in wires:
            wires[s, k + 1, q].wait_recv()
            value += up(got[s][k, q])
        running = (s * k) % DEPTH, pl.ds(q * half, half)
        sums[running] = value.astype(BF16)
        wires[s, k, q] = w.start(sums.at[running], got[s].at[k - 1, q], place[s])

    for k in (4, 3):
        for s in (1, -1):
            pass_on(s, k, int((s == 1) == (k == 3)))
    core_hits.wait_recv()
    chip_hits[...] = hits[...] + got_hits[0]
    for s in (1, -1):
        hit_wires[s, 1] = w.start(chip_hits, got_hits.at[1 if s == 1 else 5], place[s])
    for k in (3, 2, 1):
        for s, q in ((1, 0), (-1, 1)):
            pass_on(s, k, q)
        far = 5 - k
        for s in (1, -1):
            hit_wires[s, far - 1].wait_recv()
            if s == 1 or far < 4:
                base = 1 if s == 1 else 5
                hit_wires[s, far] = w.start(got_hits.at[base + far - 2], got_hits.at[base + far - 1], place[s])
        if k > 1:
            for s, q in ((1, 1), (-1, 0)):
                pass_on(s, k - 1, q)
    hit_wires[1, 4].wait_recv()
    land(0)
    degree = chip_hits[...]
    for k in range(1, DEPTH):
        degree += got_hits[k]
    lane = lax.broadcasted_iota(jnp.int32, degree.shape, 1)
    for copy in local:
        copy.wait()
    for q in range(2):
        wires[1, 1, q].wait_recv()
        wires[-1, 1, q].wait_recv()
    for q in range(2):
        summed = mine(0, q) + up(got_up[0, q]) + up(got_down[0, q])
        mine_only = jnp.where(lane == (u * 2 + e) * 2 + q, degree, 0.0)
        own_degree = jnp.sum(mine_only[0:1, :], axis=1, keepdims=True)
        merged = up(own_rows[pl.ds(q * half, half), :]) + summed / jnp.maximum(own_degree, 1.0)
        v = jnp.dot(merged.astype(BF16), up_v[...], preferred_element_type=F32)
        hidden = (v / (1.0 + jnp.exp(-v))).astype(BF16)
        out[pl.ds(q * half, half), :] = (merged + jnp.dot(hidden, down_v[...], preferred_element_type=F32)).astype(BF16)
    w.finish()
    assert len(w.made) <= COLUMN_COPIES, len(w.made)


def vmem():
    return pl.BlockSpec(memory_space=VM)


def smem():
    return pl.BlockSpec(memory_space=pltpu.SMEM)


def hbm():
    return pl.BlockSpec(memory_space=pl.ANY)


def hop1(bi, bu, count, links, items, user_rows):
    slots, channels = links.shape[0], items.shape[1]
    return pl.pallas_call(
        hop1_kernel,
        out_shape=(
            jax.ShapeDtypeStruct((user_rows, channels), BF16),
            jax.ShapeDtypeStruct((SIDE, user_rows // (3 * TILE), TILE), F32),
            jax.ShapeDtypeStruct((8, TILE), F32),
        ),
        in_specs=[smem(), smem(), smem(), vmem(), vmem(), vmem(), vmem()],
        out_specs=(vmem(), vmem(), vmem()),
        scratch_shapes=[VM((user_rows // TILE, TILE, channels), F32), VM((slots, TILE), jnp.int32)],
        compiler_params=pltpu.CompilerParams(vmem_limit_bytes=32 * 2**20),
        name="hop1",
    )(bi, bu, count, links, bi.reshape(1, slots), bu.reshape(1, slots), items)


def hop2(bi, bu, count, links, users, item_rows):
    slots, channels = links.shape[0], users.shape[1]
    return pl.pallas_call(
        hop2_kernel,
        out_shape=jax.ShapeDtypeStruct((item_rows, channels), BF16),
        in_specs=[smem(), smem(), smem(), vmem(), vmem()],
        out_specs=vmem(),
        scratch_shapes=[VM((item_rows // TILE, TILE, channels), F32), VM((slots, TILE), jnp.int32)],
        compiler_params=pltpu.CompilerParams(vmem_limit_bytes=32 * 2**20),
        name="hop2",
    )(bi, bu, count, links, users)


def plane(part, cnt, emb, weight):
    rows, channels = part.shape
    seg = rows // (4 * SIDE * SIDE)
    block = SIDE * seg
    return pl.pallas_call(
        plane_kernel,
        out_shape=jax.ShapeDtypeStruct((rows, channels), BF16),
        in_specs=[vmem(), vmem(), hbm(), vmem()],
        out_specs=vmem(),
        scratch_shapes=[
            VM((2, SIDE, block, channels), BF16),
            VM((2, SIDE, block, channels), BF16),
            VM((2, 2, block // 2, channels), BF16),
            VM((2, 2, block, channels), BF16),
            VM((2, block, channels), F32),
            VM((2, 2, seg // 2, channels), BF16),
            VM((2, 2, seg, channels), BF16),
            VM((2, 3, seg, channels), BF16),
            VM((3,) + cnt.shape, F32),
            VM((7,) + cnt.shape, F32),
            VM((2, seg, channels), BF16),
            pltpu.SemaphoreType.DMA((2,)),
            pltpu.SemaphoreType.DMA((PLANE_COPIES,)),
            pltpu.SemaphoreType.DMA((PLANE_COPIES,)),
        ],
        compiler_params=pltpu.CompilerParams(collective_id=0, has_side_effects=True, vmem_limit_bytes=32 * 2**20),
        name="plane",
    )(part, cnt, emb, weight)


def column(part, hits, items, up_weight, down_weight):
    rows, channels = part.shape
    share = rows // (2 * DEPTH)
    return pl.pallas_call(
        column_kernel,
        out_shape=jax.ShapeDtypeStruct((share, channels), BF16),
        in_specs=[vmem(), vmem(), hbm(), hbm(), hbm()],
        out_specs=vmem(),
        scratch_shapes=[
            VM((DEPTH, share, channels), BF16),
            VM((DEPTH, share, channels), BF16),
            VM((4, 2, share // 2, channels), BF16),
            VM((4, 2, share // 2, channels), BF16),
            VM(hits.shape, F32),
            VM((DEPTH,) + hits.shape, F32),
            VM((share, channels), BF16),
            VM(up_weight.shape, BF16),
            VM(down_weight.shape, BF16),
            pltpu.SemaphoreType.DMA((3,)),
            pltpu.SemaphoreType.DMA((COLUMN_COPIES,)),
            pltpu.SemaphoreType.DMA((COLUMN_COPIES,)),
        ],
        compiler_params=pltpu.CompilerParams(collective_id=1, has_side_effects=True, vmem_limit_bytes=32 * 2**20),
        name="column",
    )(part, hits, items, up_weight, down_weight)


def body(item_emb, user_emb, block_item, block_user, block_rows, block_count, user_weight, up_weight, down_weight):
    bi, bu, count = block_item.reshape(-1), block_user.reshape(-1), block_count.reshape(-1)
    links = block_rows.reshape(-1, TILE)
    user_part, cnt, hits = hop1(bi, bu, count, links, item_emb, user_emb.shape[0])
    users = plane(user_part, cnt, user_emb, user_weight)
    item_part = hop2(bi, bu, count, links, users, item_emb.shape[0])
    return column(item_part, hits, item_emb, up_weight, down_weight)


def solution(mesh):
    return jax.shard_map(
        body,
        mesh=mesh,
        in_specs=(
            P("item", None),
            P("user", None),
            P("item", "user", "edge", None),
            P("item", "user", "edge", None),
            P("item", "user", "edge", None, None),
            P("item", "user", "edge"),
            P(),
            P(),
            P(),
        ),
        out_specs=P(("item", "user", "edge"), None),
        check_vma=False,
    )
```

```python
import functools

import jax
import jax.numpy as jnp
from jax import lax
from jax.experimental import pallas as pl
from jax.experimental.pallas import tpu as pltpu
from jax.sharding import PartitionSpec as P

TILE = 128
MESH = pl.DeviceIdType.MESH
F32 = jnp.float32
BF16 = jnp.bfloat16
GROUP = 16
VM = pltpu.VMEM


def rows_at(offset, count, unit):
    return pl.ds(pl.multiple_of(offset, unit), count)


def fetch(pairs, sems):
    copies = [pltpu.make_async_copy(src, dst, sems.at[at]) for at, (src, dst) in enumerate(pairs)]
    for copy in copies:
        copy.start()
    return copies


def hop_blocks(from_items, bi, bu, count, links, source, acc):
    inside = lax.broadcasted_iota(jnp.int32, (TILE, TILE), 0)
    live_count = count[0]

    def blocks(group, carry):
        made = []
        for k in range(GROUP):
            b = group * GROUP + k
            live = b < live_count
            it = jnp.where(live, bi[0, b], 0)
            ut = jnp.where(live, bu[0, b], 0)
            row = jnp.where(live, links[pl.ds(b, 1), :], -1)
            onehot = (row == inside).astype(F32).astype(BF16)
            if from_items:
                rows = source[rows_at(it * TILE, TILE, TILE), :]
                made.append((ut, jnp.dot(onehot, rows, preferred_element_type=F32)))
            else:
                rows = source[rows_at(ut * TILE, TILE, TILE), :]
                made.append((it, lax.dot_general(onehot, rows, (((0,), (0,)), ((), ())), preferred_element_type=F32)))
        for tile, contrib in made:
            acc[rows_at(tile * TILE, TILE, TILE), :] += contrib
        return carry

    lax.fori_loop(0, (live_count + GROUP - 1) // GROUP, blocks, 0)


def hop1_kernel(bi_hbm, bu_hbm, count_hbm, links_hbm, items_hbm, acc, bi, bu, count, links, items, sems):
    copies = fetch(
        [(items_hbm, items), (links_hbm, links), (bi_hbm, bi), (bu_hbm, bu), (count_hbm, count)], sems
    )
    acc[...] = jnp.zeros_like(acc)
    for copy in copies:
        copy.wait()
    hop_blocks(True, bi, bu, count, links, items, acc)


def hop2_kernel(bi_hbm, bu_hbm, count_hbm, links_hbm, users, acc, bi, bu, count, links, sems):
    copies = fetch([(links_hbm, links), (bi_hbm, bi), (bu_hbm, bu), (count_hbm, count)], sems)
    acc[...] = jnp.zeros_like(acc)
    for copy in copies:
        copy.wait()
    hop_blocks(False, bi, bu, count, links, users, acc)


def degrees_of(cnt_ref, hits_ref, found, bi, bu, live_count):
    slots = bu.shape[1]
    triples = cnt_ref.shape[1]
    which = lax.broadcasted_iota(jnp.int32, (triples, slots), 0) * 3
    a, b, c = (
        jnp.dot((which + k == bu).astype(F32).astype(BF16), found, preferred_element_type=F32) for k in range(3)
    )
    lanes = lax.broadcasted_iota(jnp.int32, (triples, TILE), 1)
    cnt_ref[0] = a
    cnt_ref[1] = jnp.where(lanes < 32, pltpu.roll(a, 32, 1), pltpu.roll(b, 32, 1))
    cnt_ref[2] = jnp.where(lanes < 64, pltpu.roll(b, 64, 1), pltpu.roll(c, 64, 1))
    cnt_ref[3] = pltpu.roll(c, 96, 1)
    slot = lax.broadcasted_iota(jnp.int32, (TILE, slots), 1)
    tile = lax.broadcasted_iota(jnp.int32, (TILE, slots), 0)
    chosen = ((tile == bi) & (slot < live_count)).astype(F32).astype(BF16)
    ones = jnp.ones((8, slots), BF16)
    hits_ref[...] = lax.dot_general(ones, chosen, (((1,), (1,)), ((), ())), preferred_element_type=F32)


class Wires:
    def __init__(self, send_sem, recv_sem):
        self.send_sem, self.recv_sem, self.made = send_sem, recv_sem, []

    def start(self, src, dst, device):
        at = len(self.made)
        copy = pltpu.make_async_remote_copy(
            src_ref=src,
            dst_ref=dst,
            send_sem=self.send_sem.at[at],
            recv_sem=self.recv_sem.at[at],
            device_id=device,
            device_id_type=MESH,
        )
        copy.start()
        self.made.append(copy)
        return copy

    def finish(self):
        for copy in self.made:
            copy.wait_send()


def enter(peers):
    barrier = pltpu.get_barrier_semaphore()
    for peer in peers:
        pl.semaphore_signal(barrier, inc=1, device_id=peer, device_id_type=MESH)
    pl.semaphore_wait(barrier, len(peers))


def up(x):
    return x.astype(F32)


SIDE = 4
PLANE_COPIES = 111


def plane_kernel(
    part, bi_hbm, bu_hbm, count_hbm, links_hbm, emb, weight_hbm, users, hits, to_core, from_core, sums, opposite, final, total,
    opposite2, final2, small, cnt, total_cnt, got_cnt, own_rows, bi, bu, count, links, weight, local_sem, send_sem, recv_sem,
):
    item, e = lax.axis_index("item"), lax.axis_index("edge")
    x, y = item // SIDE, item % SIDE
    seg = part.shape[0] // (2 * 2 * SIDE * SIDE)
    block = SIDE * seg
    half, half2 = block // 2, seg // 2

    def step(value, by):
        return lax.rem(value + (by + SIDE), SIDE)

    def along_x(by):
        return {"item": step(x, by) * SIDE + y}

    def along_y(by):
        return {"item": x * SIDE + step(y, by)}

    other = {"edge": 1 - e}
    p1, p2 = (x, y), (y, x)
    ring1, ring2 = (along_x, along_y), (along_y, along_x)

    def block_at(core, h, k1):
        return ((core * 2 + h) * SIDE + step(p1[h], k1)) * block

    def seg_at(core, h, k1, k2):
        return block_at(core, h, k1) + step(p2[h], k2) * seg

    own_copies = fetch(
        [(emb.at[rows_at(seg_at(e, h, 0, 0), seg, seg)], own_rows.at[h]) for h in range(2)]
        + [(links_hbm, links), (bi_hbm, bi), (bu_hbm, bu), (count_hbm, count), (weight_hbm, weight)],
        local_sem,
    )
    enter([along_x(1), along_x(-1), along_y(1), along_y(-1), other])
    w = Wires(send_sem, recv_sem)

    core_sums = {}
    for k in (2, 1, 3, 0):
        for h in range(2):
            to_core[h, k] = part[rows_at(block_at(1 - e, h, k), block, seg), :].astype(BF16)
            core_sums[h, k] = w.start(to_core.at[h, k], from_core.at[h, k], other)

    for copy in own_copies[2:6]:
        copy.wait()
    slots = links.shape[0]
    live = lax.broadcasted_iota(jnp.int32, (slots, TILE), 0) < count[0]
    lane = lax.broadcasted_iota(jnp.int32, (slots, TILE), 1)
    masked = jnp.where(live, links[...], -1)

    def column_hits(first, last):
        found = jnp.zeros((slots, TILE), F32)
        for r in range(first, last):
            found += (masked[:, r : r + 1] == lane).astype(F32)
        return found

    found = column_hits(0, TILE // 2)

    def mine(h, k, start, size):
        return part[rows_at(block_at(e, h, k) + start, size, half2), :] + up(from_core[h, k, pl.ds(start, size), :])

    to_far = {}
    for h in range(2):
        core_sums[h, 2].wait_recv()
        sums[h, 2] = mine(h, 2, 0, block).astype(BF16)
        to_far[h, 1] = w.start(sums.at[h, 2, pl.ds(0, half)], opposite.at[h, 0], ring1[h](1))
        to_far[h, -1] = w.start(sums.at[h, 2, pl.ds(half, half)], opposite.at[h, 1], ring1[h](-1))
    near = {}
    for h in range(2):
        core_sums[h, 1].wait_recv()
        sums[h, 1, pl.ds(half, half)] = mine(h, 1, half, half).astype(BF16)
        near[h, 1, 0] = w.start(sums.at[h, 1, pl.ds(half, half)], final.at[h, 0, pl.ds(half, half)], ring1[h](1))
        core_sums[h, 3].wait_recv()
        sums[h, 3, pl.ds(0, half)] = mine(h, 3, 0, half).astype(BF16)
        near[h, -1, 0] = w.start(sums.at[h, 3, pl.ds(0, half)], final.at[h, 1, pl.ds(0, half)], ring1[h](-1))
    degrees_of(cnt, hits, (found + column_hits(TILE // 2, TILE)).astype(BF16), bi[...], bu[...], count[0])
    core_cnt = w.start(cnt, got_cnt.at[0], other)
    for h in range(2):
        to_far[h, 1].wait_recv()
        sums[h, 1, pl.ds(0, half)] = (mine(h, 1, 0, half) + up(opposite[h, 0])).astype(BF16)
        near[h, 1, 1] = w.start(sums.at[h, 1, pl.ds(0, half)], final.at[h, 0, pl.ds(0, half)], ring1[h](1))
        to_far[h, -1].wait_recv()
        sums[h, 3, pl.ds(half, half)] = (mine(h, 3, half, half) + up(opposite[h, 1])).astype(BF16)
        near[h, -1, 1] = w.start(sums.at[h, 3, pl.ds(half, half)], final.at[h, 1, pl.ds(half, half)], ring1[h](-1))
    core_cnt.wait_recv()
    total_cnt[0] = cnt[...] + got_cnt[0]
    cnt_x = [w.start(total_cnt.at[0], got_cnt.at[1], along_x(1)), w.start(total_cnt.at[0], got_cnt.at[2], along_x(-1))]
    for h in range(2):
        core_sums[h, 0].wait_recv()
        near[h, 1, 0].wait_recv()
        near[h, -1, 0].wait_recv()
        total[h, pl.ds(0, half)] = mine(h, 0, 0, half) + up(final[h, 1, pl.ds(0, half)])
        total[h, pl.ds(half, half)] = mine(h, 0, half, half) + up(final[h, 0, pl.ds(half, half)])
    cnt_x[0].wait_recv()
    cnt_x.append(w.start(got_cnt.at[1], got_cnt.at[3], along_x(1)))
    cnt_x[1].wait_recv()
    cnt_x[2].wait_recv()
    total_cnt[1] = total_cnt[0] + got_cnt[1] + got_cnt[2] + got_cnt[3]
    cnt_y = [w.start(total_cnt.at[1], got_cnt.at[4], along_y(1)), w.start(total_cnt.at[1], got_cnt.at[5], along_y(-1))]

    def ready(h, k, start, size):
        return total[h, rows_at(step(p2[h], k) * seg + start, size, half2), :]

    to_far2, near2 = {}, {}
    for h in range(2):
        near[h, 1, 1].wait_recv()
        near[h, -1, 1].wait_recv()
        total[h, pl.ds(0, half)] += up(final[h, 0, pl.ds(0, half)])
        total[h, pl.ds(half, half)] += up(final[h, 1, pl.ds(half, half)])
        small[h, 0] = ready(h, 2, 0, seg).astype(BF16)
        to_far2[h, 1] = w.start(small.at[h, 0, pl.ds(0, half2)], opposite2.at[h, 0], ring2[h](1))
        to_far2[h, -1] = w.start(small.at[h, 0, pl.ds(half2, half2)], opposite2.at[h, 1], ring2[h](-1))
        small[h, 1, pl.ds(half2, half2)] = ready(h, 1, half2, half2).astype(BF16)
        near2[h, 1, 0] = w.start(small.at[h, 1, pl.ds(half2, half2)], final2.at[h, 0, pl.ds(half2, half2)], ring2[h](1))
        small[h, 2, pl.ds(0, half2)] = ready(h, -1, 0, half2).astype(BF16)
        near2[h, -1, 0] = w.start(small.at[h, 2, pl.ds(0, half2)], final2.at[h, 1, pl.ds(0, half2)], ring2[h](-1))
    cnt_y[0].wait_recv()
    cnt_y.append(w.start(got_cnt.at[4], got_cnt.at[6], along_y(1)))
    for h in range(2):
        to_far2[h, 1].wait_recv()
        small[h, 1, pl.ds(0, half2)] = (ready(h, 1, 0, half2) + up(opposite2[h, 0])).astype(BF16)
        near2[h, 1, 1] = w.start(small.at[h, 1, pl.ds(0, half2)], final2.at[h, 0, pl.ds(0, half2)], ring2[h](1))
        to_far2[h, -1].wait_recv()
        small[h, 2, pl.ds(half2, half2)] = (ready(h, -1, half2, half2) + up(opposite2[h, 1])).astype(BF16)
        near2[h, -1, 1] = w.start(small.at[h, 2, pl.ds(half2, half2)], final2.at[h, 1, pl.ds(half2, half2)], ring2[h](-1))
    cnt_y[1].wait_recv()
    cnt_y[2].wait_recv()
    total_cnt[2] = total_cnt[1] + got_cnt[4] + got_cnt[5] + got_cnt[6]

    for h in (0, 1, 6):
        own_copies[h].wait()
    own_diag = lax.broadcasted_iota(jnp.int32, (seg, TILE), 0) == lax.broadcasted_iota(jnp.int32, (seg, TILE), 1)
    for h in range(2):
        degree = total_cnt[2, step(p2[h], 0), pl.ds((e * 2 + h) * SIDE + p1[h], 1), :]
        degree = jnp.sum(jnp.where(own_diag, jnp.broadcast_to(degree, (seg, TILE)), 0.0), axis=1, keepdims=True)
        for s in (1, -1):
            near2[h, s, 0].wait_recv()
            near2[h, s, 1].wait_recv()
        summed = ready(h, 0, 0, seg) + up(final2[h, 0]) + up(final2[h, 1])
        average = (summed / jnp.maximum(degree, 1.0)).astype(BF16)
        v = jnp.dot(average, weight[...], preferred_element_type=F32)
        fresh = up(own_rows[h]) + v / (1.0 + jnp.exp(-v))
        users[rows_at(seg_at(e, h, 0, 0), seg, seg), :] = fresh.astype(BF16)

    def send(h, k1, k2, start, size, device):
        there = users.at[rows_at(seg_at(e, h, k1, k2) + start, size, half2)]
        return w.start(there, there, device)

    c1, c1f, c2, c2f, d = {}, {}, {}, {}, []

    def spread(h, k2):
        for s in (1, -1):
            c2[h, k2, s] = send(h, 0, k2, 0, seg, ring1[h](s))
        d.append(send(h, 0, k2, 0, seg, other))

    def relay(h, k2):
        c2[h, k2, 1].wait_recv()
        c2f[h, k2, 1] = send(h, -1, k2, 0, half2, ring1[h](1))
        d.append(send(h, -1, k2, 0, seg, other))
        c2[h, k2, -1].wait_recv()
        c2f[h, k2, -1] = send(h, 1, k2, half2, half2, ring1[h](-1))
        d.append(send(h, 1, k2, 0, seg, other))

    for h in range(2):
        for s in (1, -1):
            c1[h, s] = send(h, 0, 0, 0, seg, ring2[h](s))
        spread(h, 0)
    for h in range(2):
        c1[h, 1].wait_recv()
        c1f[h, 1] = send(h, 0, -1, 0, half2, ring2[h](1))
        c1[h, -1].wait_recv()
        c1f[h, -1] = send(h, 0, 1, half2, half2, ring2[h](-1))
        spread(h, -1)
        spread(h, 1)
    for h in range(2):
        relay(h, 0)
    for h in range(2):
        c1f[h, 1].wait_recv()
        c1f[h, -1].wait_recv()
        spread(h, 2)
    for k2 in (-1, 1, 2):
        for h in range(2):
            relay(h, k2)
    for k2 in (0, -1, 1, 2):
        for h in range(2):
            c2f[h, k2, 1].wait_recv()
            c2f[h, k2, -1].wait_recv()
            d.append(send(h, 2, k2, 0, seg, other))
    for copy in d:
        copy.wait_recv()
    w.finish()
    assert len(w.made) <= PLANE_COPIES, len(w.made)


DEPTH = 8
COLUMN_COPIES = 8 + 14 + 8


def column_kernel(
    part, hits, items, up_weight, down_weight, out, to_core, from_core, sums, got_up, got_down, chip_hits, got_hits, own_rows, up_v,
    down_v, local_sem, send_sem, recv_sem,
):
    u, e = lax.axis_index("user"), lax.axis_index("edge")
    share = out.shape[0]
    half = share // 2

    def step(by):
        return lax.rem(u + (by + DEPTH), DEPTH)

    other = {"edge": 1 - e}
    place = {1: {"user": step(1)}, -1: {"user": step(-1)}}

    def chunk(k, core):
        return (step(k) * 2 + core) * share

    local = [
        pltpu.make_async_copy(items.at[rows_at(chunk(0, e), share, share)], own_rows, local_sem.at[0]),
        pltpu.make_async_copy(up_weight, up_v, local_sem.at[1]),
        pltpu.make_async_copy(down_weight, down_v, local_sem.at[2]),
    ]
    for copy in local:
        copy.start()
    enter([place[1], place[-1], other])
    w = Wires(send_sem, recv_sem)
    core_hits = w.start(hits, got_hits.at[0], other)
    core = {}
    for k in (4, 3, -3, 2, -2, 1, -1, 0):
        to_core[k % DEPTH] = part[rows_at(chunk(k, 1 - e), share, share), :].astype(BF16)
        core[k] = w.start(to_core.at[k % DEPTH], from_core.at[k % DEPTH], other)

    def mine(k, q):
        return part[rows_at(chunk(k, e) + q * half, half, half), :] + up(from_core[k % DEPTH, pl.ds(q * half, half), :])

    got = {1: got_up, -1: got_down}
    wires = {}
    hit_wires = {}

    landed = set()

    def land(k):
        if k not in landed:
            landed.add(k)
            core[k].wait_recv()

    def pass_on(s, k, q):
        land(4 if k == 4 else s * k)
        value = mine(s * k, q)
        if (s, k + 1, q) in wires:
            wires[s, k + 1, q].wait_recv()
            value += up(got[s][k, q])
        running = (s * k) % DEPTH, pl.ds(q * half, half)
        sums[running] = value.astype(BF16)
        wires[s, k, q] = w.start(sums.at[running], got[s].at[k - 1, q], place[s])

    for k in (4, 3):
        for s in (1, -1):
            pass_on(s, k, int((s == 1) == (k == 3)))
    core_hits.wait_recv()
    chip_hits[...] = hits[...] + got_hits[0]
    for s in (1, -1):
        hit_wires[s, 1] = w.start(chip_hits, got_hits.at[1 if s == 1 else 5], place[s])
    for k in (3, 2, 1):
        for s, q in ((1, 0), (-1, 1)):
            pass_on(s, k, q)
        far = 5 - k
        for s in (1, -1):
            hit_wires[s, far - 1].wait_recv()
            if s == 1 or far < 4:
                base = 1 if s == 1 else 5
                hit_wires[s, far] = w.start(got_hits.at[base + far - 2], got_hits.at[base + far - 1], place[s])
        if k > 1:
            for s, q in ((1, 1), (-1, 0)):
                pass_on(s, k - 1, q)
    hit_wires[1, 4].wait_recv()
    land(0)
    degree = chip_hits[...]
    for k in range(1, DEPTH):
        degree += got_hits[k]
    lane = lax.broadcasted_iota(jnp.int32, degree.shape, 1)
    for copy in local:
        copy.wait()
    for q in range(2):
        wires[1, 1, q].wait_recv()
        wires[-1, 1, q].wait_recv()
    for q in range(2):
        summed = mine(0, q) + up(got_up[0, q]) + up(got_down[0, q])
        mine_only = jnp.where(lane == (u * 2 + e) * 2 + q, degree, 0.0)
        own_degree = jnp.sum(mine_only[0:1, :], axis=1, keepdims=True)
        merged = up(own_rows[pl.ds(q * half, half), :]) + summed / jnp.maximum(own_degree, 1.0)
        v = jnp.dot(merged.astype(BF16), up_v[...], preferred_element_type=F32)
        hidden = (v / (1.0 + jnp.exp(-v))).astype(BF16)
        out[pl.ds(q * half, half), :] = (merged + jnp.dot(hidden, down_v[...], preferred_element_type=F32)).astype(BF16)
    w.finish()
    assert len(w.made) <= COLUMN_COPIES, len(w.made)


def vmem():
    return pl.BlockSpec(memory_space=VM)


def smem():
    return pl.BlockSpec(memory_space=pltpu.SMEM)


def hbm():
    return pl.BlockSpec(memory_space=pltpu.HBM)


MIB = 2**20


def lists(slots):
    return [pltpu.SMEM((1, slots), jnp.int32), pltpu.SMEM((1, slots), jnp.int32), pltpu.SMEM((1,), jnp.int32)]


def hop1(bi, bu, count, links, items, user_rows):
    return pl.pallas_call(
        hop1_kernel,
        out_shape=jax.ShapeDtypeStruct((user_rows, items.shape[1]), F32),
        in_specs=[hbm()] * 5,
        out_specs=vmem(),
        scratch_shapes=lists(bi.shape[1])
        + [VM(links.shape, jnp.int32), VM(items.shape, BF16), pltpu.SemaphoreType.DMA((5,))],
        compiler_params=pltpu.CompilerParams(vmem_limit_bytes=40 * MIB),
        name="hop1",
    )(bi, bu, count, links, items)


def hop2(bi, bu, count, links, users, item_rows):
    return pl.pallas_call(
        hop2_kernel,
        out_shape=jax.ShapeDtypeStruct((item_rows, users.shape[1]), F32),
        in_specs=[hbm()] * 4 + [vmem()],
        out_specs=vmem(),
        scratch_shapes=lists(bi.shape[1]) + [VM(links.shape, jnp.int32), pltpu.SemaphoreType.DMA((4,))],
        compiler_params=pltpu.CompilerParams(vmem_limit_bytes=40 * MIB),
        name="hop2",
    )(bi, bu, count, links, users)


def plane(part, bi, bu, count, links, emb, weight):
    rows, channels = part.shape
    slots = links.shape[0]
    seg = rows // (4 * SIDE * SIDE)
    block = SIDE * seg
    cnt = (SIDE, rows // (3 * TILE), TILE)
    return pl.pallas_call(
        plane_kernel,
        out_shape=(jax.ShapeDtypeStruct((rows, channels), BF16), jax.ShapeDtypeStruct((8, TILE), F32)),
        in_specs=[vmem()] + [hbm()] * 6,
        out_specs=(vmem(), vmem()),
        scratch_shapes=[
            VM((2, SIDE, block, channels), BF16),
            VM((2, SIDE, block, channels), BF16),
            VM((2, SIDE, block, channels), BF16),
            VM((2, 2, block // 2, channels), BF16),
            VM((2, 2, block, channels), BF16),
            VM((2, block, channels), F32),
            VM((2, 2, seg // 2, channels), BF16),
            VM((2, 2, seg, channels), BF16),
            VM((2, 3, seg, channels), BF16),
            VM(cnt, F32),
            VM((3,) + cnt, F32),
            VM((7,) + cnt, F32),
            VM((2, seg, channels), BF16),
            VM((1, slots), jnp.int32),
            VM((1, slots), jnp.int32),
            pltpu.SMEM((1,), jnp.int32),
            VM(links.shape, jnp.int32),
            VM(weight.shape, BF16),
            pltpu.SemaphoreType.DMA((7,)),
            pltpu.SemaphoreType.DMA((PLANE_COPIES,)),
            pltpu.SemaphoreType.DMA((PLANE_COPIES,)),
        ],
        compiler_params=pltpu.CompilerParams(collective_id=0, has_side_effects=True, vmem_limit_bytes=40 * MIB),
        name="plane",
    )(part, bi, bu, count, links, emb, weight)


def column(part, hits, items, up_weight, down_weight):
    rows, channels = part.shape
    share = rows // (2 * DEPTH)
    return pl.pallas_call(
        column_kernel,
        out_shape=jax.ShapeDtypeStruct((share, channels), BF16),
        in_specs=[vmem(), vmem(), hbm(), hbm(), hbm()],
        out_specs=vmem(),
        scratch_shapes=[
            VM((DEPTH, share, channels), BF16),
            VM((DEPTH, share, channels), BF16),
            VM((DEPTH, share, channels), BF16),
            VM((4, 2, share // 2, channels), BF16),
            VM((4, 2, share // 2, channels), BF16),
            VM(hits.shape, F32),
            VM((DEPTH,) + hits.shape, F32),
            VM((share, channels), BF16),
            VM(up_weight.shape, BF16),
            VM(down_weight.shape, BF16),
            pltpu.SemaphoreType.DMA((3,)),
            pltpu.SemaphoreType.DMA((COLUMN_COPIES,)),
            pltpu.SemaphoreType.DMA((COLUMN_COPIES,)),
        ],
        compiler_params=pltpu.CompilerParams(collective_id=1, has_side_effects=True, vmem_limit_bytes=40 * MIB),
        name="column",
    )(part, hits, items, up_weight, down_weight)


def pin(*xs):
    return [pltpu.with_memory_space_constraint(x, pltpu.HBM) for x in xs]


def body(item_emb, user_emb, block_item, block_user, block_rows, block_count, user_weight, up_weight, down_weight):
    bi, bu, count = block_item.reshape(1, -1), block_user.reshape(1, -1), block_count.reshape(-1)
    links = block_rows.reshape(-1, TILE)
    bi, bu, links, item_emb, user_emb, user_weight, up_weight, down_weight = pin(
        bi, bu, links, item_emb, user_emb, user_weight, up_weight, down_weight
    )
    user_part = hop1(bi, bu, count, links, item_emb, user_emb.shape[0])
    users, hits = plane(user_part, bi, bu, count, links, user_emb, user_weight)
    item_part = hop2(bi, bu, count, links, users, item_emb.shape[0])
    return column(item_part, hits, item_emb, up_weight, down_weight)


def solution(mesh):
    return jax.shard_map(
        body,
        mesh=mesh,
        in_specs=(
            P("item", None),
            P("user", None),
            P("item", "user", "edge", None),
            P("item", "user", "edge", None),
            P("item", "user", "edge", None, None),
            P("item", "user", "edge"),
            P(),
            P(),
            P(),
        ),
        out_specs=P(("item", "user", "edge"), None),
        check_vma=False,
    )
```

```python
import functools

import jax
import jax.numpy as jnp
from jax import lax
from jax.experimental import pallas as pl
from jax.experimental.pallas import tpu as pltpu
from jax.sharding import PartitionSpec as P

TILE = 128
MESH = pl.DeviceIdType.MESH
F32 = jnp.float32
BF16 = jnp.bfloat16
GROUP = 16
NOWHERE = 2**10
VM = pltpu.VMEM


def rows_at(offset, count, unit):
    return pl.ds(pl.multiple_of(offset, unit), count)


def fetch(pairs, sems):
    copies = [pltpu.make_async_copy(src, dst, sems.at[at]) for at, (src, dst) in enumerate(pairs)]
    for copy in copies:
        copy.start()
    return copies


def swap_kernel(
    bi_hbm, bu_hbm, count_hbm, links_hbm, items_hbm, meta, links, found, hits, items, bi, bu, count, local_sem, send_sem, recv_sem
):
    slots = links_hbm.shape[0]
    other = {"edge": 1 - lax.axis_index("edge")}
    own = links.at[pl.ds(0, slots)]
    copies = fetch(
        [(bi_hbm, bi), (bu_hbm, bu), (count_hbm, count), (links_hbm, own), (items_hbm, items)], local_sem
    )
    enter([other])
    w = Wires(send_sem, recv_sem)
    for copy in copies[:3]:
        copy.wait()
    slot = lax.broadcasted_iota(jnp.int32, (1, slots), 1)
    live = slot < count[0]
    meta[0:1, 0:slots] = bi[...]
    meta[1:2, 0:slots] = jnp.where(live, bu[...], NOWHERE)
    copies[3].wait()
    w.start(own, links.at[pl.ds(slots, slots)], other)
    lane = lax.broadcasted_iota(jnp.int32, (slots, TILE), 1)
    found[...] = row_hits(links[pl.ds(0, slots), :], lane, 0, TILE // 4)
    w.start(meta.at[pl.ds(0, 8)], meta.at[pl.ds(8, 8)], other)
    found[...] += row_hits(links[pl.ds(0, slots), :], lane, TILE // 4, TILE // 2)
    slot = lax.broadcasted_iota(jnp.int32, (TILE, slots), 1)
    tile = lax.broadcasted_iota(jnp.int32, (TILE, slots), 0)
    chosen = ((tile == bi[...]) & (slot < count[0])).astype(F32).astype(BF16)
    ones = jnp.ones((8, slots), BF16)
    hits[...] = lax.dot_general(ones, chosen, (((1,), (1,)), ((), ())), preferred_element_type=F32)
    copies[4].wait()
    for copy in w.made:
        copy.wait_recv()
    w.finish()


def row_hits(links, lane, first, last):
    found = jnp.zeros(lane.shape, F32)
    for r in range(first, last):
        found += (links[:, r : r + 1] == lane).astype(F32)
    return found


def hop_kernel(from_items, half_tiles, meta_ref, links, source, acc, meta, src, dst, slot, sem):
    e = lax.axis_index("edge")
    slots = links.shape[0] // 2
    copy = fetch([(meta_ref, meta)], sem)[0]
    groups = 16
    each = 2 * slots // groups
    rows = acc.shape[0] // groups
    copy.wait()

    def choose(g, n):
        acc[rows_at(g * rows, rows, rows), :] = jnp.zeros((rows, acc.shape[1]), F32)
        which = g // (groups // 2)
        base = (g - which * (groups // 2)) * each
        for j in range(each):
            ut = meta[which * 8 + 1, base + j] - e * half_tiles
            ends = meta[which * 8, base + j] * TILE, ut * TILE
            src[n], dst[n] = ends if from_items else ends[::-1]
            slot[n] = g * each + j
            n = n + jnp.where((ut >= 0) & (ut < half_tiles), 1, 0)
        return n

    count = lax.fori_loop(0, groups, choose, 0)
    inside = lax.broadcasted_iota(jnp.int32, (TILE, TILE), 0)

    def blocks(group, carry):
        made = []
        for k in range(GROUP):
            b = group * GROUP + k
            live = b < count
            row = jnp.where(live, links[pl.ds(jnp.where(live, slot[b], 0), 1), :], -1)
            onehot = (row == inside).astype(F32).astype(BF16)
            rows = source[rows_at(jnp.where(live, src[b], 0), TILE, TILE), :]
            dims = (((1,), (0,)), ((), ())) if from_items else (((0,), (0,)), ((), ()))
            contrib = lax.dot_general(onehot, rows, dims, preferred_element_type=F32)
            made.append((jnp.where(live, dst[b], 0), contrib))
        for at, contrib in made:
            acc[rows_at(at, TILE, TILE), :] += contrib
        return carry

    lax.fori_loop(0, (count + GROUP - 1) // GROUP, blocks, 0)


def degrees_of(cnt_ref, found, bu):
    slots = bu.shape[1]
    triples = cnt_ref.shape[1]
    which = lax.broadcasted_iota(jnp.int32, (triples, slots), 0) * 3
    a, b, c = (
        jnp.dot((which + k == bu).astype(F32).astype(BF16), found, preferred_element_type=F32) for k in range(3)
    )
    lanes = lax.broadcasted_iota(jnp.int32, (triples, TILE), 1)
    cnt_ref[0] = a
    cnt_ref[1] = jnp.where(lanes < 32, pltpu.roll(a, 32, 1), pltpu.roll(b, 32, 1))
    cnt_ref[2] = jnp.where(lanes < 64, pltpu.roll(b, 64, 1), pltpu.roll(c, 64, 1))
    cnt_ref[3] = pltpu.roll(c, 96, 1)


class Wires:
    def __init__(self, send_sem, recv_sem):
        self.send_sem, self.recv_sem, self.made = send_sem, recv_sem, []

    def start(self, src, dst, device):
        at = len(self.made)
        copy = pltpu.make_async_remote_copy(
            src_ref=src,
            dst_ref=dst,
            send_sem=self.send_sem.at[at],
            recv_sem=self.recv_sem.at[at],
            device_id=device,
            device_id_type=MESH,
        )
        copy.start()
        self.made.append(copy)
        return copy

    def finish(self):
        for copy in self.made:
            copy.wait_send()


def enter(peers):
    barrier = pltpu.get_barrier_semaphore()
    for peer in peers:
        pl.semaphore_signal(barrier, inc=1, device_id=peer, device_id_type=MESH)
    pl.semaphore_wait(barrier, len(peers))


def up(x):
    return x.astype(F32)


SIDE = 4
PLANE_COPIES = 69


def plane_kernel(
    part, meta, links, found, emb, weight_hbm, users, sums, opposite, final, total, opposite2, final2, small, cnt, total_cnt,
    got_cnt, own_rows, weight, local_sem, send_sem, recv_sem,
):
    item, e = lax.axis_index("item"), lax.axis_index("edge")
    x, y = item // SIDE, item % SIDE
    seg = part.shape[0] // (2 * SIDE * SIDE)
    block = SIDE * seg
    half, half2 = block // 2, seg // 2

    def step(value, by):
        return lax.rem(value + (by + SIDE), SIDE)

    def along_x(by):
        return {"item": step(x, by) * SIDE + y}

    def along_y(by):
        return {"item": x * SIDE + step(y, by)}

    other = {"edge": 1 - e}
    p1, p2 = (x, y), (y, x)
    ring1, ring2 = (along_x, along_y), (along_y, along_x)

    def block_at(h, k1):
        return (h * SIDE + step(p1[h], k1)) * block

    def seg_at(h, k1, k2):
        return block_at(h, k1) + step(p2[h], k2) * seg

    own_copies = fetch(
        [(emb.at[rows_at(e * part.shape[0] + seg_at(h, 0, 0), seg, seg)], own_rows.at[h]) for h in range(2)]
        + [(weight_hbm, weight)],
        local_sem,
    )

    def mine(h, k, start, size):
        return part[rows_at(block_at(h, k) + start, size, half2), :]

    for h in range(2):
        sums[h, 2] = mine(h, 2, 0, block).astype(BF16)
        sums[h, 1, pl.ds(half, half)] = mine(h, 1, half, half).astype(BF16)
        sums[h, 3, pl.ds(0, half)] = mine(h, 3, 0, half).astype(BF16)
    enter([along_x(1), along_x(-1), along_x(2), along_y(1), along_y(-1), along_y(2), other])
    w = Wires(send_sem, recv_sem)

    to_far, near = {}, {}
    for h in range(2):
        to_far[h, 1] = w.start(sums.at[h, 2, pl.ds(0, half)], opposite.at[h, 0], ring1[h](1))
        to_far[h, -1] = w.start(sums.at[h, 2, pl.ds(half, half)], opposite.at[h, 1], ring1[h](-1))
    for h in range(2):
        near[h, 1, 0] = w.start(sums.at[h, 1, pl.ds(half, half)], final.at[h, 0, pl.ds(half, half)], ring1[h](1))
        near[h, -1, 0] = w.start(sums.at[h, 3, pl.ds(0, half)], final.at[h, 1, pl.ds(0, half)], ring1[h](-1))

    slots = found.shape[0]
    lane = lax.broadcasted_iota(jnp.int32, (slots, TILE), 1)
    hits = found[...] + row_hits(links[pl.ds(0, slots), :], lane, TILE // 2, TILE)
    degrees_of(cnt, hits.astype(BF16), meta[1:2, 0:slots])
    core_cnt = w.start(cnt, got_cnt.at[0], other)
    for h in range(2):
        to_far[h, 1].wait_recv()
        sums[h, 1, pl.ds(0, half)] = (mine(h, 1, 0, half) + up(opposite[h, 0])).astype(BF16)
        near[h, 1, 1] = w.start(sums.at[h, 1, pl.ds(0, half)], final.at[h, 0, pl.ds(0, half)], ring1[h](1))
        to_far[h, -1].wait_recv()
        sums[h, 3, pl.ds(half, half)] = (mine(h, 3, half, half) + up(opposite[h, 1])).astype(BF16)
        near[h, -1, 1] = w.start(sums.at[h, 3, pl.ds(half, half)], final.at[h, 1, pl.ds(half, half)], ring1[h](-1))
    core_cnt.wait_recv()
    total_cnt[0] = cnt[...] + got_cnt[0]
    cnt_x = [w.start(total_cnt.at[0], got_cnt.at[1 + k], along_x(by)) for k, by in enumerate((1, -1, 2))]
    for h in range(2):
        near[h, 1, 0].wait_recv()
        near[h, -1, 0].wait_recv()
        total[h, pl.ds(0, half)] = mine(h, 0, 0, half) + up(final[h, 1, pl.ds(0, half)])
        total[h, pl.ds(half, half)] = mine(h, 0, half, half) + up(final[h, 0, pl.ds(half, half)])

    def ready(h, k, start, size):
        return total[h, rows_at(step(p2[h], k) * seg + start, size, half2), :]

    to_far2, near2 = {}, {}
    for h in range(2):
        near[h, 1, 1].wait_recv()
        near[h, -1, 1].wait_recv()
        total[h, pl.ds(0, half)] += up(final[h, 0, pl.ds(0, half)])
        total[h, pl.ds(half, half)] += up(final[h, 1, pl.ds(half, half)])
        small[h, 0] = ready(h, 2, 0, seg).astype(BF16)
        to_far2[h, 1] = w.start(small.at[h, 0, pl.ds(0, half2)], opposite2.at[h, 0], ring2[h](1))
        to_far2[h, -1] = w.start(small.at[h, 0, pl.ds(half2, half2)], opposite2.at[h, 1], ring2[h](-1))
        small[h, 1, pl.ds(half2, half2)] = ready(h, 1, half2, half2).astype(BF16)
        near2[h, 1, 0] = w.start(small.at[h, 1, pl.ds(half2, half2)], final2.at[h, 0, pl.ds(half2, half2)], ring2[h](1))
        small[h, 2, pl.ds(0, half2)] = ready(h, -1, 0, half2).astype(BF16)
        near2[h, -1, 0] = w.start(small.at[h, 2, pl.ds(0, half2)], final2.at[h, 1, pl.ds(0, half2)], ring2[h](-1))
    for copy in cnt_x:
        copy.wait_recv()
    total_cnt[1] = total_cnt[0] + got_cnt[1] + got_cnt[2] + got_cnt[3]
    cnt_y = [w.start(total_cnt.at[1], got_cnt.at[4 + k], along_y(by)) for k, by in enumerate((1, -1, 2))]
    for h in range(2):
        to_far2[h, 1].wait_recv()
        small[h, 1, pl.ds(0, half2)] = (ready(h, 1, 0, half2) + up(opposite2[h, 0])).astype(BF16)
        near2[h, 1, 1] = w.start(small.at[h, 1, pl.ds(0, half2)], final2.at[h, 0, pl.ds(0, half2)], ring2[h](1))
        to_far2[h, -1].wait_recv()
        small[h, 2, pl.ds(half2, half2)] = (ready(h, -1, half2, half2) + up(opposite2[h, 1])).astype(BF16)
        near2[h, -1, 1] = w.start(small.at[h, 2, pl.ds(half2, half2)], final2.at[h, 1, pl.ds(half2, half2)], ring2[h](-1))
    for copy in cnt_y:
        copy.wait_recv()
    total_cnt[2] = total_cnt[1] + got_cnt[4] + got_cnt[5] + got_cnt[6]

    for copy in own_copies:
        copy.wait()
    own_diag = lax.broadcasted_iota(jnp.int32, (seg, TILE), 0) == lax.broadcasted_iota(jnp.int32, (seg, TILE), 1)
    degrees = []
    for h in range(2):
        degree = total_cnt[2, step(p2[h], 0), pl.ds((e * 2 + h) * SIDE + p1[h], 1), :]
        degree = jnp.sum(jnp.where(own_diag, jnp.broadcast_to(degree, (seg, TILE)), 0.0), axis=1, keepdims=True)
        degrees.append(jnp.maximum(degree, 1.0))
    for h in range(2):
        for s in (1, -1):
            near2[h, s, 0].wait_recv()
            near2[h, s, 1].wait_recv()
        summed = ready(h, 0, 0, seg) + up(final2[h, 0]) + up(final2[h, 1])
        average = (summed / degrees[h]).astype(BF16)
        v = jnp.dot(average, weight[...], preferred_element_type=F32)
        fresh = up(own_rows[h]) + v / (1.0 + jnp.exp(-v))
        users[rows_at(seg_at(h, 0, 0), seg, seg), :] = fresh.astype(BF16)

    def send(h, k1, k2, start, size, device):
        there = users.at[rows_at(seg_at(h, k1, k2) + start, size, half2)]
        return w.start(there, there, device)

    c1, c2, c2f = {}, {}, {}

    def spread(h, k2):
        for s in (1, -1):
            c2[h, k2, s] = send(h, 0, k2, 0, seg, ring1[h](s))

    def relay(h, k2):
        c2[h, k2, 1].wait_recv()
        c2f[h, k2, 1] = send(h, -1, k2, 0, half2, ring1[h](1))
        c2[h, k2, -1].wait_recv()
        c2f[h, k2, -1] = send(h, 1, k2, half2, half2, ring1[h](-1))

    for h in range(2):
        for s in (1, -1, 2):
            c1[h, s] = send(h, 0, 0, 0, seg, ring2[h](s))
    for h in range(2):
        spread(h, 0)
    for h in range(2):
        for s in (1, -1):
            c1[h, s].wait_recv()
            spread(h, -s)
    for h in range(2):
        relay(h, 0)
    for h in range(2):
        c1[h, 2].wait_recv()
        spread(h, 2)
    for k2 in (-1, 1, 2):
        for h in range(2):
            relay(h, k2)
    for copy in c2f.values():
        copy.wait_recv()
    w.finish()
    assert len(w.made) == PLANE_COPIES, len(w.made)


DEPTH = 8
COLUMN_COPIES = 8 + 14 + 8


def column_kernel(
    part, hits, items, up_weight, down_weight, out, to_core, from_core, sums, got_up, got_down, chip_hits, got_hits, own_rows, up_v,
    down_v, local_sem, send_sem, recv_sem,
):
    u, e = lax.axis_index("user"), lax.axis_index("edge")
    share = out.shape[0]
    half = share // 2

    def step(by):
        return lax.rem(u + (by + DEPTH), DEPTH)

    other = {"edge": 1 - e}
    place = {1: {"user": step(1)}, -1: {"user": step(-1)}}

    def chunk(k, core):
        return (step(k) * 2 + core) * share

    local = [
        pltpu.make_async_copy(items.at[rows_at(chunk(0, e), share, share)], own_rows, local_sem.at[0]),
        pltpu.make_async_copy(up_weight, up_v, local_sem.at[1]),
        pltpu.make_async_copy(down_weight, down_v, local_sem.at[2]),
    ]
    for copy in local:
        copy.start()
    enter([place[1], place[-1], other])
    w = Wires(send_sem, recv_sem)
    core_hits = w.start(hits, got_hits.at[0], other)
    core = {}
    for k in (4, 3, -3, 2, -2, 1, -1, 0):
        to_core[k % DEPTH] = part[rows_at(chunk(k, 1 - e), share, share), :].astype(BF16)
        core[k] = w.start(to_core.at[k % DEPTH], from_core.at[k % DEPTH], other)

    def mine(k, q):
        return part[rows_at(chunk(k, e) + q * half, half, half), :] + up(from_core[k % DEPTH, pl.ds(q * half, half), :])

    got = {1: got_up, -1: got_down}
    wires = {}
    hit_wires = {}

    landed = set()

    def land(k):
        if k not in landed:
            landed.add(k)
            core[k].wait_recv()

    def pass_on(s, k, q):
        land(4 if k == 4 else s * k)
        value = mine(s * k, q)
        if (s, k + 1, q) in wires:
            wires[s, k + 1, q].wait_recv()
            value += up(got[s][k, q])
        running = (s * k) % DEPTH, pl.ds(q * half, half)
        sums[running] = value.astype(BF16)
        wires[s, k, q] = w.start(sums.at[running], got[s].at[k - 1, q], place[s])

    for k in (4, 3):
        for s in (1, -1):
            pass_on(s, k, int((s == 1) == (k == 3)))
    core_hits.wait_recv()
    chip_hits[...] = hits[...] + got_hits[0]
    for s in (1, -1):
        hit_wires[s, 1] = w.start(chip_hits, got_hits.at[1 if s == 1 else 5], place[s])
    for k in (3, 2, 1):
        for s, q in ((1, 0), (-1, 1)):
            pass_on(s, k, q)
        far = 5 - k
        for s in (1, -1):
            hit_wires[s, far - 1].wait_recv()
            if s == 1 or far < 4:
                base = 1 if s == 1 else 5
                hit_wires[s, far] = w.start(got_hits.at[base + far - 2], got_hits.at[base + far - 1], place[s])
        if k > 1:
            for s, q in ((1, 1), (-1, 0)):
                pass_on(s, k - 1, q)
    hit_wires[1, 4].wait_recv()
    land(0)
    degree = chip_hits[...]
    for k in range(1, DEPTH):
        degree += got_hits[k]
    lane = lax.broadcasted_iota(jnp.int32, degree.shape, 1)
    for copy in local:
        copy.wait()
    for q in range(2):
        wires[1, 1, q].wait_recv()
        wires[-1, 1, q].wait_recv()
    for q in range(2):
        summed = mine(0, q) + up(got_up[0, q]) + up(got_down[0, q])
        mine_only = jnp.where(lane == (u * 2 + e) * 2 + q, degree, 0.0)
        own_degree = jnp.sum(mine_only[0:1, :], axis=1, keepdims=True)
        merged = up(own_rows[pl.ds(q * half, half), :]) + summed / jnp.maximum(own_degree, 1.0)
        v = jnp.dot(merged.astype(BF16), up_v[...], preferred_element_type=F32)
        hidden = (v / (1.0 + jnp.exp(-v))).astype(BF16)
        out[pl.ds(q * half, half), :] = (merged + jnp.dot(hidden, down_v[...], preferred_element_type=F32)).astype(BF16)
    w.finish()
    assert len(w.made) <= COLUMN_COPIES, len(w.made)


def vmem():
    return pl.BlockSpec(memory_space=VM)


def smem():
    return pl.BlockSpec(memory_space=pltpu.SMEM)


def hbm():
    return pl.BlockSpec(memory_space=pltpu.HBM)


MIB = 2**20


def swap(bi, bu, count, links, items):
    slots = links.shape[0]
    return pl.pallas_call(
        swap_kernel,
        out_shape=(
            jax.ShapeDtypeStruct((16, TILE), jnp.int32),
            jax.ShapeDtypeStruct((2 * slots, TILE), jnp.int32),
            jax.ShapeDtypeStruct((slots, TILE), F32),
            jax.ShapeDtypeStruct((8, TILE), F32),
            jax.ShapeDtypeStruct(items.shape, BF16),
        ),
        in_specs=[hbm()] * 5,
        out_specs=(vmem(),) * 5,
        scratch_shapes=[
            VM((1, slots), jnp.int32),
            VM((1, slots), jnp.int32),
            pltpu.SMEM((1,), jnp.int32),
            pltpu.SemaphoreType.DMA((5,)),
            pltpu.SemaphoreType.DMA((2,)),
            pltpu.SemaphoreType.DMA((2,)),
        ],
        compiler_params=pltpu.CompilerParams(collective_id=2, has_side_effects=True, vmem_limit_bytes=16 * MIB),
        name="swap",
    )(bi, bu, count, links, items)


def hop(from_items, meta, links, source, rows, half_tiles):
    slots = links.shape[0]
    return pl.pallas_call(
        functools.partial(hop_kernel, from_items, half_tiles),
        out_shape=jax.ShapeDtypeStruct((rows, source.shape[1]), F32),
        in_specs=[vmem()] * 3,
        out_specs=vmem(),
        scratch_shapes=[pltpu.SMEM(meta.shape, jnp.int32)]
        + [pltpu.SMEM((slots + GROUP,), jnp.int32)] * 3
        + [pltpu.SemaphoreType.DMA((1,))],
        compiler_params=pltpu.CompilerParams(vmem_limit_bytes=24 * MIB),
        name="hop1" if from_items else "hop2",
    )(meta, links, source)


def plane(part, meta, links, found, emb, weight):
    rows, channels = part.shape
    seg = rows // (2 * SIDE * SIDE)
    block = SIDE * seg
    cnt = (SIDE, 2 * rows // (3 * TILE), TILE)
    return pl.pallas_call(
        plane_kernel,
        out_shape=jax.ShapeDtypeStruct((rows, channels), BF16),
        in_specs=[vmem()] * 4 + [hbm()] * 2,
        out_specs=vmem(),
        scratch_shapes=[
            VM((2, SIDE, block, channels), BF16),
            VM((2, 2, block // 2, channels), BF16),
            VM((2, 2, block, channels), BF16),
            VM((2, block, channels), F32),
            VM((2, 2, seg // 2, channels), BF16),
            VM((2, 2, seg, channels), BF16),
            VM((2, 3, seg, channels), BF16),
            VM(cnt, F32),
            VM((3,) + cnt, F32),
            VM((7,) + cnt, F32),
            VM((2, seg, channels), BF16),
            VM(weight.shape, BF16),
            pltpu.SemaphoreType.DMA((3,)),
            pltpu.SemaphoreType.DMA((PLANE_COPIES,)),
            pltpu.SemaphoreType.DMA((PLANE_COPIES,)),
        ],
        compiler_params=pltpu.CompilerParams(collective_id=0, has_side_effects=True, vmem_limit_bytes=32 * MIB),
        name="plane",
    )(part, meta, links, found, emb, weight)


def column(part, hits, items, up_weight, down_weight):
    rows, channels = part.shape
    share = rows // (2 * DEPTH)
    return pl.pallas_call(
        column_kernel,
        out_shape=jax.ShapeDtypeStruct((share, channels), BF16),
        in_specs=[vmem(), vmem(), hbm(), hbm(), hbm()],
        out_specs=vmem(),
        scratch_shapes=[
            VM((DEPTH, share, channels), BF16),
            VM((DEPTH, share, channels), BF16),
            VM((DEPTH, share, channels), BF16),
            VM((4, 2, share // 2, channels), BF16),
            VM((4, 2, share // 2, channels), BF16),
            VM(hits.shape, F32),
            VM((DEPTH,) + hits.shape, F32),
            VM((share, channels), BF16),
            VM(up_weight.shape, BF16),
            VM(down_weight.shape, BF16),
            pltpu.SemaphoreType.DMA((3,)),
            pltpu.SemaphoreType.DMA((COLUMN_COPIES,)),
            pltpu.SemaphoreType.DMA((COLUMN_COPIES,)),
        ],
        compiler_params=pltpu.CompilerParams(collective_id=1, has_side_effects=True, vmem_limit_bytes=40 * MIB),
        name="column",
    )(part, hits, items, up_weight, down_weight)


def pin(*xs):
    return [pltpu.with_memory_space_constraint(x, pltpu.HBM) for x in xs]


def body(item_emb, user_emb, block_item, block_user, block_rows, block_count, user_weight, up_weight, down_weight):
    bi, bu, count = block_item.reshape(1, -1), block_user.reshape(1, -1), block_count.reshape(-1)
    links = block_rows.reshape(-1, TILE)
    bi, bu, links, item_emb, user_emb, user_weight, up_weight, down_weight = pin(
        bi, bu, links, item_emb, user_emb, user_weight, up_weight, down_weight
    )
    half_rows = user_emb.shape[0] // 2
    meta, links, found, hits, items = swap(bi, bu, count, links, item_emb)
    user_part = hop(True, meta, links, items, half_rows, half_rows // TILE)
    users = plane(user_part, meta, links, found, user_emb, user_weight)
    item_part = hop(False, meta, links, users, item_emb.shape[0], half_rows // TILE)
    return column(item_part, hits, item_emb, up_weight, down_weight)


def solution(mesh):
    return jax.shard_map(
        body,
        mesh=mesh,
        in_specs=(
            P("item", None),
            P("user", None),
            P("item", "user", "edge", None),
            P("item", "user", "edge", None),
            P("item", "user", "edge", None, None),
            P("item", "user", "edge"),
            P(),
            P(),
            P(),
        ),
        out_specs=P(("item", "user", "edge"), None),
        check_vma=False,
    )
```

```python
import functools

import jax
import jax.numpy as jnp
from jax import lax
from jax.experimental import pallas as pl
from jax.experimental.pallas import tpu as pltpu
from jax.sharding import PartitionSpec as P

TILE = 128
MESH = pl.DeviceIdType.MESH
F32 = jnp.float32
BF16 = jnp.bfloat16
GROUP = 16
NOWHERE = 2**10
VM = pltpu.VMEM


def rows_at(offset, count, unit):
    return pl.ds(pl.multiple_of(offset, unit), count)


def fetch(pairs, sems):
    copies = [pltpu.make_async_copy(src, dst, sems.at[at]) for at, (src, dst) in enumerate(pairs)]
    for copy in copies:
        copy.start()
    return copies


def swap_kernel(
    bi_hbm, bu_hbm, count_hbm, links_hbm, items_hbm, meta, links, found, hits, items, bi, bu, count, local_sem, send_sem, recv_sem
):
    slots = links_hbm.shape[0]
    other = {"edge": 1 - lax.axis_index("edge")}
    own = links.at[pl.ds(0, slots)]
    copies = fetch(
        [(bi_hbm, bi), (bu_hbm, bu), (count_hbm, count), (links_hbm, own), (items_hbm, items)], local_sem
    )
    enter([other])
    w = Wires(send_sem, recv_sem)
    for copy in copies[:3]:
        copy.wait()
    slot = lax.broadcasted_iota(jnp.int32, (1, slots), 1)
    live = slot < count[0]
    meta[0:1, 0:slots] = bi[...]
    meta[1:2, 0:slots] = jnp.where(live, bu[...], NOWHERE)
    copies[3].wait()
    w.start(own, links.at[pl.ds(slots, slots)], other)
    lane = lax.broadcasted_iota(jnp.int32, (slots, TILE), 1)
    found[...] = row_hits(links[pl.ds(0, slots), :], lane, 0, TILE // 4)
    w.start(meta.at[pl.ds(0, 8)], meta.at[pl.ds(8, 8)], other)
    found[...] += row_hits(links[pl.ds(0, slots), :], lane, TILE // 4, TILE // 2)
    slot = lax.broadcasted_iota(jnp.int32, (TILE, slots), 1)
    tile = lax.broadcasted_iota(jnp.int32, (TILE, slots), 0)
    chosen = ((tile == bi[...]) & (slot < count[0])).astype(F32).astype(BF16)
    ones = jnp.ones((8, slots), BF16)
    hits[...] = lax.dot_general(ones, chosen, (((1,), (1,)), ((), ())), preferred_element_type=F32)
    copies[4].wait()
    for copy in w.made:
        copy.wait_recv()
    w.finish()


def row_hits(links, lane, first, last):
    found = jnp.zeros(lane.shape, F32)
    for r in range(first, last):
        found += (links[:, r : r + 1] == lane).astype(F32)
    return found


def hop_kernel(from_items, half_tiles, meta_ref, links, source, acc, meta, src, dst, slot, sem):
    e = lax.axis_index("edge")
    slots = links.shape[0] // 2
    copy = fetch([(meta_ref, meta)], sem)[0]
    groups = 16
    each = 2 * slots // groups
    rows = acc.shape[0] // groups
    copy.wait()

    def choose(g, n):
        acc[rows_at(g * rows, rows, rows), :] = jnp.zeros((rows, acc.shape[1]), F32)
        which = g // (groups // 2)
        base = (g - which * (groups // 2)) * each
        for j in range(each):
            ut = meta[which * 8 + 1, base + j] - e * half_tiles
            ends = meta[which * 8, base + j] * TILE, ut * TILE
            src[n], dst[n] = ends if from_items else ends[::-1]
            slot[n] = g * each + j
            n = n + jnp.where((ut >= 0) & (ut < half_tiles), 1, 0)
        return n

    count = lax.fori_loop(0, groups, choose, 0)
    inside = lax.broadcasted_iota(jnp.int32, (TILE, TILE), 0)

    def blocks(group, carry):
        made = []
        for k in range(GROUP):
            b = group * GROUP + k
            live = b < count
            row = jnp.where(live, links[pl.ds(jnp.where(live, slot[b], 0), 1), :], -1)
            onehot = (row == inside).astype(F32).astype(BF16)
            rows = source[rows_at(jnp.where(live, src[b], 0), TILE, TILE), :]
            dims = (((1,), (0,)), ((), ())) if from_items else (((0,), (0,)), ((), ()))
            contrib = lax.dot_general(onehot, rows, dims, preferred_element_type=F32)
            made.append((jnp.where(live, dst[b], 0), contrib))
        for at, contrib in made:
            acc[rows_at(at, TILE, TILE), :] += contrib
        return carry

    lax.fori_loop(0, (count + GROUP - 1) // GROUP, blocks, 0)


def degrees_of(cnt_ref, found, bu):
    slots = bu.shape[1]
    triples = cnt_ref.shape[0]
    which = lax.broadcasted_iota(jnp.int32, (triples, slots), 0) * 3
    a, b, c = (
        jnp.dot((which + k == bu).astype(F32).astype(BF16), found, preferred_element_type=F32) for k in range(3)
    )
    lanes = lax.broadcasted_iota(jnp.int32, (triples, TILE), 1)
    quarters = (
        a,
        jnp.where(lanes < 32, pltpu.roll(a, 32, 1), pltpu.roll(b, 32, 1)),
        jnp.where(lanes < 64, pltpu.roll(b, 64, 1), pltpu.roll(c, 64, 1)),
        pltpu.roll(c, 96, 1),
    )
    for j in range(triples):
        for q, counts in enumerate(quarters):
            cnt_ref[j, q : q + 1, :] = counts[j : j + 1, :]


class Wires:
    def __init__(self, send_sem, recv_sem):
        self.send_sem, self.recv_sem, self.made = send_sem, recv_sem, []

    def start(self, src, dst, device):
        at = len(self.made)
        copy = pltpu.make_async_remote_copy(
            src_ref=src,
            dst_ref=dst,
            send_sem=self.send_sem.at[at],
            recv_sem=self.recv_sem.at[at],
            device_id=device,
            device_id_type=MESH,
        )
        copy.start()
        self.made.append(copy)
        return copy

    def finish(self):
        for copy in self.made:
            copy.wait_send()


def enter(peers):
    barrier = pltpu.get_barrier_semaphore()
    for peer in peers:
        pl.semaphore_signal(barrier, inc=1, device_id=peer, device_id_type=MESH)
    pl.semaphore_wait(barrier, len(peers))


def up(x):
    return x.astype(F32)


SIDE = 4
PLANE_COPIES = 103


def plane_kernel(
    part, meta, links, found, emb, weight_hbm, users, sums, opposite, final, total, small, final2, cnt, got_core, chip_cnt,
    got_cnt, ring_cnt, got_cnt2, own_rows, weight, local_sem, send_sem, recv_sem,
):
    item, e = lax.axis_index("item"), lax.axis_index("edge")
    x, y = item // SIDE, item % SIDE
    seg = part.shape[0] // (2 * SIDE * SIDE)
    block = SIDE * seg
    half2 = seg // 2

    def step(value, by):
        return lax.rem(value + (by + SIDE), SIDE)

    def along_x(by):
        return {"item": step(x, by) * SIDE + y}

    def along_y(by):
        return {"item": x * SIDE + step(y, by)}

    other = {"edge": 1 - e}
    p1, p2 = (x, y), (y, x)
    ring1, ring2 = (along_x, along_y), (along_y, along_x)

    def block_at(h, k1):
        return (h * SIDE + step(p1[h], k1)) * block

    def seg_at(h, k1, k2):
        return block_at(h, k1) + step(p2[h], k2) * seg

    own_copies = fetch(
        [(emb.at[rows_at(e * part.shape[0] + seg_at(h, 0, 0), seg, seg)], own_rows.at[h]) for h in range(2)]
        + [(weight_hbm, weight)],
        local_sem,
    )

    def mine(h, k1, k2, start, size):
        return part[rows_at(seg_at(h, k1, k2) + start, size, half2), :]

    low, high = pl.ds(0, half2), pl.ds(half2, half2)
    order = (2, 1, -1, 0)
    for k2 in order:
        for h in range(2):
            sums[h, 2, k2 % SIDE] = mine(h, 2, k2, 0, seg).astype(BF16)
    cnt[...] = jnp.zeros_like(cnt)
    enter([along_x(1), along_x(-1), along_x(2), along_y(1), along_y(-1), along_y(2), other])
    w = Wires(send_sem, recv_sem)

    far, near, passed = {}, {}, {}

    def direct(k2):
        at = k2 % SIDE
        for h in range(2):
            sums[h, 1, at, high] = mine(h, 1, k2, half2, half2).astype(BF16)
            near[h, k2, 1] = w.start(sums.at[h, 1, at, high], final.at[h, 0, at, high], ring1[h](1))
            sums[h, 3, at, low] = mine(h, -1, k2, 0, half2).astype(BF16)
            near[h, k2, -1] = w.start(sums.at[h, 3, at, low], final.at[h, 1, at, low], ring1[h](-1))

    def combine(k2):
        at = k2 % SIDE
        for h in range(2):
            far[h, k2, 1].wait_recv()
            sums[h, 1, at, low] = (mine(h, 1, k2, 0, half2) + up(opposite[h, 0, at])).astype(BF16)
            passed[h, k2, 1] = w.start(sums.at[h, 1, at, low], final.at[h, 0, at, low], ring1[h](1))
            far[h, k2, -1].wait_recv()
            sums[h, 3, at, high] = (mine(h, -1, k2, half2, half2) + up(opposite[h, 1, at])).astype(BF16)
            passed[h, k2, -1] = w.start(sums.at[h, 3, at, high], final.at[h, 1, at, high], ring1[h](-1))

    def finished(h, k2):
        for s in (1, -1):
            near[h, k2, s].wait_recv()
            passed[h, k2, s].wait_recv()
        at = k2 % SIDE
        return mine(h, 0, k2, 0, seg) + up(final[h, 0, at]) + up(final[h, 1, at])

    for k2 in order:
        at = k2 % SIDE
        for h in range(2):
            far[h, k2, 1] = w.start(sums.at[h, 2, at, low], opposite.at[h, 0, at], ring1[h](1))
            far[h, k2, -1] = w.start(sums.at[h, 2, at, high], opposite.at[h, 1, at], ring1[h](-1))
    direct(2)

    slots = found.shape[0]
    lane = lax.broadcasted_iota(jnp.int32, (slots, TILE), 1)
    hits = found[...] + row_hits(links[pl.ds(0, slots), :], lane, TILE // 2, TILE)
    degrees_of(cnt, hits.astype(BF16), meta[1:2, 0:slots])
    shared = 2 * SIDE
    core_cnt = w.start(cnt.at[pl.ds((1 - e) * shared, shared)], got_core, other)

    combine(2)
    direct(1)
    direct(-1)
    core_cnt.wait_recv()
    chip_cnt[...] = cnt[pl.ds(e * shared, shared)] + got_core[...]
    cnt1 = [
        w.start(chip_cnt.at[h * SIDE + step(p1[h], by)], got_cnt.at[h, k], ring1[h](by))
        for h in range(2)
        for k, by in enumerate((1, -1, 2))
    ]
    combine(1)
    combine(-1)
    direct(0)

    near2 = []
    for h in range(2):
        small[h, 0] = finished(h, 2).astype(BF16)
        near2.append(w.start(small.at[h, 0], final2.at[h, 0], ring2[h](2)))
    combine(0)
    for copy in cnt1:
        copy.wait_recv()
    for h in range(2):
        ring_cnt[h] = chip_cnt[h * SIDE + step(p1[h], 0)] + got_cnt[h, 0] + got_cnt[h, 1] + got_cnt[h, 2]
    cnt2 = [
        w.start(ring_cnt.at[h], got_cnt2.at[h, k], ring2[h](by)) for h in range(2) for k, by in enumerate((1, -1, 2))
    ]
    for h in range(2):
        small[h, 1] = finished(h, 1).astype(BF16)
        near2.append(w.start(small.at[h, 1], final2.at[h, 1], ring2[h](1)))
        small[h, 2] = finished(h, -1).astype(BF16)
        near2.append(w.start(small.at[h, 2], final2.at[h, 2], ring2[h](-1)))
    for h in range(2):
        total[h] = finished(h, 0)

    for copy in own_copies:
        copy.wait()
    for copy in cnt2:
        copy.wait_recv()
    own_diag = lax.broadcasted_iota(jnp.int32, (seg, TILE), 0) == lax.broadcasted_iota(jnp.int32, (seg, TILE), 1)
    degrees = []
    for h in range(2):
        counts = ring_cnt[h] + got_cnt2[h, 0] + got_cnt2[h, 1] + got_cnt2[h, 2]
        own_row = lax.broadcasted_iota(jnp.int32, counts.shape, 0) == p2[h]
        degree = jnp.sum(jnp.where(own_row, counts, 0.0), axis=0, keepdims=True)
        degree = jnp.sum(jnp.where(own_diag, jnp.broadcast_to(degree, (seg, TILE)), 0.0), axis=1, keepdims=True)
        degrees.append(jnp.maximum(degree, 1.0))
    for copy in near2:
        copy.wait_recv()
    for h in range(2):
        summed = total[h] + up(final2[h, 0]) + up(final2[h, 1]) + up(final2[h, 2])
        average = (summed / degrees[h]).astype(BF16)
        v = jnp.dot(average, weight[...], preferred_element_type=F32)
        fresh = up(own_rows[h]) + v / (1.0 + jnp.exp(-v))
        users[rows_at(seg_at(h, 0, 0), seg, seg), :] = fresh.astype(BF16)

    def send(h, k1, k2, start, size, device):
        there = users.at[rows_at(seg_at(h, k1, k2) + start, size, half2)]
        return w.start(there, there, device)

    c1, c2, c2f = {}, {}, {}

    def spread(h, k2):
        for s in (1, -1):
            c2[h, k2, s] = send(h, 0, k2, 0, seg, ring1[h](s))
        if k2 == 2:
            c2f[h, k2, 0] = send(h, 0, k2, 0, seg, ring1[h](2))

    def relay(h, k2):
        c2[h, k2, 1].wait_recv()
        c2f[h, k2, 1] = send(h, -1, k2, 0, half2, ring1[h](1))
        c2[h, k2, -1].wait_recv()
        c2f[h, k2, -1] = send(h, 1, k2, half2, half2, ring1[h](-1))

    for h in range(2):
        for s in (1, -1, 2):
            c1[h, s] = send(h, 0, 0, 0, seg, ring2[h](s))
    for h in range(2):
        spread(h, 0)
    for h in range(2):
        for s in (1, -1):
            c1[h, s].wait_recv()
            spread(h, -s)
    for h in range(2):
        c1[h, 2].wait_recv()
        spread(h, 2)
    for k2 in (0, -1, 1):
        for h in range(2):
            relay(h, k2)
    for h in range(2):
        for s in (1, -1):
            c2[h, 2, s].wait_recv()
    for copy in c2f.values():
        copy.wait_recv()
    w.finish()
    assert len(w.made) == PLANE_COPIES, len(w.made)


DEPTH = 8
PARTS = 4
COLUMN_COPIES = 8 + 7 * PARTS + 8


def column_kernel(
    part, hits, items, up_weight, down_weight, out, to_core, from_core, sums, got_up, got_down, chip_hits, got_hits, own_rows, arrived,
    up_v, down_v, local_sem, send_sem, recv_sem,
):
    u, e = lax.axis_index("user"), lax.axis_index("edge")
    share = out.shape[0]
    half = share // PARTS

    def step(by):
        return lax.rem(u + (by + DEPTH), DEPTH)

    other = {"edge": 1 - e}
    place = {1: {"user": step(1)}, -1: {"user": step(-1)}}

    def chunk(k, core):
        return (step(k) * 2 + core) * share

    local = [
        pltpu.make_async_copy(items.at[rows_at(chunk(0, e), share, share)], own_rows, local_sem.at[0]),
        pltpu.make_async_copy(up_weight, up_v, local_sem.at[1]),
        pltpu.make_async_copy(down_weight, down_v, local_sem.at[2]),
    ]
    for copy in local:
        copy.start()
    enter([place[1], place[-1], other])
    w = Wires(send_sem, recv_sem)
    core_hits = w.start(hits, got_hits.at[0], other)
    core = {}
    for k in (4, 3, -3, 2, -2, 1, -1, 0):
        to_core[k % DEPTH] = part[rows_at(chunk(k, 1 - e), share, share), :].astype(BF16)
        core[k] = w.start(to_core.at[k % DEPTH], from_core.at[k % DEPTH], other)

    def mine(k, q):
        return part[rows_at(chunk(k, e) + q * half, half, half), :] + up(from_core[k % DEPTH, pl.ds(q * half, half), :])

    got = {1: got_up, -1: got_down}
    wires = {}
    hit_wires = {}

    landed = set()

    def land(k):
        if k not in landed:
            landed.add(k)
            core[k].wait_recv()

    def pass_on(s, k, q):
        land(4 if k == 4 else s * k)
        value = mine(s * k, q)
        if (s, k + 1, q) in wires:
            wires[s, k + 1, q].wait_recv()
            value += up(got[s][k, q])
        running = (s * k) % DEPTH, pl.ds(q * half, half)
        sums[running] = value.astype(BF16)
        wires[s, k, q] = w.start(sums.at[running], got[s].at[k - 1, q], place[s])

    first = [(s, j if s == 1 else PARTS // 2 + j) for j in range(PARTS // 2) for s in (1, -1)]
    second = [(s, PARTS // 2 + j if s == 1 else j) for j in range(PARTS // 2) for s in (1, -1)]
    for s, q in first:
        pass_on(s, 4, q)
    for s, q in second:
        pass_on(s, 3, q)
    core_hits.wait_recv()
    chip_hits[...] = hits[...] + got_hits[0]
    for s in (1, -1):
        hit_wires[s, 1] = w.start(chip_hits, got_hits.at[1 if s == 1 else 5], place[s])
    for k in (3, 2, 1):
        for s, q in first:
            pass_on(s, k, q)
        far = 5 - k
        for s in (1, -1):
            hit_wires[s, far - 1].wait_recv()
            if s == 1 or far < 4:
                base = 1 if s == 1 else 5
                hit_wires[s, far] = w.start(got_hits.at[base + far - 2], got_hits.at[base + far - 1], place[s])
        if k > 1:
            for s, q in second:
                pass_on(s, k - 1, q)
    hit_wires[1, 4].wait_recv()
    land(0)
    degree = chip_hits[...]
    for k in range(1, DEPTH):
        degree += got_hits[k]
    lane = lax.broadcasted_iota(jnp.int32, degree.shape, 1)
    for copy in local:
        copy.wait()
    tile = lax.div(lax.broadcasted_iota(jnp.int32, (share, 1), 0), TILE)
    own = [jnp.sum(jnp.where(lane == (u * 2 + e) * 2 + k, degree, 0.0)[0:1, :], axis=1, keepdims=True) for k in range(2)]
    own_degree = jnp.maximum(jnp.where(tile == 0, own[0], own[1]), 1.0)
    for q in range(PARTS):
        wires[1, 1, q].wait_recv()
        wires[-1, 1, q].wait_recv()
    summed = part[rows_at(chunk(0, e), share, share), :] + up(from_core[0])
    for q in range(PARTS):
        rows = pl.ds(q * half, half)
        arrived[rows, :] = up(got_up[0, q]) + up(got_down[0, q])
    merged = up(own_rows[...]) + (summed + arrived[...]) / own_degree
    v = jnp.dot(merged.astype(BF16), up_v[...], preferred_element_type=F32)
    hidden = (v / (1.0 + jnp.exp(-v))).astype(BF16)
    out[...] = (merged + jnp.dot(hidden, down_v[...], preferred_element_type=F32)).astype(BF16)
    w.finish()
    assert len(w.made) <= COLUMN_COPIES, len(w.made)


def vmem():
    return pl.BlockSpec(memory_space=VM)


def smem():
    return pl.BlockSpec(memory_space=pltpu.SMEM)


def hbm():
    return pl.BlockSpec(memory_space=pltpu.HBM)


MIB = 2**20


def swap(bi, bu, count, links, items):
    slots = links.shape[0]
    return pl.pallas_call(
        swap_kernel,
        out_shape=(
            jax.ShapeDtypeStruct((16, TILE), jnp.int32),
            jax.ShapeDtypeStruct((2 * slots, TILE), jnp.int32),
            jax.ShapeDtypeStruct((slots, TILE), F32),
            jax.ShapeDtypeStruct((8, TILE), F32),
            jax.ShapeDtypeStruct(items.shape, BF16),
        ),
        in_specs=[hbm()] * 5,
        out_specs=(vmem(),) * 5,
        scratch_shapes=[
            VM((1, slots), jnp.int32),
            VM((1, slots), jnp.int32),
            pltpu.SMEM((1,), jnp.int32),
            pltpu.SemaphoreType.DMA((5,)),
            pltpu.SemaphoreType.DMA((2,)),
            pltpu.SemaphoreType.DMA((2,)),
        ],
        compiler_params=pltpu.CompilerParams(collective_id=2, has_side_effects=True, vmem_limit_bytes=16 * MIB),
        name="swap",
    )(bi, bu, count, links, items)


def hop(from_items, meta, links, source, rows, half_tiles):
    slots = links.shape[0]
    return pl.pallas_call(
        functools.partial(hop_kernel, from_items, half_tiles),
        out_shape=jax.ShapeDtypeStruct((rows, source.shape[1]), F32),
        in_specs=[vmem()] * 3,
        out_specs=vmem(),
        scratch_shapes=[pltpu.SMEM(meta.shape, jnp.int32)]
        + [pltpu.SMEM((slots + GROUP,), jnp.int32)] * 3
        + [pltpu.SemaphoreType.DMA((1,))],
        compiler_params=pltpu.CompilerParams(vmem_limit_bytes=24 * MIB),
        name="hop1" if from_items else "hop2",
    )(meta, links, source)


def plane(part, meta, links, found, emb, weight):
    rows, channels = part.shape
    seg = rows // (2 * SIDE * SIDE)
    pieces = 4 * SIDE
    return pl.pallas_call(
        plane_kernel,
        out_shape=jax.ShapeDtypeStruct((rows, channels), BF16),
        in_specs=[vmem()] * 4 + [hbm()] * 2,
        out_specs=vmem(),
        scratch_shapes=[
            VM((2, SIDE, SIDE, seg, channels), BF16),
            VM((2, 2, SIDE, seg // 2, channels), BF16),
            VM((2, 2, SIDE, seg, channels), BF16),
            VM((2, seg, channels), F32),
            VM((2, 3, seg, channels), BF16),
            VM((2, 3, seg, channels), BF16),
            VM((pieces, 8, TILE), F32),
            VM((pieces // 2, 8, TILE), F32),
            VM((pieces // 2, 8, TILE), F32),
            VM((2, 3, 8, TILE), F32),
            VM((2, 8, TILE), F32),
            VM((2, 3, 8, TILE), F32),
            VM((2, seg, channels), BF16),
            VM(weight.shape, BF16),
            pltpu.SemaphoreType.DMA((3,)),
            pltpu.SemaphoreType.DMA((PLANE_COPIES,)),
            pltpu.SemaphoreType.DMA((PLANE_COPIES,)),
        ],
        compiler_params=pltpu.CompilerParams(collective_id=0, has_side_effects=True, vmem_limit_bytes=32 * MIB),
        name="plane",
    )(part, meta, links, found, emb, weight)


def column(part, hits, items, up_weight, down_weight):
    rows, channels = part.shape
    share = rows // (2 * DEPTH)
    return pl.pallas_call(
        column_kernel,
        out_shape=jax.ShapeDtypeStruct((share, channels), BF16),
        in_specs=[vmem(), vmem(), hbm(), hbm(), hbm()],
        out_specs=vmem(),
        scratch_shapes=[
            VM((DEPTH, share, channels), BF16),
            VM((DEPTH, share, channels), BF16),
            VM((DEPTH, share, channels), BF16),
            VM((4, PARTS, share // PARTS, channels), BF16),
            VM((4, PARTS, share // PARTS, channels), BF16),
            VM(hits.shape, F32),
            VM((DEPTH,) + hits.shape, F32),
            VM((share, channels), BF16),
            VM((share, channels), F32),
            VM(up_weight.shape, BF16),
            VM(down_weight.shape, BF16),
            pltpu.SemaphoreType.DMA((3,)),
            pltpu.SemaphoreType.DMA((COLUMN_COPIES,)),
            pltpu.SemaphoreType.DMA((COLUMN_COPIES,)),
        ],
        compiler_params=pltpu.CompilerParams(collective_id=1, has_side_effects=True, vmem_limit_bytes=40 * MIB),
        name="column",
    )(part, hits, items, up_weight, down_weight)


def pin(*xs):
    return [pltpu.with_memory_space_constraint(x, pltpu.HBM) for x in xs]


def body(item_emb, user_emb, block_item, block_user, block_rows, block_count, user_weight, up_weight, down_weight):
    bi, bu, count = block_item.reshape(1, -1), block_user.reshape(1, -1), block_count.reshape(-1)
    links = block_rows.reshape(-1, TILE)
    bi, bu, links, item_emb, user_emb, user_weight, up_weight, down_weight = pin(
        bi, bu, links, item_emb, user_emb, user_weight, up_weight, down_weight
    )
    half_rows = user_emb.shape[0] // 2
    meta, links, found, hits, items = swap(bi, bu, count, links, item_emb)
    user_part = hop(True, meta, links, items, half_rows, half_rows // TILE)
    users = plane(user_part, meta, links, found, user_emb, user_weight)
    item_part = hop(False, meta, links, users, item_emb.shape[0], half_rows // TILE)
    return column(item_part, hits, item_emb, up_weight, down_weight)


def solution(mesh):
    return jax.shard_map(
        body,
        mesh=mesh,
        in_specs=(
            P("item", None),
            P("user", None),
            P("item", "user", "edge", None),
            P("item", "user", "edge", None),
            P("item", "user", "edge", None, None),
            P("item", "user", "edge"),
            P(),
            P(),
            P(),
        ),
        out_specs=P(("item", "user", "edge"), None),
        check_vma=False,
    )
```

```python
import functools

import jax
import jax.numpy as jnp
from jax import lax
from jax.experimental import pallas as pl
from jax.experimental.pallas import tpu as pltpu
from jax.sharding import PartitionSpec as P

TILE = 128
MESH = pl.DeviceIdType.MESH
F32 = jnp.float32
BF16 = jnp.bfloat16
GROUP = 16
NOWHERE = 2**10
ITEM_TILES = 32
SLOTS = 256
VM = pltpu.VMEM


def rows_at(offset, count, unit):
    return pl.ds(pl.multiple_of(offset, unit), count)


def fetch(pairs, sems):
    copies = [pltpu.make_async_copy(src, dst, sems.at[at]) for at, (src, dst) in enumerate(pairs)]
    for copy in copies:
        copy.start()
    return copies


def swap_kernel(
    half_tiles, bi_hbm, bu_hbm, count_hbm, links_hbm, items_hbm, meta, links, found, hits, items, bi, bu, count, to_other,
    local_sem, send_sem, recv_sem,
):
    slots = links_hbm.shape[0]
    e = lax.axis_index("edge")
    other = {"edge": 1 - e}
    own = links.at[pl.ds(0, slots)]
    copies = fetch(
        [(bi_hbm, bi), (bu_hbm, bu), (count_hbm, count), (links_hbm, own), (items_hbm, items)], local_sem
    )
    greet([other])
    for copy in copies[:3]:
        copy.wait()
    slot = lax.broadcasted_iota(jnp.int32, (1, slots), 1)
    live = slot < count[0]

    def codes(core, first):
        ut = bu[...] - core * half_tiles
        code = (ut * ITEM_TILES + bi[...]) * SLOTS + slot + first
        return jnp.where(live & (ut >= 0) & (ut < half_tiles), code, -1)

    meta[0:1, 0:slots] = codes(e, 0)
    meta[1:2, 0:slots] = jnp.where(live, bu[...], NOWHERE)
    to_other[...] = jnp.zeros_like(to_other)
    to_other[0:1, 0:slots] = codes(1 - e, slots)
    meet([other])
    w = Wires(send_sem, recv_sem)
    copies[3].wait()
    w.start(own, links.at[pl.ds(slots, slots)], other)
    lane = lax.broadcasted_iota(jnp.int32, (slots, TILE), 1)
    found[...] = row_hits(links[pl.ds(0, slots), :], lane, 0, TILE // 4)
    w.start(to_other, meta.at[pl.ds(8, 8)], other)
    found[...] += row_hits(links[pl.ds(0, slots), :], lane, TILE // 4, TILE // 2)
    slot = lax.broadcasted_iota(jnp.int32, (TILE, slots), 1)
    tile = lax.broadcasted_iota(jnp.int32, (TILE, slots), 0)
    chosen = ((tile == bi[...]) & (slot < count[0])).astype(F32).astype(BF16)
    ones = jnp.ones((8, slots), BF16)
    hits[...] = lax.dot_general(ones, chosen, (((1,), (1,)), ((), ())), preferred_element_type=F32)
    copies[4].wait()
    for copy in w.made:
        copy.wait_recv()
    w.finish()


def row_hits(links, lane, first, last):
    found = jnp.zeros(lane.shape, F32)
    for r in range(first, last):
        found += (links[:, r : r + 1] == lane).astype(F32)
    return found


def hop_kernel(from_items, meta_ref, links, source, acc, meta, chosen, sem):
    slots = links.shape[0] // 2
    copy = fetch([(meta_ref, meta)], sem)[0]
    acc[...] = jnp.zeros_like(acc)
    copy.wait()
    each = 24

    def choose(g, n):
        for which in range(2):
            for j in range(each):
                code = meta[which * 8, g * each + j]
                chosen[n] = code
                n = n + 1 + lax.shift_right_arithmetic(code, 31)
        return n

    count = lax.fori_loop(0, slots // each, choose, 0)
    inside = lax.broadcasted_iota(jnp.int32, (TILE, TILE), 0)

    def blocks(group, carry):
        made = []
        for k in range(GROUP):
            b = group * GROUP + k
            live = b < count
            code = jnp.where(live, chosen[b], 0)
            it = jnp.bitwise_and(lax.shift_right_logical(code, 8), ITEM_TILES - 1) * TILE
            ut = lax.shift_right_logical(code, 13) * TILE
            src, dst = (it, ut) if from_items else (ut, it)
            row = jnp.where(live, links[pl.ds(jnp.bitwise_and(code, SLOTS - 1), 1), :], -1)
            onehot = (row == inside).astype(F32).astype(BF16)
            rows = source[rows_at(src, TILE, TILE), :]
            dims = (((1,), (0,)), ((), ())) if from_items else (((0,), (0,)), ((), ()))
            contrib = lax.dot_general(onehot, rows, dims, preferred_element_type=F32)
            made.append((dst, contrib))
        for at, contrib in made:
            acc[rows_at(at, TILE, TILE), :] += contrib
        return carry

    lax.fori_loop(0, (count + GROUP - 1) // GROUP, blocks, 0)


def degrees_of(cnt_ref, found, bu):
    slots = bu.shape[1]
    triples = cnt_ref.shape[0]
    which = lax.broadcasted_iota(jnp.int32, (triples, slots), 0) * 3
    a, b, c = (
        jnp.dot((which + k == bu).astype(F32).astype(BF16), found, preferred_element_type=F32) for k in range(3)
    )
    lanes = lax.broadcasted_iota(jnp.int32, (triples, TILE), 1)
    quarters = (
        a,
        jnp.where(lanes < 32, pltpu.roll(a, 32, 1), pltpu.roll(b, 32, 1)),
        jnp.where(lanes < 64, pltpu.roll(b, 64, 1), pltpu.roll(c, 64, 1)),
        pltpu.roll(c, 96, 1),
    )
    for j in range(triples):
        for q, counts in enumerate(quarters):
            cnt_ref[j, q : q + 1, :] = counts[j : j + 1, :]


class Wires:
    def __init__(self, send_sem, recv_sem):
        self.send_sem, self.recv_sem, self.made = send_sem, recv_sem, []

    def start(self, src, dst, device):
        at = len(self.made)
        copy = pltpu.make_async_remote_copy(
            src_ref=src,
            dst_ref=dst,
            send_sem=self.send_sem.at[at],
            recv_sem=self.recv_sem.at[at],
            device_id=device,
            device_id_type=MESH,
        )
        copy.start()
        self.made.append(copy)
        return copy

    def finish(self):
        for copy in self.made:
            copy.wait_send()


def greet(peers):
    for peer in peers:
        pl.semaphore_signal(pltpu.get_barrier_semaphore(), inc=1, device_id=peer, device_id_type=MESH)


def meet(peers):
    pl.semaphore_wait(pltpu.get_barrier_semaphore(), len(peers))


def up(x):
    return x.astype(F32)


SIDE = 4
PLANE_COPIES = 103


def plane_kernel(
    part, meta, links, found, emb, weight_hbm, users, sums, opposite, final, total, small, final2, cnt, got_core, chip_cnt,
    got_cnt, ring_cnt, got_cnt2, own_rows, weight, local_sem, send_sem, recv_sem,
):
    item, e = lax.axis_index("item"), lax.axis_index("edge")
    x, y = item // SIDE, item % SIDE
    seg = part.shape[0] // (2 * SIDE * SIDE)
    block = SIDE * seg
    half2 = seg // 2

    def step(value, by):
        return lax.rem(value + (by + SIDE), SIDE)

    def along_x(by):
        return {"item": step(x, by) * SIDE + y}

    def along_y(by):
        return {"item": x * SIDE + step(y, by)}

    other = {"edge": 1 - e}
    p1, p2 = (x, y), (y, x)
    ring1, ring2 = (along_x, along_y), (along_y, along_x)

    def block_at(h, k1):
        return (h * SIDE + step(p1[h], k1)) * block

    def seg_at(h, k1, k2):
        return block_at(h, k1) + step(p2[h], k2) * seg

    peers = [along_x(1), along_x(-1), along_x(2), along_y(1), along_y(-1), along_y(2), other]
    greet(peers)
    own_copies = fetch(
        [(emb.at[rows_at(e * part.shape[0] + seg_at(h, 0, 0), seg, seg)], own_rows.at[h]) for h in range(2)]
        + [(weight_hbm, weight)],
        local_sem,
    )

    def mine(h, k1, k2, start, size):
        return part[rows_at(seg_at(h, k1, k2) + start, size, half2), :]

    low, high = pl.ds(0, half2), pl.ds(half2, half2)
    order = (2, 1, -1, 0)
    for k2 in order:
        for h in range(2):
            sums[h, 2, k2 % SIDE] = mine(h, 2, k2, 0, seg).astype(BF16)
    cnt[...] = jnp.zeros_like(cnt)
    meet(peers)
    w = Wires(send_sem, recv_sem)

    far, near, passed = {}, {}, {}

    def direct(k2):
        at = k2 % SIDE
        for h in range(2):
            sums[h, 1, at, high] = mine(h, 1, k2, half2, half2).astype(BF16)
            near[h, k2, 1] = w.start(sums.at[h, 1, at, high], final.at[h, 0, at, high], ring1[h](1))
            sums[h, 3, at, low] = mine(h, -1, k2, 0, half2).astype(BF16)
            near[h, k2, -1] = w.start(sums.at[h, 3, at, low], final.at[h, 1, at, low], ring1[h](-1))

    def combine(k2):
        at = k2 % SIDE
        for h in range(2):
            far[h, k2, 1].wait_recv()
            sums[h, 1, at, low] = (mine(h, 1, k2, 0, half2) + up(opposite[h, 0, at])).astype(BF16)
            passed[h, k2, 1] = w.start(sums.at[h, 1, at, low], final.at[h, 0, at, low], ring1[h](1))
            far[h, k2, -1].wait_recv()
            sums[h, 3, at, high] = (mine(h, -1, k2, half2, half2) + up(opposite[h, 1, at])).astype(BF16)
            passed[h, k2, -1] = w.start(sums.at[h, 3, at, high], final.at[h, 1, at, high], ring1[h](-1))

    def finished(h, k2):
        for s in (1, -1):
            near[h, k2, s].wait_recv()
            passed[h, k2, s].wait_recv()
        at = k2 % SIDE
        return mine(h, 0, k2, 0, seg) + up(final[h, 0, at]) + up(final[h, 1, at])

    for k2 in order:
        at = k2 % SIDE
        for h in range(2):
            far[h, k2, 1] = w.start(sums.at[h, 2, at, low], opposite.at[h, 0, at], ring1[h](1))
            far[h, k2, -1] = w.start(sums.at[h, 2, at, high], opposite.at[h, 1, at], ring1[h](-1))
    direct(2)

    slots = found.shape[0]
    lane = lax.broadcasted_iota(jnp.int32, (slots, TILE), 1)
    hits = found[...] + row_hits(links[pl.ds(0, slots), :], lane, TILE // 2, TILE)
    degrees_of(cnt, hits.astype(BF16), meta[1:2, 0:slots])
    shared = 2 * SIDE
    core_cnt = w.start(cnt.at[pl.ds((1 - e) * shared, shared)], got_core, other)

    combine(2)
    direct(1)
    direct(-1)
    core_cnt.wait_recv()
    chip_cnt[...] = cnt[pl.ds(e * shared, shared)] + got_core[...]
    cnt1 = [
        w.start(chip_cnt.at[h * SIDE + step(p1[h], by)], got_cnt.at[h, k], ring1[h](by))
        for h in range(2)
        for k, by in enumerate((1, -1, 2))
    ]
    combine(1)
    combine(-1)
    direct(0)

    near2 = []
    for h in range(2):
        small[h, 0] = finished(h, 2).astype(BF16)
        near2.append(w.start(small.at[h, 0], final2.at[h, 0], ring2[h](2)))
    combine(0)
    for copy in cnt1:
        copy.wait_recv()
    for h in range(2):
        ring_cnt[h] = chip_cnt[h * SIDE + step(p1[h], 0)] + got_cnt[h, 0] + got_cnt[h, 1] + got_cnt[h, 2]
    cnt2 = [
        w.start(ring_cnt.at[h], got_cnt2.at[h, k], ring2[h](by)) for h in range(2) for k, by in enumerate((1, -1, 2))
    ]
    for h in range(2):
        small[h, 1] = finished(h, 1).astype(BF16)
        near2.append(w.start(small.at[h, 1], final2.at[h, 1], ring2[h](1)))
        small[h, 2] = finished(h, -1).astype(BF16)
        near2.append(w.start(small.at[h, 2], final2.at[h, 2], ring2[h](-1)))
    for h in range(2):
        total[h] = finished(h, 0)

    for copy in own_copies:
        copy.wait()
    for copy in cnt2:
        copy.wait_recv()
    own_diag = lax.broadcasted_iota(jnp.int32, (seg, TILE), 0) == lax.broadcasted_iota(jnp.int32, (seg, TILE), 1)
    degrees = []
    for h in range(2):
        counts = ring_cnt[h] + got_cnt2[h, 0] + got_cnt2[h, 1] + got_cnt2[h, 2]
        own_row = lax.broadcasted_iota(jnp.int32, counts.shape, 0) == p2[h]
        degree = jnp.sum(jnp.where(own_row, counts, 0.0), axis=0, keepdims=True)
        degree = jnp.sum(jnp.where(own_diag, jnp.broadcast_to(degree, (seg, TILE)), 0.0), axis=1, keepdims=True)
        degrees.append(jnp.maximum(degree, 1.0))
    for copy in near2:
        copy.wait_recv()
    for h in range(2):
        summed = total[h] + up(final2[h, 0]) + up(final2[h, 1]) + up(final2[h, 2])
        average = (summed / degrees[h]).astype(BF16)
        v = jnp.dot(average, weight[...], preferred_element_type=F32)
        fresh = up(own_rows[h]) + v / (1.0 + jnp.exp(-v))
        users[rows_at(seg_at(h, 0, 0), seg, seg), :] = fresh.astype(BF16)

    def send(h, k1, k2, start, size, device):
        there = users.at[rows_at(seg_at(h, k1, k2) + start, size, half2)]
        return w.start(there, there, device)

    c1, c2, c2f = {}, {}, {}

    def spread(h, k2):
        for s in (1, -1):
            c2[h, k2, s] = send(h, 0, k2, 0, seg, ring1[h](s))
        if k2 == 2:
            c2f[h, k2, 0] = send(h, 0, k2, 0, seg, ring1[h](2))

    def relay(h, k2):
        c2[h, k2, 1].wait_recv()
        c2f[h, k2, 1] = send(h, -1, k2, 0, half2, ring1[h](1))
        c2[h, k2, -1].wait_recv()
        c2f[h, k2, -1] = send(h, 1, k2, half2, half2, ring1[h](-1))

    for h in range(2):
        for s in (1, -1, 2):
            c1[h, s] = send(h, 0, 0, 0, seg, ring2[h](s))
    for h in range(2):
        spread(h, 0)
    for h in range(2):
        for s in (1, -1):
            c1[h, s].wait_recv()
            spread(h, -s)
    for h in range(2):
        c1[h, 2].wait_recv()
        spread(h, 2)
    for k2 in (0, -1, 1):
        for h in range(2):
            relay(h, k2)
    for h in range(2):
        for s in (1, -1):
            c2[h, 2, s].wait_recv()
    for copy in c2f.values():
        copy.wait_recv()
    w.finish()
    assert len(w.made) == PLANE_COPIES, len(w.made)


DEPTH = 8
PARTS = 4
COLUMN_COPIES = 8 + 7 * PARTS + 8


def column_kernel(
    part, hits, items, up_weight, down_weight, out, to_core, from_core, sums, got_up, got_down, chip_hits, got_hits, own_rows, arrived,
    up_v, down_v, local_sem, send_sem, recv_sem,
):
    u, e = lax.axis_index("user"), lax.axis_index("edge")
    share = out.shape[0]
    half = share // PARTS

    def step(by):
        return lax.rem(u + (by + DEPTH), DEPTH)

    other = {"edge": 1 - e}
    place = {1: {"user": step(1)}, -1: {"user": step(-1)}}

    peers = [place[1], place[-1], other]
    greet(peers)

    def chunk(k, core):
        return (step(k) * 2 + core) * share

    local = [
        pltpu.make_async_copy(items.at[rows_at(chunk(0, e), share, share)], own_rows, local_sem.at[0]),
        pltpu.make_async_copy(up_weight, up_v, local_sem.at[1]),
        pltpu.make_async_copy(down_weight, down_v, local_sem.at[2]),
    ]
    for copy in local:
        copy.start()
    for k in (4, 3, -3, 2, -2, 1, -1, 0):
        to_core[k % DEPTH] = part[rows_at(chunk(k, 1 - e), share, share), :].astype(BF16)
    meet(peers)
    w = Wires(send_sem, recv_sem)
    core = {}
    for k in (4, 3, -3, 2, -2, 1, -1, 0):
        core[k] = w.start(to_core.at[k % DEPTH], from_core.at[k % DEPTH], other)
    core_hits = w.start(hits, got_hits.at[0], other)

    def mine(k, q):
        return part[rows_at(chunk(k, e) + q * half, half, half), :] + up(from_core[k % DEPTH, pl.ds(q * half, half), :])

    got = {1: got_up, -1: got_down}
    wires = {}
    hit_wires = {}

    landed = set()

    def land(k):
        if k not in landed:
            landed.add(k)
            core[k].wait_recv()

    def pass_on(s, k, q):
        land(4 if k == 4 else s * k)
        value = mine(s * k, q)
        if (s, k + 1, q) in wires:
            wires[s, k + 1, q].wait_recv()
            value += up(got[s][k, q])
        running = (s * k) % DEPTH, pl.ds(q * half, half)
        sums[running] = value.astype(BF16)
        wires[s, k, q] = w.start(sums.at[running], got[s].at[k - 1, q], place[s])

    first = [(s, j if s == 1 else PARTS // 2 + j) for j in range(PARTS // 2) for s in (1, -1)]
    second = [(s, PARTS // 2 + j if s == 1 else j) for j in range(PARTS // 2) for s in (1, -1)]
    for s, q in first:
        pass_on(s, 4, q)
    for s, q in second:
        pass_on(s, 3, q)
    core_hits.wait_recv()
    chip_hits[...] = hits[...] + got_hits[0]
    for s in (1, -1):
        hit_wires[s, 1] = w.start(chip_hits, got_hits.at[1 if s == 1 else 5], place[s])
    for k in (3, 2, 1):
        for s, q in first:
            pass_on(s, k, q)
        far = 5 - k
        for s in (1, -1):
            hit_wires[s, far - 1].wait_recv()
            if s == 1 or far < 4:
                base = 1 if s == 1 else 5
                hit_wires[s, far] = w.start(got_hits.at[base + far - 2], got_hits.at[base + far - 1], place[s])
        if k > 1:
            for s, q in second:
                pass_on(s, k - 1, q)
    hit_wires[1, 4].wait_recv()
    land(0)
    degree = chip_hits[...]
    for k in range(1, DEPTH):
        degree += got_hits[k]
    lane = lax.broadcasted_iota(jnp.int32, degree.shape, 1)
    for copy in local:
        copy.wait()
    tile = lax.div(lax.broadcasted_iota(jnp.int32, (share, 1), 0), TILE)
    own = [jnp.sum(jnp.where(lane == (u * 2 + e) * 2 + k, degree, 0.0)[0:1, :], axis=1, keepdims=True) for k in range(2)]
    own_degree = jnp.maximum(jnp.where(tile == 0, own[0], own[1]), 1.0)
    for q in range(PARTS):
        wires[1, 1, q].wait_recv()
        wires[-1, 1, q].wait_recv()
    summed = part[rows_at(chunk(0, e), share, share), :] + up(from_core[0])
    for q in range(PARTS):
        rows = pl.ds(q * half, half)
        arrived[rows, :] = up(got_up[0, q]) + up(got_down[0, q])
    merged = up(own_rows[...]) + (summed + arrived[...]) / own_degree
    v = jnp.dot(merged.astype(BF16), up_v[...], preferred_element_type=F32)
    hidden = (v / (1.0 + jnp.exp(-v))).astype(BF16)
    out[...] = (merged + jnp.dot(hidden, down_v[...], preferred_element_type=F32)).astype(BF16)
    w.finish()
    assert len(w.made) <= COLUMN_COPIES, len(w.made)


def vmem():
    return pl.BlockSpec(memory_space=VM)


def smem():
    return pl.BlockSpec(memory_space=pltpu.SMEM)


def hbm():
    return pl.BlockSpec(memory_space=pltpu.HBM)


MIB = 2**20


def swap(bi, bu, count, links, items, half_tiles):
    slots = links.shape[0]
    assert items.shape[0] == ITEM_TILES * TILE and 2 * slots <= SLOTS
    return pl.pallas_call(
        functools.partial(swap_kernel, half_tiles),
        out_shape=(
            jax.ShapeDtypeStruct((16, TILE), jnp.int32),
            jax.ShapeDtypeStruct((2 * slots, TILE), jnp.int32),
            jax.ShapeDtypeStruct((slots, TILE), F32),
            jax.ShapeDtypeStruct((8, TILE), F32),
            jax.ShapeDtypeStruct(items.shape, BF16),
        ),
        in_specs=[hbm()] * 5,
        out_specs=(vmem(),) * 5,
        scratch_shapes=[
            VM((1, slots), jnp.int32),
            VM((1, slots), jnp.int32),
            pltpu.SMEM((1,), jnp.int32),
            VM((8, TILE), jnp.int32),
            pltpu.SemaphoreType.DMA((5,)),
            pltpu.SemaphoreType.DMA((2,)),
            pltpu.SemaphoreType.DMA((2,)),
        ],
        compiler_params=pltpu.CompilerParams(collective_id=2, has_side_effects=True, vmem_limit_bytes=16 * MIB),
        name="swap",
    )(bi, bu, count, links, items)


def hop(from_items, meta, links, source, rows):
    slots = links.shape[0]
    return pl.pallas_call(
        functools.partial(hop_kernel, from_items),
        out_shape=jax.ShapeDtypeStruct((rows, source.shape[1]), F32),
        in_specs=[vmem()] * 3,
        out_specs=vmem(),
        scratch_shapes=[
            pltpu.SMEM(meta.shape, jnp.int32),
            pltpu.SMEM((slots + GROUP,), jnp.int32),
            pltpu.SemaphoreType.DMA((1,)),
        ],
        compiler_params=pltpu.CompilerParams(vmem_limit_bytes=24 * MIB),
        name="hop1" if from_items else "hop2",
    )(meta, links, source)


def plane(part, meta, links, found, emb, weight):
    rows, channels = part.shape
    seg = rows // (2 * SIDE * SIDE)
    pieces = 4 * SIDE
    return pl.pallas_call(
        plane_kernel,
        out_shape=jax.ShapeDtypeStruct((rows, channels), BF16),
        in_specs=[vmem()] * 4 + [hbm()] * 2,
        out_specs=vmem(),
        scratch_shapes=[
            VM((2, SIDE, SIDE, seg, channels), BF16),
            VM((2, 2, SIDE, seg // 2, channels), BF16),
            VM((2, 2, SIDE, seg, channels), BF16),
            VM((2, seg, channels), F32),
            VM((2, 3, seg, channels), BF16),
            VM((2, 3, seg, channels), BF16),
            VM((pieces, 8, TILE), F32),
            VM((pieces // 2, 8, TILE), F32),
            VM((pieces // 2, 8, TILE), F32),
            VM((2, 3, 8, TILE), F32),
            VM((2, 8, TILE), F32),
            VM((2, 3, 8, TILE), F32),
            VM((2, seg, channels), BF16),
            VM(weight.shape, BF16),
            pltpu.SemaphoreType.DMA((3,)),
            pltpu.SemaphoreType.DMA((PLANE_COPIES,)),
            pltpu.SemaphoreType.DMA((PLANE_COPIES,)),
        ],
        compiler_params=pltpu.CompilerParams(collective_id=0, has_side_effects=True, vmem_limit_bytes=32 * MIB),
        name="plane",
    )(part, meta, links, found, emb, weight)


def column(part, hits, items, up_weight, down_weight):
    rows, channels = part.shape
    share = rows // (2 * DEPTH)
    return pl.pallas_call(
        column_kernel,
        out_shape=jax.ShapeDtypeStruct((share, channels), BF16),
        in_specs=[vmem(), vmem(), hbm(), hbm(), hbm()],
        out_specs=vmem(),
        scratch_shapes=[
            VM((DEPTH, share, channels), BF16),
            VM((DEPTH, share, channels), BF16),
            VM((DEPTH, share, channels), BF16),
            VM((4, PARTS, share // PARTS, channels), BF16),
            VM((4, PARTS, share // PARTS, channels), BF16),
            VM(hits.shape, F32),
            VM((DEPTH,) + hits.shape, F32),
            VM((share, channels), BF16),
            VM((share, channels), F32),
            VM(up_weight.shape, BF16),
            VM(down_weight.shape, BF16),
            pltpu.SemaphoreType.DMA((3,)),
            pltpu.SemaphoreType.DMA((COLUMN_COPIES,)),
            pltpu.SemaphoreType.DMA((COLUMN_COPIES,)),
        ],
        compiler_params=pltpu.CompilerParams(collective_id=1, has_side_effects=True, vmem_limit_bytes=40 * MIB),
        name="column",
    )(part, hits, items, up_weight, down_weight)


def pin(*xs):
    return [pltpu.with_memory_space_constraint(x, pltpu.HBM) for x in xs]


def body(item_emb, user_emb, block_item, block_user, block_rows, block_count, user_weight, up_weight, down_weight):
    bi, bu, count = block_item.reshape(1, -1), block_user.reshape(1, -1), block_count.reshape(-1)
    links = block_rows.reshape(-1, TILE)
    bi, bu, links, item_emb, user_emb, user_weight, up_weight, down_weight = pin(
        bi, bu, links, item_emb, user_emb, user_weight, up_weight, down_weight
    )
    half_rows = user_emb.shape[0] // 2
    meta, links, found, hits, items = swap(bi, bu, count, links, item_emb, half_rows // TILE)
    user_part = hop(True, meta, links, items, half_rows)
    users = plane(user_part, meta, links, found, user_emb, user_weight)
    item_part = hop(False, meta, links, users, item_emb.shape[0])
    return column(item_part, hits, item_emb, up_weight, down_weight)


def solution(mesh):
    return jax.shard_map(
        body,
        mesh=mesh,
        in_specs=(
            P("item", None),
            P("user", None),
            P("item", "user", "edge", None),
            P("item", "user", "edge", None),
            P("item", "user", "edge", None, None),
            P("item", "user", "edge"),
            P(),
            P(),
            P(),
        ),
        out_specs=P(("item", "user", "edge"), None),
        check_vma=False,
    )
```

```python
import functools

import jax
import jax.numpy as jnp
from jax import lax
from jax.experimental import pallas as pl
from jax.experimental.pallas import tpu as pltpu
from jax.sharding import PartitionSpec as P

TILE = 128
MESH = pl.DeviceIdType.MESH
F32 = jnp.float32
BF16 = jnp.bfloat16
GROUP = 28
NOWHERE = 2**10
ITEM_TILES = 32
SLOTS = 256
VM = pltpu.VMEM


def rows_at(offset, count, unit):
    return pl.ds(pl.multiple_of(offset, unit), count)


def fetch(pairs, sems):
    copies = [pltpu.make_async_copy(src, dst, sems.at[at]) for at, (src, dst) in enumerate(pairs)]
    for copy in copies:
        copy.start()
    return copies


def swap_kernel(
    half_tiles, bi_hbm, bu_hbm, count_hbm, links_hbm, items_hbm, meta, links, found, hits, items, bi, bu, count, to_other,
    local_sem, send_sem, recv_sem,
):
    slots = links_hbm.shape[0]
    e = lax.axis_index("edge")
    other = {"edge": 1 - e}
    own = links.at[pl.ds(0, slots)]
    copies = fetch(
        [(bi_hbm, bi), (bu_hbm, bu), (count_hbm, count), (links_hbm, own), (items_hbm, items)], local_sem
    )
    greet([other])
    for copy in copies[:3]:
        copy.wait()
    slot = lax.broadcasted_iota(jnp.int32, (1, slots), 1)
    live = slot < count[0]

    def codes(core, first):
        ut = bu[...] - core * half_tiles
        code = (ut * ITEM_TILES + bi[...]) * SLOTS + slot + first
        return jnp.where(live & (ut >= 0) & (ut < half_tiles), code, -1)

    meta[0:1, 0:slots] = codes(e, 0)
    meta[1:2, 0:slots] = jnp.where(live, bu[...], NOWHERE)
    to_other[...] = jnp.zeros_like(to_other)
    to_other[0:1, 0:slots] = codes(1 - e, slots)
    meet([other])
    w = Wires(send_sem, recv_sem)
    copies[3].wait()
    w.start(own, links.at[pl.ds(slots, slots)], other)
    lane = lax.broadcasted_iota(jnp.int32, (slots, TILE), 1)
    found[...] = row_hits(links[pl.ds(0, slots), :], lane, 0, TILE // 4)
    w.start(to_other, meta.at[pl.ds(8, 8)], other)
    found[...] += row_hits(links[pl.ds(0, slots), :], lane, TILE // 4, TILE // 2)
    slot = lax.broadcasted_iota(jnp.int32, (TILE, slots), 1)
    tile = lax.broadcasted_iota(jnp.int32, (TILE, slots), 0)
    chosen = ((tile == bi[...]) & (slot < count[0])).astype(F32).astype(BF16)
    ones = jnp.ones((8, slots), BF16)
    hits[...] = lax.dot_general(ones, chosen, (((1,), (1,)), ((), ())), preferred_element_type=F32)
    copies[4].wait()
    for copy in w.made:
        copy.wait_recv()
    w.finish()


def row_hits(links, lane, first, last):
    found = jnp.zeros(lane.shape, F32)
    for r in range(first, last):
        found += (links[:, r : r + 1] == lane).astype(F32)
    return found


def hop_kernel(from_items, meta_ref, links, source, acc, meta, chosen, sem):
    slots = links.shape[0] // 2
    copy = fetch([(meta_ref, meta)], sem)[0]
    acc[...] = jnp.zeros_like(acc)
    copy.wait()
    each = 24

    def choose(g, n):
        for which in range(2):
            for j in range(each):
                code = meta[which * 8, g * each + j]
                chosen[n] = code
                n = n + 1 + lax.shift_right_arithmetic(code, 31)
        return n

    count = lax.fori_loop(0, slots // each, choose, 0)
    inside = lax.broadcasted_iota(jnp.int32, (TILE, TILE), 0)

    def blocks(group, carry):
        made = []
        for k in range(GROUP):
            b = group * GROUP + k
            live = b < count
            code = jnp.where(live, chosen[b], 0)
            it = jnp.bitwise_and(lax.shift_right_logical(code, 8), ITEM_TILES - 1) * TILE
            ut = lax.shift_right_logical(code, 13) * TILE
            src, dst = (it, ut) if from_items else (ut, it)
            row = jnp.where(live, links[pl.ds(jnp.bitwise_and(code, SLOTS - 1), 1), :], -1)
            onehot = (row == inside).astype(F32).astype(BF16)
            rows = source[rows_at(src, TILE, TILE), :]
            dims = (((1,), (0,)), ((), ())) if from_items else (((0,), (0,)), ((), ()))
            contrib = lax.dot_general(onehot, rows, dims, preferred_element_type=F32)
            made.append((dst, contrib))
        for at, contrib in made:
            acc[rows_at(at, TILE, TILE), :] += contrib
        return carry

    lax.fori_loop(0, (count + GROUP - 1) // GROUP, blocks, 0)


def degrees_of(cnt_ref, found, bu):
    slots = bu.shape[1]
    triples = cnt_ref.shape[0]
    which = lax.broadcasted_iota(jnp.int32, (triples, slots), 0) * 3
    a, b, c = (
        jnp.dot((which + k == bu).astype(F32).astype(BF16), found, preferred_element_type=F32) for k in range(3)
    )
    lanes = lax.broadcasted_iota(jnp.int32, (triples, TILE), 1)
    quarters = (
        a,
        jnp.where(lanes < 32, pltpu.roll(a, 32, 1), pltpu.roll(b, 32, 1)),
        jnp.where(lanes < 64, pltpu.roll(b, 64, 1), pltpu.roll(c, 64, 1)),
        pltpu.roll(c, 96, 1),
    )
    for j in range(triples):
        for q, counts in enumerate(quarters):
            cnt_ref[j, q : q + 1, :] = counts[j : j + 1, :]


class Wires:
    def __init__(self, send_sem, recv_sem):
        self.send_sem, self.recv_sem, self.made = send_sem, recv_sem, []

    def start(self, src, dst, device):
        at = len(self.made)
        copy = pltpu.make_async_remote_copy(
            src_ref=src,
            dst_ref=dst,
            send_sem=self.send_sem.at[at],
            recv_sem=self.recv_sem.at[at],
            device_id=device,
            device_id_type=MESH,
        )
        copy.start()
        self.made.append(copy)
        return copy

    def finish(self):
        for copy in self.made:
            copy.wait_send()


def greet(peers):
    for peer in peers:
        pl.semaphore_signal(pltpu.get_barrier_semaphore(), inc=1, device_id=peer, device_id_type=MESH)


def meet(peers):
    pl.semaphore_wait(pltpu.get_barrier_semaphore(), len(peers))


def up(x):
    return x.astype(F32)


SIDE = 4
PLANE_COPIES = 103


def plane_kernel(
    part, meta, links, found, emb, weight_hbm, users, sums, opposite, final, total, small, final2, cnt, got_core, chip_cnt,
    got_cnt, ring_cnt, got_cnt2, own_rows, weight, local_sem, send_sem, recv_sem,
):
    item, e = lax.axis_index("item"), lax.axis_index("edge")
    x, y = item // SIDE, item % SIDE
    seg = part.shape[0] // (2 * SIDE * SIDE)
    block = SIDE * seg
    half2 = seg // 2

    def step(value, by):
        return lax.rem(value + (by + SIDE), SIDE)

    def along_x(by):
        return {"item": step(x, by) * SIDE + y}

    def along_y(by):
        return {"item": x * SIDE + step(y, by)}

    other = {"edge": 1 - e}
    p1, p2 = (x, y), (y, x)
    ring1, ring2 = (along_x, along_y), (along_y, along_x)

    def block_at(h, k1):
        return (h * SIDE + step(p1[h], k1)) * block

    def seg_at(h, k1, k2):
        return block_at(h, k1) + step(p2[h], k2) * seg

    peers = [along_x(1), along_x(-1), along_x(2), along_y(1), along_y(-1), along_y(2), other]
    greet(peers)
    own_copies = fetch(
        [(emb.at[rows_at(e * part.shape[0] + seg_at(h, 0, 0), seg, seg)], own_rows.at[h]) for h in range(2)]
        + [(weight_hbm, weight)],
        local_sem,
    )

    def mine(h, k1, k2, start, size):
        return part[rows_at(seg_at(h, k1, k2) + start, size, half2), :]

    low, high = pl.ds(0, half2), pl.ds(half2, half2)
    order = (2, 1, -1, 0)
    for k2 in order:
        for h in range(2):
            sums[h, 2, k2 % SIDE] = mine(h, 2, k2, 0, seg).astype(BF16)
    cnt[...] = jnp.zeros_like(cnt)
    meet(peers)
    w = Wires(send_sem, recv_sem)

    far, near, passed = {}, {}, {}

    def direct(k2):
        at = k2 % SIDE
        for h in range(2):
            sums[h, 1, at, high] = mine(h, 1, k2, half2, half2).astype(BF16)
            near[h, k2, 1] = w.start(sums.at[h, 1, at, high], final.at[h, 0, at, high], ring1[h](1))
            sums[h, 3, at, low] = mine(h, -1, k2, 0, half2).astype(BF16)
            near[h, k2, -1] = w.start(sums.at[h, 3, at, low], final.at[h, 1, at, low], ring1[h](-1))

    def combine(k2):
        at = k2 % SIDE
        for h in range(2):
            far[h, k2, 1].wait_recv()
            sums[h, 1, at, low] = (mine(h, 1, k2, 0, half2) + up(opposite[h, 0, at])).astype(BF16)
            passed[h, k2, 1] = w.start(sums.at[h, 1, at, low], final.at[h, 0, at, low], ring1[h](1))
            far[h, k2, -1].wait_recv()
            sums[h, 3, at, high] = (mine(h, -1, k2, half2, half2) + up(opposite[h, 1, at])).astype(BF16)
            passed[h, k2, -1] = w.start(sums.at[h, 3, at, high], final.at[h, 1, at, high], ring1[h](-1))

    def finished(h, k2):
        for s in (1, -1):
            near[h, k2, s].wait_recv()
            passed[h, k2, s].wait_recv()
        at = k2 % SIDE
        return mine(h, 0, k2, 0, seg) + up(final[h, 0, at]) + up(final[h, 1, at])

    for k2 in order:
        at = k2 % SIDE
        for h in range(2):
            far[h, k2, 1] = w.start(sums.at[h, 2, at, low], opposite.at[h, 0, at], ring1[h](1))
            far[h, k2, -1] = w.start(sums.at[h, 2, at, high], opposite.at[h, 1, at], ring1[h](-1))
    direct(2)

    slots = found.shape[0]
    lane = lax.broadcasted_iota(jnp.int32, (slots, TILE), 1)
    hits = found[...] + row_hits(links[pl.ds(0, slots), :], lane, TILE // 2, TILE)
    degrees_of(cnt, hits.astype(BF16), meta[1:2, 0:slots])
    shared = 2 * SIDE
    core_cnt = w.start(cnt.at[pl.ds((1 - e) * shared, shared)], got_core, other)

    combine(2)
    direct(1)
    direct(-1)
    core_cnt.wait_recv()
    chip_cnt[...] = cnt[pl.ds(e * shared, shared)] + got_core[...]
    cnt1 = [
        w.start(chip_cnt.at[h * SIDE + step(p1[h], by)], got_cnt.at[h, k], ring1[h](by))
        for h in range(2)
        for k, by in enumerate((1, -1, 2))
    ]
    combine(1)
    combine(-1)
    direct(0)

    near2 = {0: [], 1: []}
    for h in range(2):
        small[h, 0] = finished(h, 2).astype(BF16)
        near2[h].append(w.start(small.at[h, 0], final2.at[h, 0], ring2[h](2)))
    combine(0)
    for copy in cnt1:
        copy.wait_recv()
    for h in range(2):
        ring_cnt[h] = chip_cnt[h * SIDE + step(p1[h], 0)] + got_cnt[h, 0] + got_cnt[h, 1] + got_cnt[h, 2]
    cnt2 = [
        w.start(ring_cnt.at[h], got_cnt2.at[h, k], ring2[h](by)) for h in range(2) for k, by in enumerate((1, -1, 2))
    ]
    for h in range(2):
        small[h, 1] = finished(h, 1).astype(BF16)
        near2[h].append(w.start(small.at[h, 1], final2.at[h, 1], ring2[h](1)))
        small[h, 2] = finished(h, -1).astype(BF16)
        near2[h].append(w.start(small.at[h, 2], final2.at[h, 2], ring2[h](-1)))
    for h in range(2):
        total[h] = finished(h, 0)

    for copy in own_copies:
        copy.wait()
    for copy in cnt2:
        copy.wait_recv()
    own_diag = lax.broadcasted_iota(jnp.int32, (seg, TILE), 0) == lax.broadcasted_iota(jnp.int32, (seg, TILE), 1)
    degrees = []
    for h in range(2):
        counts = ring_cnt[h] + got_cnt2[h, 0] + got_cnt2[h, 1] + got_cnt2[h, 2]
        own_row = lax.broadcasted_iota(jnp.int32, counts.shape, 0) == p2[h]
        degree = jnp.sum(jnp.where(own_row, counts, 0.0), axis=0, keepdims=True)
        degree = jnp.sum(jnp.where(own_diag, jnp.broadcast_to(degree, (seg, TILE)), 0.0), axis=1, keepdims=True)
        degrees.append(jnp.maximum(degree, 1.0))
    def send(h, k1, k2, start, size, device):
        there = users.at[rows_at(seg_at(h, k1, k2) + start, size, half2)]
        return w.start(there, there, device)

    c1, c2, c2f = {}, {}, {}

    def spread(h, k2):
        for s in (1, -1):
            c2[h, k2, s] = send(h, 0, k2, 0, seg, ring1[h](s))
        if k2 == 2:
            c2f[h, k2, 0] = send(h, 0, k2, 0, seg, ring1[h](2))

    def relay(h, k2):
        c2[h, k2, 1].wait_recv()
        c2f[h, k2, 1] = send(h, -1, k2, 0, half2, ring1[h](1))
        c2[h, k2, -1].wait_recv()
        c2f[h, k2, -1] = send(h, 1, k2, half2, half2, ring1[h](-1))

    for h in range(2):
        for copy in near2[h]:
            copy.wait_recv()
        summed = total[h] + up(final2[h, 0]) + up(final2[h, 1]) + up(final2[h, 2])
        average = (summed / degrees[h]).astype(BF16)
        v = jnp.dot(average, weight[...], preferred_element_type=F32)
        fresh = up(own_rows[h]) + v / (1.0 + jnp.exp(-v))
        users[rows_at(seg_at(h, 0, 0), seg, seg), :] = fresh.astype(BF16)
        for s in (1, -1, 2):
            c1[h, s] = send(h, 0, 0, 0, seg, ring2[h](s))
        spread(h, 0)
    for h in range(2):
        for s in (1, -1):
            c1[h, s].wait_recv()
            spread(h, -s)
    for h in range(2):
        c1[h, 2].wait_recv()
        spread(h, 2)
    for k2 in (0, -1, 1):
        for h in range(2):
            relay(h, k2)
    for h in range(2):
        for s in (1, -1):
            c2[h, 2, s].wait_recv()
    for copy in c2f.values():
        copy.wait_recv()
    w.finish()
    assert len(w.made) == PLANE_COPIES, len(w.made)


DEPTH = 8
PARTS = 4
COLUMN_COPIES = 8 + 7 * PARTS + 8


def column_kernel(
    part, hits, items, up_weight, down_weight, out, to_core, from_core, sums, got_up, got_down, chip_hits, got_hits, own_rows, arrived,
    up_v, down_v, local_sem, send_sem, recv_sem,
):
    u, e = lax.axis_index("user"), lax.axis_index("edge")
    share = out.shape[0]
    half = share // PARTS

    def step(by):
        return lax.rem(u + (by + DEPTH), DEPTH)

    other = {"edge": 1 - e}
    place = {1: {"user": step(1)}, -1: {"user": step(-1)}}

    peers = [place[1], place[-1], other]
    greet(peers)

    def chunk(k, core):
        return (step(k) * 2 + core) * share

    local = [
        pltpu.make_async_copy(items.at[rows_at(chunk(0, e), share, share)], own_rows, local_sem.at[0]),
        pltpu.make_async_copy(up_weight, up_v, local_sem.at[1]),
        pltpu.make_async_copy(down_weight, down_v, local_sem.at[2]),
    ]
    for copy in local:
        copy.start()
    for k in (4, 3, -3, 2, -2, 1, -1, 0):
        to_core[k % DEPTH] = part[rows_at(chunk(k, 1 - e), share, share), :].astype(BF16)
    meet(peers)
    w = Wires(send_sem, recv_sem)
    core = {}
    for k in (4, 3, -3, 2, -2, 1, -1, 0):
        core[k] = w.start(to_core.at[k % DEPTH], from_core.at[k % DEPTH], other)
    core_hits = w.start(hits, got_hits.at[0], other)

    def mine(k, q):
        return part[rows_at(chunk(k, e) + q * half, half, half), :] + up(from_core[k % DEPTH, pl.ds(q * half, half), :])

    got = {1: got_up, -1: got_down}
    wires = {}
    hit_wires = {}

    landed = set()

    def land(k):
        if k not in landed:
            landed.add(k)
            core[k].wait_recv()

    def pass_on(s, k, q):
        land(4 if k == 4 else s * k)
        value = mine(s * k, q)
        if (s, k + 1, q) in wires:
            wires[s, k + 1, q].wait_recv()
            value += up(got[s][k, q])
        running = (s * k) % DEPTH, pl.ds(q * half, half)
        sums[running] = value.astype(BF16)
        wires[s, k, q] = w.start(sums.at[running], got[s].at[k - 1, q], place[s])

    first = [(s, j if s == 1 else PARTS // 2 + j) for j in range(PARTS // 2) for s in (1, -1)]
    second = [(s, PARTS // 2 + j if s == 1 else j) for j in range(PARTS // 2) for s in (1, -1)]
    for s, q in first:
        pass_on(s, 4, q)
    for s, q in second:
        pass_on(s, 3, q)
    core_hits.wait_recv()
    chip_hits[...] = hits[...] + got_hits[0]
    for s in (1, -1):
        hit_wires[s, 1] = w.start(chip_hits, got_hits.at[1 if s == 1 else 5], place[s])
    for k in (3, 2, 1):
        for s, q in first:
            pass_on(s, k, q)
        far = 5 - k
        for s in (1, -1):
            hit_wires[s, far - 1].wait_recv()
            if s == 1 or far < 4:
                base = 1 if s == 1 else 5
                hit_wires[s, far] = w.start(got_hits.at[base + far - 2], got_hits.at[base + far - 1], place[s])
        if k > 1:
            for s, q in second:
                pass_on(s, k - 1, q)
    hit_wires[1, 4].wait_recv()
    land(0)
    degree = chip_hits[...]
    for k in range(1, DEPTH):
        degree += got_hits[k]
    lane = lax.broadcasted_iota(jnp.int32, degree.shape, 1)
    for copy in local:
        copy.wait()
    own = [jnp.sum(jnp.where(lane == (u * 2 + e) * 2 + k, degree, 0.0)[0:1, :], axis=1, keepdims=True) for k in range(2)]
    own = [jnp.maximum(count, 1.0) for count in own]
    for q in range(PARTS):
        arrived[pl.ds(q * half, half), :] = mine(0, q)
    for pair in ((0, PARTS // 2), (1, PARTS // 2 + 1)):
        merged = []
        for q in pair:
            wires[1, 1, q].wait_recv()
            wires[-1, 1, q].wait_recv()
            rows = pl.ds(q * half, half)
            summed = arrived[rows, :] + up(got_up[0, q]) + up(got_down[0, q])
            merged.append(up(own_rows[rows, :]) + summed / own[q * half // TILE])
        merged = jnp.concatenate(merged, axis=0)
        v = jnp.dot(merged.astype(BF16), up_v[...], preferred_element_type=F32)
        hidden = (v / (1.0 + jnp.exp(-v))).astype(BF16)
        fresh = (merged + jnp.dot(hidden, down_v[...], preferred_element_type=F32)).astype(BF16)
        for at, q in enumerate(pair):
            out[pl.ds(q * half, half), :] = fresh[at * half : (at + 1) * half]
    w.finish()
    assert len(w.made) <= COLUMN_COPIES, len(w.made)


def vmem():
    return pl.BlockSpec(memory_space=VM)


def smem():
    return pl.BlockSpec(memory_space=pltpu.SMEM)


def hbm():
    return pl.BlockSpec(memory_space=pltpu.HBM)


MIB = 2**20


def swap(bi, bu, count, links, items, half_tiles):
    slots = links.shape[0]
    assert items.shape[0] == ITEM_TILES * TILE and 2 * slots <= SLOTS
    return pl.pallas_call(
        functools.partial(swap_kernel, half_tiles),
        out_shape=(
            jax.ShapeDtypeStruct((16, TILE), jnp.int32),
            jax.ShapeDtypeStruct((2 * slots, TILE), jnp.int32),
            jax.ShapeDtypeStruct((slots, TILE), F32),
            jax.ShapeDtypeStruct((8, TILE), F32),
            jax.ShapeDtypeStruct(items.shape, BF16),
        ),
        in_specs=[hbm()] * 5,
        out_specs=(vmem(),) * 5,
        scratch_shapes=[
            VM((1, slots), jnp.int32),
            VM((1, slots), jnp.int32),
            pltpu.SMEM((1,), jnp.int32),
            VM((8, TILE), jnp.int32),
            pltpu.SemaphoreType.DMA((5,)),
            pltpu.SemaphoreType.DMA((2,)),
            pltpu.SemaphoreType.DMA((2,)),
        ],
        compiler_params=pltpu.CompilerParams(collective_id=2, has_side_effects=True, vmem_limit_bytes=16 * MIB),
        name="swap",
    )(bi, bu, count, links, items)


def hop(from_items, meta, links, source, rows):
    slots = links.shape[0]
    return pl.pallas_call(
        functools.partial(hop_kernel, from_items),
        out_shape=jax.ShapeDtypeStruct((rows, source.shape[1]), F32),
        in_specs=[vmem()] * 3,
        out_specs=vmem(),
        scratch_shapes=[
            pltpu.SMEM(meta.shape, jnp.int32),
            pltpu.SMEM((slots + GROUP,), jnp.int32),
            pltpu.SemaphoreType.DMA((1,)),
        ],
        compiler_params=pltpu.CompilerParams(vmem_limit_bytes=24 * MIB),
        name="hop1" if from_items else "hop2",
    )(meta, links, source)


def plane(part, meta, links, found, emb, weight):
    rows, channels = part.shape
    seg = rows // (2 * SIDE * SIDE)
    pieces = 4 * SIDE
    return pl.pallas_call(
        plane_kernel,
        out_shape=jax.ShapeDtypeStruct((rows, channels), BF16),
        in_specs=[vmem()] * 4 + [hbm()] * 2,
        out_specs=vmem(),
        scratch_shapes=[
            VM((2, SIDE, SIDE, seg, channels), BF16),
            VM((2, 2, SIDE, seg // 2, channels), BF16),
            VM((2, 2, SIDE, seg, channels), BF16),
            VM((2, seg, channels), F32),
            VM((2, 3, seg, channels), BF16),
            VM((2, 3, seg, channels), BF16),
            VM((pieces, 8, TILE), F32),
            VM((pieces // 2, 8, TILE), F32),
            VM((pieces // 2, 8, TILE), F32),
            VM((2, 3, 8, TILE), F32),
            VM((2, 8, TILE), F32),
            VM((2, 3, 8, TILE), F32),
            VM((2, seg, channels), BF16),
            VM(weight.shape, BF16),
            pltpu.SemaphoreType.DMA((3,)),
            pltpu.SemaphoreType.DMA((PLANE_COPIES,)),
            pltpu.SemaphoreType.DMA((PLANE_COPIES,)),
        ],
        compiler_params=pltpu.CompilerParams(collective_id=0, has_side_effects=True, vmem_limit_bytes=32 * MIB),
        name="plane",
    )(part, meta, links, found, emb, weight)


def column(part, hits, items, up_weight, down_weight):
    rows, channels = part.shape
    share = rows // (2 * DEPTH)
    return pl.pallas_call(
        column_kernel,
        out_shape=jax.ShapeDtypeStruct((share, channels), BF16),
        in_specs=[vmem(), vmem(), hbm(), hbm(), hbm()],
        out_specs=vmem(),
        scratch_shapes=[
            VM((DEPTH, share, channels), BF16),
            VM((DEPTH, share, channels), BF16),
            VM((DEPTH, share, channels), BF16),
            VM((4, PARTS, share // PARTS, channels), BF16),
            VM((4, PARTS, share // PARTS, channels), BF16),
            VM(hits.shape, F32),
            VM((DEPTH,) + hits.shape, F32),
            VM((share, channels), BF16),
            VM((share, channels), F32),
            VM(up_weight.shape, BF16),
            VM(down_weight.shape, BF16),
            pltpu.SemaphoreType.DMA((3,)),
            pltpu.SemaphoreType.DMA((COLUMN_COPIES,)),
            pltpu.SemaphoreType.DMA((COLUMN_COPIES,)),
        ],
        compiler_params=pltpu.CompilerParams(collective_id=1, has_side_effects=True, vmem_limit_bytes=40 * MIB),
        name="column",
    )(part, hits, items, up_weight, down_weight)


def pin(*xs):
    return [pltpu.with_memory_space_constraint(x, pltpu.HBM) for x in xs]


def body(item_emb, user_emb, block_item, block_user, block_rows, block_count, user_weight, up_weight, down_weight):
    bi, bu, count = block_item.reshape(1, -1), block_user.reshape(1, -1), block_count.reshape(-1)
    links = block_rows.reshape(-1, TILE)
    bi, bu, links, item_emb, user_emb, user_weight, up_weight, down_weight = pin(
        bi, bu, links, item_emb, user_emb, user_weight, up_weight, down_weight
    )
    half_rows = user_emb.shape[0] // 2
    meta, links, found, hits, items = swap(bi, bu, count, links, item_emb, half_rows // TILE)
    user_part = hop(True, meta, links, items, half_rows)
    users = plane(user_part, meta, links, found, user_emb, user_weight)
    item_part = hop(False, meta, links, users, item_emb.shape[0])
    return column(item_part, hits, item_emb, up_weight, down_weight)


def solution(mesh):
    return jax.shard_map(
        body,
        mesh=mesh,
        in_specs=(
            P("item", None),
            P("user", None),
            P("item", "user", "edge", None),
            P("item", "user", "edge", None),
            P("item", "user", "edge", None, None),
            P("item", "user", "edge"),
            P(),
            P(),
            P(),
        ),
        out_specs=P(("item", "user", "edge"), None),
        check_vma=False,
    )
```

```python
import functools

import jax
import jax.numpy as jnp
from jax import lax
from jax.experimental import pallas as pl
from jax.experimental.pallas import tpu as pltpu
from jax.sharding import PartitionSpec as P

TILE = 128
MESH = pl.DeviceIdType.MESH
F32 = jnp.float32
BF16 = jnp.bfloat16
GROUP = 28
NOWHERE = 2**10
ITEM_TILES = 32
SLOTS = 256
VM = pltpu.VMEM


def rows_at(offset, count, unit):
    return pl.ds(pl.multiple_of(offset, unit), count)


def fetch(pairs, sems):
    copies = [pltpu.make_async_copy(src, dst, sems.at[at]) for at, (src, dst) in enumerate(pairs)]
    for copy in copies:
        copy.start()
    return copies


def swap_kernel(
    half_tiles, bi_hbm, bu_hbm, count_hbm, links_hbm, items_hbm, meta, links, found, hits, items, bi, bu, count, to_other,
    local_sem, send_sem, recv_sem,
):
    slots = links_hbm.shape[0]
    e = lax.axis_index("edge")
    other = {"edge": 1 - e}
    own = links.at[pl.ds(0, slots)]
    copies = fetch(
        [(bi_hbm, bi), (bu_hbm, bu), (count_hbm, count), (links_hbm, own), (items_hbm, items)], local_sem
    )
    greet([other])
    for copy in copies[:3]:
        copy.wait()
    slot = lax.broadcasted_iota(jnp.int32, (1, slots), 1)
    live = slot < count[0]

    def codes(core, first):
        ut = bu[...] - core * half_tiles
        code = (ut * ITEM_TILES + bi[...]) * SLOTS + slot + first
        return jnp.where(live & (ut >= 0) & (ut < half_tiles), code, -1)

    meta[0:1, 0:slots] = codes(e, 0)
    meta[1:2, 0:slots] = jnp.where(live, bu[...], NOWHERE)
    to_other[...] = jnp.zeros_like(to_other)
    to_other[0:1, 0:slots] = codes(1 - e, slots)
    meet([other])
    w = Wires(send_sem, recv_sem)
    copies[3].wait()
    w.start(own, links.at[pl.ds(slots, slots)], other)
    lane = lax.broadcasted_iota(jnp.int32, (slots, TILE), 1)
    found[...] = row_hits(links[pl.ds(0, slots), :], lane, 0, TILE // 4)
    w.start(to_other, meta.at[pl.ds(8, 8)], other)
    found[...] += row_hits(links[pl.ds(0, slots), :], lane, TILE // 4, TILE // 2)
    slot = lax.broadcasted_iota(jnp.int32, (TILE, slots), 1)
    tile = lax.broadcasted_iota(jnp.int32, (TILE, slots), 0)
    chosen = ((tile == bi[...]) & (slot < count[0])).astype(F32).astype(BF16)
    ones = jnp.ones((8, slots), BF16)
    hits[...] = lax.dot_general(ones, chosen, (((1,), (1,)), ((), ())), preferred_element_type=F32)
    copies[4].wait()
    for copy in w.made:
        copy.wait_recv()
    w.finish()


def row_hits(links, lane, first, last):
    found = jnp.zeros(lane.shape, F32)
    for r in range(first, last):
        found += (links[:, r : r + 1] == lane).astype(F32)
    return found


def hop_kernel(from_items, meta_ref, links, source, acc, meta, chosen, sem):
    slots = links.shape[0] // 2
    copy = fetch([(meta_ref, meta)], sem)[0]
    acc[...] = jnp.zeros_like(acc)
    copy.wait()
    each = 24

    def choose(g, n):
        for which in range(2):
            for j in range(each):
                code = meta[which * 8, g * each + j]
                chosen[n] = code
                n = n + 1 + lax.shift_right_arithmetic(code, 31)
        return n

    count = lax.fori_loop(0, slots // each, choose, 0)
    inside = lax.broadcasted_iota(jnp.int32, (TILE, TILE), 0)

    def blocks(group, carry):
        made = []
        for k in range(GROUP):
            b = group * GROUP + k
            live = b < count
            code = jnp.where(live, chosen[b], 0)
            it = jnp.bitwise_and(lax.shift_right_logical(code, 8), ITEM_TILES - 1) * TILE
            ut = lax.shift_right_logical(code, 13) * TILE
            src, dst = (it, ut) if from_items else (ut, it)
            row = jnp.where(live, links[pl.ds(jnp.bitwise_and(code, SLOTS - 1), 1), :], -1)
            onehot = (row == inside).astype(F32).astype(BF16)
            rows = source[rows_at(src, TILE, TILE), :]
            dims = (((1,), (0,)), ((), ())) if from_items else (((0,), (0,)), ((), ()))
            contrib = lax.dot_general(onehot, rows, dims, preferred_element_type=F32)
            made.append((dst, contrib))
        for at, contrib in made:
            acc[rows_at(at, TILE, TILE), :] += contrib
        return carry

    lax.fori_loop(0, (count + GROUP - 1) // GROUP, blocks, 0)


def degrees_of(cnt_ref, found, bu):
    slots = bu.shape[1]
    triples = cnt_ref.shape[0]
    which = lax.broadcasted_iota(jnp.int32, (triples, slots), 0) * 3
    a, b, c = (
        jnp.dot((which + k == bu).astype(F32).astype(BF16), found, preferred_element_type=F32) for k in range(3)
    )
    lanes = lax.broadcasted_iota(jnp.int32, (triples, TILE), 1)
    quarters = (
        a,
        jnp.where(lanes < 32, pltpu.roll(a, 32, 1), pltpu.roll(b, 32, 1)),
        jnp.where(lanes < 64, pltpu.roll(b, 64, 1), pltpu.roll(c, 64, 1)),
        pltpu.roll(c, 96, 1),
    )
    for j in range(triples):
        for q, counts in enumerate(quarters):
            cnt_ref[j, q : q + 1, :] = counts[j : j + 1, :]


class Wires:
    def __init__(self, send_sem, recv_sem):
        self.send_sem, self.recv_sem, self.made = send_sem, recv_sem, []

    def start(self, src, dst, device):
        at = len(self.made)
        copy = pltpu.make_async_remote_copy(
            src_ref=src,
            dst_ref=dst,
            send_sem=self.send_sem.at[at],
            recv_sem=self.recv_sem.at[at],
            device_id=device,
            device_id_type=MESH,
        )
        copy.start()
        self.made.append(copy)
        return copy

    def finish(self):
        for copy in self.made:
            copy.wait_send()


def greet(peers):
    for peer in peers:
        pl.semaphore_signal(pltpu.get_barrier_semaphore(), inc=1, device_id=peer, device_id_type=MESH)


def meet(peers):
    pl.semaphore_wait(pltpu.get_barrier_semaphore(), len(peers))


def up(x):
    return x.astype(F32)


SIDE = 4
PLANE_COPIES = 103


def plane_kernel(
    part, meta, links, found, emb, weight_hbm, users, sums, opposite, final, total, small, final2, cnt, got_core, chip_cnt,
    got_cnt, ring_cnt, got_cnt2, own_rows, weight, local_sem, send_sem, recv_sem,
):
    item, e = lax.axis_index("item"), lax.axis_index("edge")
    x, y = item // SIDE, item % SIDE
    seg = part.shape[0] // (2 * SIDE * SIDE)
    block = SIDE * seg
    half2 = seg // 2

    def step(value, by):
        return lax.rem(value + (by + SIDE), SIDE)

    def along_x(by):
        return {"item": step(x, by) * SIDE + y}

    def along_y(by):
        return {"item": x * SIDE + step(y, by)}

    other = {"edge": 1 - e}
    p1, p2 = (x, y), (y, x)
    ring1, ring2 = (along_x, along_y), (along_y, along_x)

    def block_at(h, k1):
        return (h * SIDE + step(p1[h], k1)) * block

    def seg_at(h, k1, k2):
        return block_at(h, k1) + step(p2[h], k2) * seg

    peers = [along_x(1), along_x(-1), along_x(2), along_y(1), along_y(-1), along_y(2), other]
    greet(peers)
    own_copies = fetch(
        [(emb.at[rows_at(e * part.shape[0] + seg_at(h, 0, 0), seg, seg)], own_rows.at[h]) for h in range(2)]
        + [(weight_hbm, weight)],
        local_sem,
    )

    def mine(h, k1, k2, start, size):
        return part[rows_at(seg_at(h, k1, k2) + start, size, half2), :]

    low, high = pl.ds(0, half2), pl.ds(half2, half2)
    order = (2, 1, -1, 0)
    for h in range(2):
        sums[h, 2, 2] = mine(h, 2, 2, 0, seg).astype(BF16)
    meet(peers)
    w = Wires(send_sem, recv_sem)

    far, near, passed = {}, {}, {}

    def direct(k2):
        at = k2 % SIDE
        for h in range(2):
            sums[h, 1, at, high] = mine(h, 1, k2, half2, half2).astype(BF16)
            near[h, k2, 1] = w.start(sums.at[h, 1, at, high], final.at[h, 0, at, high], ring1[h](1))
            sums[h, 3, at, low] = mine(h, -1, k2, 0, half2).astype(BF16)
            near[h, k2, -1] = w.start(sums.at[h, 3, at, low], final.at[h, 1, at, low], ring1[h](-1))

    def combine(k2):
        at = k2 % SIDE
        for h in range(2):
            far[h, k2, 1].wait_recv()
            sums[h, 1, at, low] = (mine(h, 1, k2, 0, half2) + up(opposite[h, 0, at])).astype(BF16)
            passed[h, k2, 1] = w.start(sums.at[h, 1, at, low], final.at[h, 0, at, low], ring1[h](1))
            far[h, k2, -1].wait_recv()
            sums[h, 3, at, high] = (mine(h, -1, k2, half2, half2) + up(opposite[h, 1, at])).astype(BF16)
            passed[h, k2, -1] = w.start(sums.at[h, 3, at, high], final.at[h, 1, at, high], ring1[h](-1))

    def finished(h, k2):
        for s in (1, -1):
            near[h, k2, s].wait_recv()
            passed[h, k2, s].wait_recv()
        at = k2 % SIDE
        return mine(h, 0, k2, 0, seg) + up(final[h, 0, at]) + up(final[h, 1, at])

    for k2 in order:
        at = k2 % SIDE
        for h in range(2):
            if k2 != 2:
                sums[h, 2, at] = mine(h, 2, k2, 0, seg).astype(BF16)
            far[h, k2, 1] = w.start(sums.at[h, 2, at, low], opposite.at[h, 0, at], ring1[h](1))
            far[h, k2, -1] = w.start(sums.at[h, 2, at, high], opposite.at[h, 1, at], ring1[h](-1))
    direct(2)

    cnt[...] = jnp.zeros_like(cnt)
    slots = found.shape[0]
    lane = lax.broadcasted_iota(jnp.int32, (slots, TILE), 1)
    hits = found[...] + row_hits(links[pl.ds(0, slots), :], lane, TILE // 2, TILE)
    degrees_of(cnt, hits.astype(BF16), meta[1:2, 0:slots])
    shared = 2 * SIDE
    core_cnt = w.start(cnt.at[pl.ds((1 - e) * shared, shared)], got_core, other)

    combine(2)
    direct(1)
    direct(-1)
    core_cnt.wait_recv()
    chip_cnt[...] = cnt[pl.ds(e * shared, shared)] + got_core[...]
    cnt1 = [
        w.start(chip_cnt.at[h * SIDE + step(p1[h], by)], got_cnt.at[h, k], ring1[h](by))
        for h in range(2)
        for k, by in enumerate((1, -1, 2))
    ]
    combine(1)
    combine(-1)
    direct(0)

    near2 = {0: [], 1: []}
    for h in range(2):
        small[h, 0] = finished(h, 2).astype(BF16)
        near2[h].append(w.start(small.at[h, 0], final2.at[h, 0], ring2[h](2)))
    combine(0)
    for copy in cnt1:
        copy.wait_recv()
    for h in range(2):
        ring_cnt[h] = chip_cnt[h * SIDE + step(p1[h], 0)] + got_cnt[h, 0] + got_cnt[h, 1] + got_cnt[h, 2]
    cnt2 = [
        w.start(ring_cnt.at[h], got_cnt2.at[h, k], ring2[h](by)) for h in range(2) for k, by in enumerate((1, -1, 2))
    ]
    for h in range(2):
        small[h, 1] = finished(h, 1).astype(BF16)
        near2[h].append(w.start(small.at[h, 1], final2.at[h, 1], ring2[h](1)))
        small[h, 2] = finished(h, -1).astype(BF16)
        near2[h].append(w.start(small.at[h, 2], final2.at[h, 2], ring2[h](-1)))
    for h in range(2):
        total[h] = finished(h, 0)

    for copy in own_copies:
        copy.wait()
    for copy in cnt2:
        copy.wait_recv()
    own_diag = lax.broadcasted_iota(jnp.int32, (seg, TILE), 0) == lax.broadcasted_iota(jnp.int32, (seg, TILE), 1)
    degrees = []
    for h in range(2):
        counts = ring_cnt[h] + got_cnt2[h, 0] + got_cnt2[h, 1] + got_cnt2[h, 2]
        own_row = lax.broadcasted_iota(jnp.int32, counts.shape, 0) == p2[h]
        degree = jnp.sum(jnp.where(own_row, counts, 0.0), axis=0, keepdims=True)
        degree = jnp.sum(jnp.where(own_diag, jnp.broadcast_to(degree, (seg, TILE)), 0.0), axis=1, keepdims=True)
        degrees.append(jnp.maximum(degree, 1.0))
    def send(h, k1, k2, start, size, device):
        there = users.at[rows_at(seg_at(h, k1, k2) + start, size, half2)]
        return w.start(there, there, device)

    c1, c2, c2f = {}, {}, {}

    def spread(h, k2):
        for s in (1, -1):
            c2[h, k2, s] = send(h, 0, k2, 0, seg, ring1[h](s))
        if k2 == 2:
            c2f[h, k2, 0] = send(h, 0, k2, 0, seg, ring1[h](2))

    def relay(h, k2):
        c2[h, k2, 1].wait_recv()
        c2f[h, k2, 1] = send(h, -1, k2, 0, half2, ring1[h](1))
        c2[h, k2, -1].wait_recv()
        c2f[h, k2, -1] = send(h, 1, k2, half2, half2, ring1[h](-1))

    for h in range(2):
        for copy in near2[h]:
            copy.wait_recv()
        summed = total[h] + up(final2[h, 0]) + up(final2[h, 1]) + up(final2[h, 2])
        average = (summed / degrees[h]).astype(BF16)
        v = jnp.dot(average, weight[...], preferred_element_type=F32)
        fresh = up(own_rows[h]) + v / (1.0 + jnp.exp(-v))
        users[rows_at(seg_at(h, 0, 0), seg, seg), :] = fresh.astype(BF16)
        for s in (1, -1, 2):
            c1[h, s] = send(h, 0, 0, 0, seg, ring2[h](s))
        spread(h, 0)
    for h in range(2):
        for s in (1, -1):
            c1[h, s].wait_recv()
            spread(h, -s)
    for h in range(2):
        c1[h, 2].wait_recv()
        spread(h, 2)
    for k2 in (0, -1, 1):
        for h in range(2):
            relay(h, k2)
    for h in range(2):
        for s in (1, -1):
            c2[h, 2, s].wait_recv()
    for copy in c2f.values():
        copy.wait_recv()
    w.finish()
    assert len(w.made) == PLANE_COPIES, len(w.made)


DEPTH = 8
PARTS = 4
COLUMN_COPIES = 8 + 7 * PARTS + 8


def column_kernel(
    part, hits, items, up_weight, down_weight, out, to_core, from_core, sums, got_up, got_down, chip_hits, got_hits, own_rows, arrived,
    up_v, down_v, local_sem, send_sem, recv_sem,
):
    u, e = lax.axis_index("user"), lax.axis_index("edge")
    share = out.shape[0]
    half = share // PARTS

    def step(by):
        return lax.rem(u + (by + DEPTH), DEPTH)

    other = {"edge": 1 - e}
    place = {1: {"user": step(1)}, -1: {"user": step(-1)}}

    peers = [place[1], place[-1], other]
    greet(peers)

    def chunk(k, core):
        return (step(k) * 2 + core) * share

    local = [
        pltpu.make_async_copy(items.at[rows_at(chunk(0, e), share, share)], own_rows, local_sem.at[0]),
        pltpu.make_async_copy(up_weight, up_v, local_sem.at[1]),
        pltpu.make_async_copy(down_weight, down_v, local_sem.at[2]),
    ]
    for copy in local:
        copy.start()
    def round_off(k):
        to_core[k % DEPTH] = part[rows_at(chunk(k, 1 - e), share, share), :].astype(BF16)

    round_off(4)
    meet(peers)
    w = Wires(send_sem, recv_sem)
    core = {}
    for k in (4, 3, -3, 2, -2, 1, -1, 0):
        if k != 4:
            round_off(k)
        core[k] = w.start(to_core.at[k % DEPTH], from_core.at[k % DEPTH], other)
    core_hits = w.start(hits, got_hits.at[0], other)

    def mine(k, q):
        return part[rows_at(chunk(k, e) + q * half, half, half), :] + up(from_core[k % DEPTH, pl.ds(q * half, half), :])

    got = {1: got_up, -1: got_down}
    wires = {}
    hit_wires = {}

    landed = set()

    def land(k):
        if k not in landed:
            landed.add(k)
            core[k].wait_recv()

    def pass_on(s, k, q):
        land(4 if k == 4 else s * k)
        value = mine(s * k, q)
        if (s, k + 1, q) in wires:
            wires[s, k + 1, q].wait_recv()
            value += up(got[s][k, q])
        running = (s * k) % DEPTH, pl.ds(q * half, half)
        sums[running] = value.astype(BF16)
        wires[s, k, q] = w.start(sums.at[running], got[s].at[k - 1, q], place[s])

    first = [(s, j if s == 1 else PARTS // 2 + j) for j in range(PARTS // 2) for s in (1, -1)]
    second = [(s, PARTS // 2 + j if s == 1 else j) for j in range(PARTS // 2) for s in (1, -1)]
    for s, q in first:
        pass_on(s, 4, q)
    for s, q in second:
        pass_on(s, 3, q)
    core_hits.wait_recv()
    chip_hits[...] = hits[...] + got_hits[0]
    for s in (1, -1):
        hit_wires[s, 1] = w.start(chip_hits, got_hits.at[1 if s == 1 else 5], place[s])
    for k in (3, 2, 1):
        for s, q in first:
            pass_on(s, k, q)
        far = 5 - k
        for s in (1, -1):
            hit_wires[s, far - 1].wait_recv()
            if s == 1 or far < 4:
                base = 1 if s == 1 else 5
                hit_wires[s, far] = w.start(got_hits.at[base + far - 2], got_hits.at[base + far - 1], place[s])
        if k > 1:
            for s, q in second:
                pass_on(s, k - 1, q)
    hit_wires[1, 4].wait_recv()
    land(0)
    degree = chip_hits[...]
    for k in range(1, DEPTH):
        degree += got_hits[k]
    lane = lax.broadcasted_iota(jnp.int32, degree.shape, 1)
    for copy in local:
        copy.wait()
    own = [jnp.sum(jnp.where(lane == (u * 2 + e) * 2 + k, degree, 0.0)[0:1, :], axis=1, keepdims=True) for k in range(2)]
    own = [jnp.maximum(count, 1.0) for count in own]
    for q in range(PARTS):
        arrived[pl.ds(q * half, half), :] = mine(0, q)
    for pair in ((0, PARTS // 2), (1, PARTS // 2 + 1)):
        merged = []
        for q in pair:
            wires[1, 1, q].wait_recv()
            wires[-1, 1, q].wait_recv()
            rows = pl.ds(q * half, half)
            summed = arrived[rows, :] + up(got_up[0, q]) + up(got_down[0, q])
            merged.append(up(own_rows[rows, :]) + summed / own[q * half // TILE])
        merged = jnp.concatenate(merged, axis=0)
        v = jnp.dot(merged.astype(BF16), up_v[...], preferred_element_type=F32)
        hidden = (v / (1.0 + jnp.exp(-v))).astype(BF16)
        fresh = (merged + jnp.dot(hidden, down_v[...], preferred_element_type=F32)).astype(BF16)
        for at, q in enumerate(pair):
            out[pl.ds(q * half, half), :] = fresh[at * half : (at + 1) * half]
    w.finish()
    assert len(w.made) <= COLUMN_COPIES, len(w.made)


def vmem():
    return pl.BlockSpec(memory_space=VM)


def smem():
    return pl.BlockSpec(memory_space=pltpu.SMEM)


def hbm():
    return pl.BlockSpec(memory_space=pltpu.HBM)


MIB = 2**20


def swap(bi, bu, count, links, items, half_tiles):
    slots = links.shape[0]
    assert items.shape[0] == ITEM_TILES * TILE and 2 * slots <= SLOTS
    return pl.pallas_call(
        functools.partial(swap_kernel, half_tiles),
        out_shape=(
            jax.ShapeDtypeStruct((16, TILE), jnp.int32),
            jax.ShapeDtypeStruct((2 * slots, TILE), jnp.int32),
            jax.ShapeDtypeStruct((slots, TILE), F32),
            jax.ShapeDtypeStruct((8, TILE), F32),
            jax.ShapeDtypeStruct(items.shape, BF16),
        ),
        in_specs=[hbm()] * 5,
        out_specs=(vmem(),) * 5,
        scratch_shapes=[
            VM((1, slots), jnp.int32),
            VM((1, slots), jnp.int32),
            pltpu.SMEM((1,), jnp.int32),
            VM((8, TILE), jnp.int32),
            pltpu.SemaphoreType.DMA((5,)),
            pltpu.SemaphoreType.DMA((2,)),
            pltpu.SemaphoreType.DMA((2,)),
        ],
        compiler_params=pltpu.CompilerParams(collective_id=2, has_side_effects=True, vmem_limit_bytes=16 * MIB),
        name="swap",
    )(bi, bu, count, links, items)


def hop(from_items, meta, links, source, rows):
    slots = links.shape[0]
    return pl.pallas_call(
        functools.partial(hop_kernel, from_items),
        out_shape=jax.ShapeDtypeStruct((rows, source.shape[1]), F32),
        in_specs=[vmem()] * 3,
        out_specs=vmem(),
        scratch_shapes=[
            pltpu.SMEM(meta.shape, jnp.int32),
            pltpu.SMEM((slots + GROUP,), jnp.int32),
            pltpu.SemaphoreType.DMA((1,)),
        ],
        compiler_params=pltpu.CompilerParams(vmem_limit_bytes=24 * MIB),
        name="hop1" if from_items else "hop2",
    )(meta, links, source)


def plane(part, meta, links, found, emb, weight):
    rows, channels = part.shape
    seg = rows // (2 * SIDE * SIDE)
    pieces = 4 * SIDE
    return pl.pallas_call(
        plane_kernel,
        out_shape=jax.ShapeDtypeStruct((rows, channels), BF16),
        in_specs=[vmem()] * 4 + [hbm()] * 2,
        out_specs=vmem(),
        scratch_shapes=[
            VM((2, SIDE, SIDE, seg, channels), BF16),
            VM((2, 2, SIDE, seg // 2, channels), BF16),
            VM((2, 2, SIDE, seg, channels), BF16),
            VM((2, seg, channels), F32),
            VM((2, 3, seg, channels), BF16),
            VM((2, 3, seg, channels), BF16),
            VM((pieces, 8, TILE), F32),
            VM((pieces // 2, 8, TILE), F32),
            VM((pieces // 2, 8, TILE), F32),
            VM((2, 3, 8, TILE), F32),
            VM((2, 8, TILE), F32),
            VM((2, 3, 8, TILE), F32),
            VM((2, seg, channels), BF16),
            VM(weight.shape, BF16),
            pltpu.SemaphoreType.DMA((3,)),
            pltpu.SemaphoreType.DMA((PLANE_COPIES,)),
            pltpu.SemaphoreType.DMA((PLANE_COPIES,)),
        ],
        compiler_params=pltpu.CompilerParams(collective_id=0, has_side_effects=True, vmem_limit_bytes=32 * MIB),
        name="plane",
    )(part, meta, links, found, emb, weight)


def column(part, hits, items, up_weight, down_weight):
    rows, channels = part.shape
    share = rows // (2 * DEPTH)
    return pl.pallas_call(
        column_kernel,
        out_shape=jax.ShapeDtypeStruct((share, channels), BF16),
        in_specs=[vmem(), vmem(), hbm(), hbm(), hbm()],
        out_specs=vmem(),
        scratch_shapes=[
            VM((DEPTH, share, channels), BF16),
            VM((DEPTH, share, channels), BF16),
            VM((DEPTH, share, channels), BF16),
            VM((4, PARTS, share // PARTS, channels), BF16),
            VM((4, PARTS, share // PARTS, channels), BF16),
            VM(hits.shape, F32),
            VM((DEPTH,) + hits.shape, F32),
            VM((share, channels), BF16),
            VM((share, channels), F32),
            VM(up_weight.shape, BF16),
            VM(down_weight.shape, BF16),
            pltpu.SemaphoreType.DMA((3,)),
            pltpu.SemaphoreType.DMA((COLUMN_COPIES,)),
            pltpu.SemaphoreType.DMA((COLUMN_COPIES,)),
        ],
        compiler_params=pltpu.CompilerParams(collective_id=1, has_side_effects=True, vmem_limit_bytes=40 * MIB),
        name="column",
    )(part, hits, items, up_weight, down_weight)


def pin(*xs):
    return [pltpu.with_memory_space_constraint(x, pltpu.HBM) for x in xs]


def body(item_emb, user_emb, block_item, block_user, block_rows, block_count, user_weight, up_weight, down_weight):
    bi, bu, count = block_item.reshape(1, -1), block_user.reshape(1, -1), block_count.reshape(-1)
    links = block_rows.reshape(-1, TILE)
    bi, bu, links, item_emb, user_emb, user_weight, up_weight, down_weight = pin(
        bi, bu, links, item_emb, user_emb, user_weight, up_weight, down_weight
    )
    half_rows = user_emb.shape[0] // 2
    meta, links, found, hits, items = swap(bi, bu, count, links, item_emb, half_rows // TILE)
    user_part = hop(True, meta, links, items, half_rows)
    users = plane(user_part, meta, links, found, user_emb, user_weight)
    item_part = hop(False, meta, links, users, item_emb.shape[0])
    return column(item_part, hits, item_emb, up_weight, down_weight)


def solution(mesh):
    return jax.shard_map(
        body,
        mesh=mesh,
        in_specs=(
            P("item", None),
            P("user", None),
            P("item", "user", "edge", None),
            P("item", "user", "edge", None),
            P("item", "user", "edge", None, None),
            P("item", "user", "edge"),
            P(),
            P(),
            P(),
        ),
        out_specs=P(("item", "user", "edge"), None),
        check_vma=False,
    )
```

```python
import functools

import jax
import jax.numpy as jnp
from jax import lax
from jax.experimental import pallas as pl
from jax.experimental.pallas import tpu as pltpu
from jax.sharding import PartitionSpec as P

TILE = 128
MESH = pl.DeviceIdType.MESH
F32 = jnp.float32
BF16 = jnp.bfloat16
GROUP = 28
NOWHERE = 2**10
ITEM_TILES = 32
SLOTS = 256
VM = pltpu.VMEM


def rows_at(offset, count, unit):
    return pl.ds(pl.multiple_of(offset, unit), count)


def fetch(pairs, sems):
    copies = [pltpu.make_async_copy(src, dst, sems.at[at]) for at, (src, dst) in enumerate(pairs)]
    for copy in copies:
        copy.start()
    return copies


def swap_kernel(
    half_tiles, bi_hbm, bu_hbm, count_hbm, links_hbm, items_hbm, meta, links, found, hits, items, bi, bu, count, to_other,
    local_sem, send_sem, recv_sem,
):
    slots = links_hbm.shape[0]
    e = lax.axis_index("edge")
    other = {"edge": 1 - e}
    own = links.at[pl.ds(0, slots)]
    copies = fetch(
        [(bi_hbm, bi), (bu_hbm, bu), (count_hbm, count), (links_hbm, own), (items_hbm, items)], local_sem
    )
    greet([other])
    for copy in copies[:3]:
        copy.wait()
    slot = lax.broadcasted_iota(jnp.int32, (1, slots), 1)
    live = slot < count[0]

    def codes(core, first):
        ut = bu[...] - core * half_tiles
        code = (ut * ITEM_TILES + bi[...]) * SLOTS + slot + first
        return jnp.where(live & (ut >= 0) & (ut < half_tiles), code, -1)

    meta[0:1, 0:slots] = codes(e, 0)
    meta[1:2, 0:slots] = jnp.where(live, bu[...], NOWHERE)
    to_other[...] = jnp.zeros_like(to_other)
    to_other[0:1, 0:slots] = codes(1 - e, slots)
    copies[3].wait()
    meet([other])
    w = Wires(send_sem, recv_sem)
    w.start(own, links.at[pl.ds(slots, slots)], other)
    w.start(to_other, meta.at[pl.ds(8, 8)], other)
    lane = lax.broadcasted_iota(jnp.int32, (slots, TILE), 1)
    found[...] = row_hits(links[pl.ds(0, slots), :], lane, 0, TILE // 4)
    slot = lax.broadcasted_iota(jnp.int32, (TILE, slots), 1)
    tile = lax.broadcasted_iota(jnp.int32, (TILE, slots), 0)
    chosen = ((tile == bi[...]) & (slot < count[0])).astype(F32).astype(BF16)
    ones = jnp.ones((8, slots), BF16)
    hits[...] = lax.dot_general(ones, chosen, (((1,), (1,)), ((), ())), preferred_element_type=F32)
    copies[4].wait()
    for copy in w.made:
        copy.wait_recv()
    w.finish()


def row_hits(links, lane, first, last):
    found = jnp.zeros(lane.shape, F32)
    for r in range(first, last):
        found += (links[:, r : r + 1] == lane).astype(F32)
    return found


def hop_kernel(from_items, meta_ref, links, source, acc, meta, chosen, sem):
    slots = links.shape[0] // 2
    copy = fetch([(meta_ref, meta)], sem)[0]
    acc[...] = jnp.zeros_like(acc)
    copy.wait()
    each = 24

    def choose(g, n):
        for which in range(2):
            for j in range(each):
                code = meta[which * 8, g * each + j]
                chosen[n] = code
                n = n + 1 + lax.shift_right_arithmetic(code, 31)
        return n

    count = lax.fori_loop(0, slots // each, choose, 0)
    inside = lax.broadcasted_iota(jnp.int32, (TILE, TILE), 0)

    def blocks(group, carry):
        made = []
        for k in range(GROUP):
            b = group * GROUP + k
            live = b < count
            code = jnp.where(live, chosen[b], 0)
            it = jnp.bitwise_and(lax.shift_right_logical(code, 8), ITEM_TILES - 1) * TILE
            ut = lax.shift_right_logical(code, 13) * TILE
            src, dst = (it, ut) if from_items else (ut, it)
            row = jnp.where(live, links[pl.ds(jnp.bitwise_and(code, SLOTS - 1), 1), :], -1)
            onehot = (row == inside).astype(F32).astype(BF16)
            rows = source[rows_at(src, TILE, TILE), :]
            dims = (((1,), (0,)), ((), ())) if from_items else (((0,), (0,)), ((), ()))
            contrib = lax.dot_general(onehot, rows, dims, preferred_element_type=F32)
            made.append((dst, contrib))
        for at, contrib in made:
            acc[rows_at(at, TILE, TILE), :] += contrib
        return carry

    lax.fori_loop(0, (count + GROUP - 1) // GROUP, blocks, 0)


def degrees_of(cnt_ref, found, bu):
    slots = bu.shape[1]
    triples = cnt_ref.shape[0]
    which = lax.broadcasted_iota(jnp.int32, (triples, slots), 0) * 3
    a, b, c = (
        jnp.dot((which + k == bu).astype(F32).astype(BF16), found, preferred_element_type=F32) for k in range(3)
    )
    lanes = lax.broadcasted_iota(jnp.int32, (triples, TILE), 1)
    quarters = (
        a,
        jnp.where(lanes < 32, pltpu.roll(a, 32, 1), pltpu.roll(b, 32, 1)),
        jnp.where(lanes < 64, pltpu.roll(b, 64, 1), pltpu.roll(c, 64, 1)),
        pltpu.roll(c, 96, 1),
    )
    for j in range(triples):
        for q, counts in enumerate(quarters):
            cnt_ref[j, q : q + 1, :] = counts[j : j + 1, :]


class Wires:
    def __init__(self, send_sem, recv_sem):
        self.send_sem, self.recv_sem, self.made = send_sem, recv_sem, []

    def start(self, src, dst, device):
        at = len(self.made)
        copy = pltpu.make_async_remote_copy(
            src_ref=src,
            dst_ref=dst,
            send_sem=self.send_sem.at[at],
            recv_sem=self.recv_sem.at[at],
            device_id=device,
            device_id_type=MESH,
        )
        copy.start()
        self.made.append(copy)
        return copy

    def finish(self):
        for copy in self.made:
            copy.wait_send()


def greet(peers):
    for peer in peers:
        pl.semaphore_signal(pltpu.get_barrier_semaphore(), inc=1, device_id=peer, device_id_type=MESH)


def meet(peers):
    pl.semaphore_wait(pltpu.get_barrier_semaphore(), len(peers))


def up(x):
    return x.astype(F32)


SIDE = 4
PLANE_COPIES = 103


def plane_kernel(
    part, meta, links, found, emb, weight_hbm, users, sums, opposite, final, total, small, final2, cnt, got_core, chip_cnt,
    got_cnt, ring_cnt, got_cnt2, own_rows, weight, local_sem, send_sem, recv_sem,
):
    item, e = lax.axis_index("item"), lax.axis_index("edge")
    x, y = item // SIDE, item % SIDE
    seg = part.shape[0] // (2 * SIDE * SIDE)
    block = SIDE * seg
    half2 = seg // 2

    def step(value, by):
        return lax.rem(value + (by + SIDE), SIDE)

    def along_x(by):
        return {"item": step(x, by) * SIDE + y}

    def along_y(by):
        return {"item": x * SIDE + step(y, by)}

    other = {"edge": 1 - e}
    p1, p2 = (x, y), (y, x)
    ring1, ring2 = (along_x, along_y), (along_y, along_x)

    def block_at(h, k1):
        return (h * SIDE + step(p1[h], k1)) * block

    def seg_at(h, k1, k2):
        return block_at(h, k1) + step(p2[h], k2) * seg

    peers = [along_x(1), along_x(-1), along_x(2), along_y(1), along_y(-1), along_y(2), other]
    greet(peers)
    own_copies = fetch(
        [(emb.at[rows_at(e * part.shape[0] + seg_at(h, 0, 0), seg, seg)], own_rows.at[h]) for h in range(2)]
        + [(weight_hbm, weight)],
        local_sem,
    )

    def mine(h, k1, k2, start, size):
        return part[rows_at(seg_at(h, k1, k2) + start, size, half2), :]

    low, high = pl.ds(0, half2), pl.ds(half2, half2)
    order = (2, 1, -1, 0)
    for h in range(2):
        sums[h, 2, 2] = mine(h, 2, 2, 0, seg).astype(BF16)
    meet(peers)
    w = Wires(send_sem, recv_sem)

    far, near, passed = {}, {}, {}

    def direct(k2):
        at = k2 % SIDE
        for h in range(2):
            sums[h, 1, at, high] = mine(h, 1, k2, half2, half2).astype(BF16)
            near[h, k2, 1] = w.start(sums.at[h, 1, at, high], final.at[h, 0, at, high], ring1[h](1))
            sums[h, 3, at, low] = mine(h, -1, k2, 0, half2).astype(BF16)
            near[h, k2, -1] = w.start(sums.at[h, 3, at, low], final.at[h, 1, at, low], ring1[h](-1))

    def combine(k2):
        at = k2 % SIDE
        for h in range(2):
            far[h, k2, 1].wait_recv()
            sums[h, 1, at, low] = (mine(h, 1, k2, 0, half2) + up(opposite[h, 0, at])).astype(BF16)
            passed[h, k2, 1] = w.start(sums.at[h, 1, at, low], final.at[h, 0, at, low], ring1[h](1))
            far[h, k2, -1].wait_recv()
            sums[h, 3, at, high] = (mine(h, -1, k2, half2, half2) + up(opposite[h, 1, at])).astype(BF16)
            passed[h, k2, -1] = w.start(sums.at[h, 3, at, high], final.at[h, 1, at, high], ring1[h](-1))

    def finished(h, k2):
        for s in (1, -1):
            near[h, k2, s].wait_recv()
            passed[h, k2, s].wait_recv()
        at = k2 % SIDE
        return mine(h, 0, k2, 0, seg) + up(final[h, 0, at]) + up(final[h, 1, at])

    for k2 in order:
        at = k2 % SIDE
        for h in range(2):
            if k2 != 2:
                sums[h, 2, at] = mine(h, 2, k2, 0, seg).astype(BF16)
            far[h, k2, 1] = w.start(sums.at[h, 2, at, low], opposite.at[h, 0, at], ring1[h](1))
            far[h, k2, -1] = w.start(sums.at[h, 2, at, high], opposite.at[h, 1, at], ring1[h](-1))
    direct(2)

    cnt[...] = jnp.zeros_like(cnt)
    slots = found.shape[0]
    lane = lax.broadcasted_iota(jnp.int32, (slots, TILE), 1)
    hits = found[...] + row_hits(links[pl.ds(0, slots), :], lane, TILE // 4, TILE)
    degrees_of(cnt, hits.astype(BF16), meta[1:2, 0:slots])
    shared = 2 * SIDE
    core_cnt = w.start(cnt.at[pl.ds((1 - e) * shared, shared)], got_core, other)

    combine(2)
    direct(1)
    direct(-1)
    core_cnt.wait_recv()
    chip_cnt[...] = cnt[pl.ds(e * shared, shared)] + got_core[...]
    cnt1 = [
        w.start(chip_cnt.at[h * SIDE + step(p1[h], by)], got_cnt.at[h, k], ring1[h](by))
        for h in range(2)
        for k, by in enumerate((1, -1, 2))
    ]
    combine(1)
    combine(-1)
    direct(0)

    near2 = {0: [], 1: []}
    for h in range(2):
        small[h, 0] = finished(h, 2).astype(BF16)
        near2[h].append(w.start(small.at[h, 0], final2.at[h, 0], ring2[h](2)))
    combine(0)
    for copy in cnt1:
        copy.wait_recv()
    for h in range(2):
        ring_cnt[h] = chip_cnt[h * SIDE + step(p1[h], 0)] + got_cnt[h, 0] + got_cnt[h, 1] + got_cnt[h, 2]
    cnt2 = [
        w.start(ring_cnt.at[h], got_cnt2.at[h, k], ring2[h](by)) for h in range(2) for k, by in enumerate((1, -1, 2))
    ]
    for h in range(2):
        small[h, 1] = finished(h, 1).astype(BF16)
        near2[h].append(w.start(small.at[h, 1], final2.at[h, 1], ring2[h](1)))
        small[h, 2] = finished(h, -1).astype(BF16)
        near2[h].append(w.start(small.at[h, 2], final2.at[h, 2], ring2[h](-1)))
    for h in range(2):
        total[h] = finished(h, 0)

    for copy in own_copies:
        copy.wait()
    for copy in cnt2:
        copy.wait_recv()
    own_diag = lax.broadcasted_iota(jnp.int32, (seg, TILE), 0) == lax.broadcasted_iota(jnp.int32, (seg, TILE), 1)
    degrees = []
    for h in range(2):
        counts = ring_cnt[h] + got_cnt2[h, 0] + got_cnt2[h, 1] + got_cnt2[h, 2]
        own_row = lax.broadcasted_iota(jnp.int32, counts.shape, 0) == p2[h]
        degree = jnp.sum(jnp.where(own_row, counts, 0.0), axis=0, keepdims=True)
        degree = jnp.sum(jnp.where(own_diag, jnp.broadcast_to(degree, (seg, TILE)), 0.0), axis=1, keepdims=True)
        degrees.append(jnp.maximum(degree, 1.0))
    def send(h, k1, k2, start, size, device):
        there = users.at[rows_at(seg_at(h, k1, k2) + start, size, half2)]
        return w.start(there, there, device)

    c1, c2, c2f = {}, {}, {}

    def spread(h, k2):
        for s in (1, -1):
            c2[h, k2, s] = send(h, 0, k2, 0, seg, ring1[h](s))
        if k2 == 2:
            c2f[h, k2, 0] = send(h, 0, k2, 0, seg, ring1[h](2))

    def relay(h, k2):
        c2[h, k2, 1].wait_recv()
        c2f[h, k2, 1] = send(h, -1, k2, 0, half2, ring1[h](1))
        c2[h, k2, -1].wait_recv()
        c2f[h, k2, -1] = send(h, 1, k2, half2, half2, ring1[h](-1))

    for h in range(2):
        for copy in near2[h]:
            copy.wait_recv()
        summed = total[h] + up(final2[h, 0]) + up(final2[h, 1]) + up(final2[h, 2])
        average = (summed / degrees[h]).astype(BF16)
        v = jnp.dot(average, weight[...], preferred_element_type=F32)
        fresh = up(own_rows[h]) + v / (1.0 + jnp.exp(-v))
        users[rows_at(seg_at(h, 0, 0), seg, seg), :] = fresh.astype(BF16)
        for s in (1, -1, 2):
            c1[h, s] = send(h, 0, 0, 0, seg, ring2[h](s))
        spread(h, 0)
    for h in range(2):
        for s in (1, -1):
            c1[h, s].wait_recv()
            spread(h, -s)
    for h in range(2):
        c1[h, 2].wait_recv()
        spread(h, 2)
    for k2 in (0, -1, 1):
        for h in range(2):
            relay(h, k2)
    for h in range(2):
        for s in (1, -1):
            c2[h, 2, s].wait_recv()
    for copy in c2f.values():
        copy.wait_recv()
    w.finish()
    assert len(w.made) == PLANE_COPIES, len(w.made)


DEPTH = 8
PARTS = 4
COLUMN_COPIES = 8 + 7 * PARTS + 8


def column_kernel(
    part, hits, items, up_weight, down_weight, out, to_core, from_core, sums, got_up, got_down, chip_hits, got_hits, own_rows, arrived,
    up_v, down_v, local_sem, send_sem, recv_sem,
):
    u, e = lax.axis_index("user"), lax.axis_index("edge")
    share = out.shape[0]
    half = share // PARTS

    def step(by):
        return lax.rem(u + (by + DEPTH), DEPTH)

    other = {"edge": 1 - e}
    place = {1: {"user": step(1)}, -1: {"user": step(-1)}}

    peers = [place[1], place[-1], other]
    greet(peers)

    def chunk(k, core):
        return (step(k) * 2 + core) * share

    local = [
        pltpu.make_async_copy(items.at[rows_at(chunk(0, e), share, share)], own_rows, local_sem.at[0]),
        pltpu.make_async_copy(up_weight, up_v, local_sem.at[1]),
        pltpu.make_async_copy(down_weight, down_v, local_sem.at[2]),
    ]
    for copy in local:
        copy.start()
    def round_off(k):
        to_core[k % DEPTH] = part[rows_at(chunk(k, 1 - e), share, share), :].astype(BF16)

    round_off(4)
    meet(peers)
    w = Wires(send_sem, recv_sem)
    core = {}
    for k in (4, 3, -3, 2, -2, 1, -1, 0):
        if k != 4:
            round_off(k)
        core[k] = w.start(to_core.at[k % DEPTH], from_core.at[k % DEPTH], other)
    core_hits = w.start(hits, got_hits.at[0], other)

    def mine(k, q):
        return part[rows_at(chunk(k, e) + q * half, half, half), :] + up(from_core[k % DEPTH, pl.ds(q * half, half), :])

    got = {1: got_up, -1: got_down}
    wires = {}
    hit_wires = {}

    landed = set()

    def land(k):
        if k not in landed:
            landed.add(k)
            core[k].wait_recv()

    def pass_on(s, k, q):
        land(4 if k == 4 else s * k)
        value = mine(s * k, q)
        if (s, k + 1, q) in wires:
            wires[s, k + 1, q].wait_recv()
            value += up(got[s][k, q])
        running = (s * k) % DEPTH, pl.ds(q * half, half)
        sums[running] = value.astype(BF16)
        wires[s, k, q] = w.start(sums.at[running], got[s].at[k - 1, q], place[s])

    first = [(s, j if s == 1 else PARTS // 2 + j) for j in range(PARTS // 2) for s in (1, -1)]
    second = [(s, PARTS // 2 + j if s == 1 else j) for j in range(PARTS // 2) for s in (1, -1)]
    for s, q in first:
        pass_on(s, 4, q)
    for s, q in second:
        pass_on(s, 3, q)
    core_hits.wait_recv()
    chip_hits[...] = hits[...] + got_hits[0]
    for s in (1, -1):
        hit_wires[s, 1] = w.start(chip_hits, got_hits.at[1 if s == 1 else 5], place[s])
    for k in (3, 2, 1):
        for s, q in first:
            pass_on(s, k, q)
        far = 5 - k
        for s in (1, -1):
            hit_wires[s, far - 1].wait_recv()
            if s == 1 or far < 4:
                base = 1 if s == 1 else 5
                hit_wires[s, far] = w.start(got_hits.at[base + far - 2], got_hits.at[base + far - 1], place[s])
        if k > 1:
            for s, q in second:
                pass_on(s, k - 1, q)
    hit_wires[1, 4].wait_recv()
    land(0)
    degree = chip_hits[...]
    for k in range(1, DEPTH):
        degree += got_hits[k]
    lane = lax.broadcasted_iota(jnp.int32, degree.shape, 1)
    for copy in local:
        copy.wait()
    own = [jnp.sum(jnp.where(lane == (u * 2 + e) * 2 + k, degree, 0.0)[0:1, :], axis=1, keepdims=True) for k in range(2)]
    own = [jnp.maximum(count, 1.0) for count in own]
    for q in range(PARTS):
        arrived[pl.ds(q * half, half), :] = mine(0, q)
    for pair in ((0, PARTS // 2), (1, PARTS // 2 + 1)):
        merged = []
        for q in pair:
            wires[1, 1, q].wait_recv()
            wires[-1, 1, q].wait_recv()
            rows = pl.ds(q * half, half)
            summed = arrived[rows, :] + up(got_up[0, q]) + up(got_down[0, q])
            merged.append(up(own_rows[rows, :]) + summed / own[q * half // TILE])
        merged = jnp.concatenate(merged, axis=0)
        v = jnp.dot(merged.astype(BF16), up_v[...], preferred_element_type=F32)
        hidden = (v / (1.0 + jnp.exp(-v))).astype(BF16)
        fresh = (merged + jnp.dot(hidden, down_v[...], preferred_element_type=F32)).astype(BF16)
        for at, q in enumerate(pair):
            out[pl.ds(q * half, half), :] = fresh[at * half : (at + 1) * half]
    w.finish()
    assert len(w.made) <= COLUMN_COPIES, len(w.made)


def vmem():
    return pl.BlockSpec(memory_space=VM)


def smem():
    return pl.BlockSpec(memory_space=pltpu.SMEM)


def hbm():
    return pl.BlockSpec(memory_space=pltpu.HBM)


MIB = 2**20


def swap(bi, bu, count, links, items, half_tiles):
    slots = links.shape[0]
    assert items.shape[0] == ITEM_TILES * TILE and 2 * slots <= SLOTS
    return pl.pallas_call(
        functools.partial(swap_kernel, half_tiles),
        out_shape=(
            jax.ShapeDtypeStruct((16, TILE), jnp.int32),
            jax.ShapeDtypeStruct((2 * slots, TILE), jnp.int32),
            jax.ShapeDtypeStruct((slots, TILE), F32),
            jax.ShapeDtypeStruct((8, TILE), F32),
            jax.ShapeDtypeStruct(items.shape, BF16),
        ),
        in_specs=[hbm()] * 5,
        out_specs=(vmem(),) * 5,
        scratch_shapes=[
            VM((1, slots), jnp.int32),
            VM((1, slots), jnp.int32),
            pltpu.SMEM((1,), jnp.int32),
            VM((8, TILE), jnp.int32),
            pltpu.SemaphoreType.DMA((5,)),
            pltpu.SemaphoreType.DMA((2,)),
            pltpu.SemaphoreType.DMA((2,)),
        ],
        compiler_params=pltpu.CompilerParams(collective_id=2, has_side_effects=True, vmem_limit_bytes=16 * MIB),
        name="swap",
    )(bi, bu, count, links, items)


def hop(from_items, meta, links, source, rows):
    slots = links.shape[0]
    return pl.pallas_call(
        functools.partial(hop_kernel, from_items),
        out_shape=jax.ShapeDtypeStruct((rows, source.shape[1]), F32),
        in_specs=[vmem()] * 3,
        out_specs=vmem(),
        scratch_shapes=[
            pltpu.SMEM(meta.shape, jnp.int32),
            pltpu.SMEM((slots + GROUP,), jnp.int32),
            pltpu.SemaphoreType.DMA((1,)),
        ],
        compiler_params=pltpu.CompilerParams(vmem_limit_bytes=24 * MIB),
        name="hop1" if from_items else "hop2",
    )(meta, links, source)


def plane(part, meta, links, found, emb, weight):
    rows, channels = part.shape
    seg = rows // (2 * SIDE * SIDE)
    pieces = 4 * SIDE
    return pl.pallas_call(
        plane_kernel,
        out_shape=jax.ShapeDtypeStruct((rows, channels), BF16),
        in_specs=[vmem()] * 4 + [hbm()] * 2,
        out_specs=vmem(),
        scratch_shapes=[
            VM((2, SIDE, SIDE, seg, channels), BF16),
            VM((2, 2, SIDE, seg // 2, channels), BF16),
            VM((2, 2, SIDE, seg, channels), BF16),
            VM((2, seg, channels), F32),
            VM((2, 3, seg, channels), BF16),
            VM((2, 3, seg, channels), BF16),
            VM((pieces, 8, TILE), F32),
            VM((pieces // 2, 8, TILE), F32),
            VM((pieces // 2, 8, TILE), F32),
            VM((2, 3, 8, TILE), F32),
            VM((2, 8, TILE), F32),
            VM((2, 3, 8, TILE), F32),
            VM((2, seg, channels), BF16),
            VM(weight.shape, BF16),
            pltpu.SemaphoreType.DMA((3,)),
            pltpu.SemaphoreType.DMA((PLANE_COPIES,)),
            pltpu.SemaphoreType.DMA((PLANE_COPIES,)),
        ],
        compiler_params=pltpu.CompilerParams(collective_id=0, has_side_effects=True, vmem_limit_bytes=32 * MIB),
        name="plane",
    )(part, meta, links, found, emb, weight)


def column(part, hits, items, up_weight, down_weight):
    rows, channels = part.shape
    share = rows // (2 * DEPTH)
    return pl.pallas_call(
        column_kernel,
        out_shape=jax.ShapeDtypeStruct((share, channels), BF16),
        in_specs=[vmem(), vmem(), hbm(), hbm(), hbm()],
        out_specs=vmem(),
        scratch_shapes=[
            VM((DEPTH, share, channels), BF16),
            VM((DEPTH, share, channels), BF16),
            VM((DEPTH, share, channels), BF16),
            VM((4, PARTS, share // PARTS, channels), BF16),
            VM((4, PARTS, share // PARTS, channels), BF16),
            VM(hits.shape, F32),
            VM((DEPTH,) + hits.shape, F32),
            VM((share, channels), BF16),
            VM((share, channels), F32),
            VM(up_weight.shape, BF16),
            VM(down_weight.shape, BF16),
            pltpu.SemaphoreType.DMA((3,)),
            pltpu.SemaphoreType.DMA((COLUMN_COPIES,)),
            pltpu.SemaphoreType.DMA((COLUMN_COPIES,)),
        ],
        compiler_params=pltpu.CompilerParams(collective_id=1, has_side_effects=True, vmem_limit_bytes=40 * MIB),
        name="column",
    )(part, hits, items, up_weight, down_weight)


def pin(*xs):
    return [pltpu.with_memory_space_constraint(x, pltpu.HBM) for x in xs]


def body(item_emb, user_emb, block_item, block_user, block_rows, block_count, user_weight, up_weight, down_weight):
    bi, bu, count = block_item.reshape(1, -1), block_user.reshape(1, -1), block_count.reshape(-1)
    links = block_rows.reshape(-1, TILE)
    bi, bu, links, item_emb, user_emb, user_weight, up_weight, down_weight = pin(
        bi, bu, links, item_emb, user_emb, user_weight, up_weight, down_weight
    )
    half_rows = user_emb.shape[0] // 2
    meta, links, found, hits, items = swap(bi, bu, count, links, item_emb, half_rows // TILE)
    user_part = hop(True, meta, links, items, half_rows)
    users = plane(user_part, meta, links, found, user_emb, user_weight)
    item_part = hop(False, meta, links, users, item_emb.shape[0])
    return column(item_part, hits, item_emb, up_weight, down_weight)


def solution(mesh):
    return jax.shard_map(
        body,
        mesh=mesh,
        in_specs=(
            P("item", None),
            P("user", None),
            P("item", "user", "edge", None),
            P("item", "user", "edge", None),
            P("item", "user", "edge", None, None),
            P("item", "user", "edge"),
            P(),
            P(),
            P(),
        ),
        out_specs=P(("item", "user", "edge"), None),
        check_vma=False,
    )
```

```python
import functools

import jax
import jax.numpy as jnp
from jax import lax
from jax.experimental import pallas as pl
from jax.experimental.pallas import tpu as pltpu
from jax.sharding import PartitionSpec as P

TILE = 128
MESH = pl.DeviceIdType.MESH
F32 = jnp.float32
BF16 = jnp.bfloat16
GROUP = 28
NOWHERE = 2**10
ITEM_TILES = 32
SLOTS = 256
VM = pltpu.VMEM


def rows_at(offset, count, unit):
    return pl.ds(pl.multiple_of(offset, unit), count)


def fetch(pairs, sems):
    copies = [pltpu.make_async_copy(src, dst, sems.at[at]) for at, (src, dst) in enumerate(pairs)]
    for copy in copies:
        copy.start()
    return copies


def swap_kernel(
    half_tiles, bi_hbm, bu_hbm, count_hbm, links_hbm, items_hbm, meta, links, found, hits, items, bi, bu, count, to_other,
    local_sem, send_sem, recv_sem,
):
    slots = links_hbm.shape[0]
    e = lax.axis_index("edge")
    other = {"edge": 1 - e}
    own = links.at[pl.ds(0, slots)]
    copies = fetch(
        [(bi_hbm, bi), (bu_hbm, bu), (count_hbm, count), (links_hbm, own), (items_hbm, items)], local_sem
    )
    greet([other])
    for copy in copies[:3]:
        copy.wait()
    slot = lax.broadcasted_iota(jnp.int32, (1, slots), 1)
    live = slot < count[0]

    def codes(core, first):
        ut = bu[...] - core * half_tiles
        code = (ut * ITEM_TILES + bi[...]) * SLOTS + slot + first
        return jnp.where(live & (ut >= 0) & (ut < half_tiles), code, -1)

    meta[0:1, 0:slots] = codes(e, 0)
    meta[1:2, 0:slots] = jnp.where(live, bu[...], NOWHERE)
    to_other[...] = jnp.zeros_like(to_other)
    to_other[0:1, 0:slots] = codes(1 - e, slots)
    copies[3].wait()
    meet([other])
    w = Wires(send_sem, recv_sem)
    w.start(own, links.at[pl.ds(slots, slots)], other)
    w.start(to_other, meta.at[pl.ds(8, 8)], other)
    lane = lax.broadcasted_iota(jnp.int32, (slots, TILE), 1)
    found[...] = row_hits(links[pl.ds(0, slots), :], lane, 0, TILE // 4)
    slot = lax.broadcasted_iota(jnp.int32, (TILE, slots), 1)
    tile = lax.broadcasted_iota(jnp.int32, (TILE, slots), 0)
    chosen = ((tile == bi[...]) & (slot < count[0])).astype(F32).astype(BF16)
    ones = jnp.ones((8, slots), BF16)
    hits[...] = lax.dot_general(ones, chosen, (((1,), (1,)), ((), ())), preferred_element_type=F32)
    copies[4].wait()
    for copy in w.made:
        copy.wait_recv()
    w.finish()


def row_hits(links, lane, first, last):
    found = jnp.zeros(lane.shape, F32)
    for r in range(first, last):
        found += (links[:, r : r + 1] == lane).astype(F32)
    return found


def hop_kernel(from_items, meta_ref, links, source, acc, meta, chosen, sem):
    slots = links.shape[0] // 2
    copy = fetch([(meta_ref, meta)], sem)[0]
    acc[...] = jnp.zeros_like(acc)
    copy.wait()
    each = 24

    def choose(g, n):
        for which in range(2):
            for j in range(each):
                code = meta[which * 8, g * each + j]
                chosen[n] = code
                n = n + 1 + lax.shift_right_arithmetic(code, 31)
        return n

    count = lax.fori_loop(0, slots // each, choose, 0)
    inside = lax.broadcasted_iota(jnp.int32, (TILE, TILE), 0)

    def blocks(group, carry):
        made = []
        for k in range(GROUP):
            b = group * GROUP + k
            live = b < count
            code = jnp.where(live, chosen[b], 0)
            it = jnp.bitwise_and(lax.shift_right_logical(code, 8), ITEM_TILES - 1) * TILE
            ut = lax.shift_right_logical(code, 13) * TILE
            src, dst = (it, ut) if from_items else (ut, it)
            row = jnp.where(live, links[pl.ds(jnp.bitwise_and(code, SLOTS - 1), 1), :], -1)
            onehot = (row == inside).astype(F32).astype(BF16)
            rows = source[rows_at(src, TILE, TILE), :]
            dims = (((1,), (0,)), ((), ())) if from_items else (((0,), (0,)), ((), ()))
            contrib = lax.dot_general(onehot, rows, dims, preferred_element_type=F32)
            made.append((dst, contrib))
        for at, contrib in made:
            acc[rows_at(at, TILE, TILE), :] += contrib
        return carry

    lax.fori_loop(0, (count + GROUP - 1) // GROUP, blocks, 0)


def degrees_of(cnt_ref, found, bu):
    slots = bu.shape[1]
    triples = cnt_ref.shape[0]
    which = lax.broadcasted_iota(jnp.int32, (triples, slots), 0) * 3
    a, b, c = (
        jnp.dot((which + k == bu).astype(F32).astype(BF16), found, preferred_element_type=F32) for k in range(3)
    )
    lanes = lax.broadcasted_iota(jnp.int32, (triples, TILE), 1)
    quarters = (
        a,
        jnp.where(lanes < 32, pltpu.roll(a, 32, 1), pltpu.roll(b, 32, 1)),
        jnp.where(lanes < 64, pltpu.roll(b, 64, 1), pltpu.roll(c, 64, 1)),
        pltpu.roll(c, 96, 1),
    )
    for j in range(triples):
        for q, counts in enumerate(quarters):
            cnt_ref[j, q : q + 1, :] = counts[j : j + 1, :]


class Wires:
    def __init__(self, send_sem, recv_sem):
        self.send_sem, self.recv_sem, self.made = send_sem, recv_sem, []

    def start(self, src, dst, device):
        at = len(self.made)
        copy = pltpu.make_async_remote_copy(
            src_ref=src,
            dst_ref=dst,
            send_sem=self.send_sem.at[at],
            recv_sem=self.recv_sem.at[at],
            device_id=device,
            device_id_type=MESH,
        )
        copy.start()
        self.made.append(copy)
        return copy

    def finish(self):
        for copy in self.made:
            copy.wait_send()


def greet(peers):
    for peer in peers:
        pl.semaphore_signal(pltpu.get_barrier_semaphore(), inc=1, device_id=peer, device_id_type=MESH)


def meet(peers):
    pl.semaphore_wait(pltpu.get_barrier_semaphore(), len(peers))


def up(x):
    return x.astype(F32)


SIDE = 4
PLANE_COPIES = 103


def plane_kernel(
    part, meta, links, found, emb, weight_hbm, users, sums, opposite, final, total, small, final2, cnt, got_core, chip_cnt,
    got_cnt, ring_cnt, got_cnt2, own_rows, weight, local_sem, send_sem, recv_sem,
):
    item, e = lax.axis_index("item"), lax.axis_index("edge")
    x, y = item // SIDE, item % SIDE
    seg = part.shape[0] // (2 * SIDE * SIDE)
    block = SIDE * seg
    half2 = seg // 2

    def step(value, by):
        return lax.rem(value + (by + SIDE), SIDE)

    def along_x(by):
        return {"item": step(x, by) * SIDE + y}

    def along_y(by):
        return {"item": x * SIDE + step(y, by)}

    other = {"edge": 1 - e}
    p1, p2 = (x, y), (y, x)
    ring1, ring2 = (along_x, along_y), (along_y, along_x)

    def block_at(h, k1):
        return (h * SIDE + step(p1[h], k1)) * block

    def seg_at(h, k1, k2):
        return block_at(h, k1) + step(p2[h], k2) * seg

    peers = [along_x(1), along_x(-1), along_x(2), along_y(1), along_y(-1), along_y(2), other]
    greet(peers)
    own_copies = fetch(
        [(emb.at[rows_at(e * part.shape[0] + seg_at(h, 0, 0), seg, seg)], own_rows.at[h]) for h in range(2)]
        + [(weight_hbm, weight)],
        local_sem,
    )

    def mine(h, k1, k2, start, size):
        return part[rows_at(seg_at(h, k1, k2) + start, size, half2), :]

    low, high = pl.ds(0, half2), pl.ds(half2, half2)
    order = (2, 1, -1, 0)
    for h in range(2):
        sums[h, 2, 2] = mine(h, 2, 2, 0, seg).astype(BF16)
    meet(peers)
    w = Wires(send_sem, recv_sem)

    far, near, passed = {}, {}, {}

    def direct(k2):
        at = k2 % SIDE
        for h in range(2):
            sums[h, 1, at, high] = mine(h, 1, k2, half2, half2).astype(BF16)
            near[h, k2, 1] = w.start(sums.at[h, 1, at, high], final.at[h, 0, at, high], ring1[h](1))
            sums[h, 3, at, low] = mine(h, -1, k2, 0, half2).astype(BF16)
            near[h, k2, -1] = w.start(sums.at[h, 3, at, low], final.at[h, 1, at, low], ring1[h](-1))

    def combine(k2):
        at = k2 % SIDE
        for h in range(2):
            far[h, k2, 1].wait_recv()
            sums[h, 1, at, low] = (mine(h, 1, k2, 0, half2) + up(opposite[h, 0, at])).astype(BF16)
            passed[h, k2, 1] = w.start(sums.at[h, 1, at, low], final.at[h, 0, at, low], ring1[h](1))
            far[h, k2, -1].wait_recv()
            sums[h, 3, at, high] = (mine(h, -1, k2, half2, half2) + up(opposite[h, 1, at])).astype(BF16)
            passed[h, k2, -1] = w.start(sums.at[h, 3, at, high], final.at[h, 1, at, high], ring1[h](-1))

    def finished(h, k2):
        for s in (1, -1):
            near[h, k2, s].wait_recv()
            passed[h, k2, s].wait_recv()
        at = k2 % SIDE
        return mine(h, 0, k2, 0, seg) + up(final[h, 0, at]) + up(final[h, 1, at])

    for k2 in order:
        at = k2 % SIDE
        for h in range(2):
            if k2 != 2:
                sums[h, 2, at] = mine(h, 2, k2, 0, seg).astype(BF16)
            far[h, k2, 1] = w.start(sums.at[h, 2, at, low], opposite.at[h, 0, at], ring1[h](1))
            far[h, k2, -1] = w.start(sums.at[h, 2, at, high], opposite.at[h, 1, at], ring1[h](-1))
    direct(2)

    cnt[...] = jnp.zeros_like(cnt)
    slots = found.shape[0]
    lane = lax.broadcasted_iota(jnp.int32, (slots, TILE), 1)
    hits = found[...] + row_hits(links[pl.ds(0, slots), :], lane, TILE // 4, TILE)
    degrees_of(cnt, hits.astype(BF16), meta[1:2, 0:slots])
    shared = 2 * SIDE
    core_cnt = w.start(cnt.at[pl.ds((1 - e) * shared, shared)], got_core, other)

    combine(2)
    direct(1)
    direct(-1)
    combine(1)
    combine(-1)
    core_cnt.wait_recv()
    chip_cnt[...] = cnt[pl.ds(e * shared, shared)] + got_core[...]
    cnt1 = [
        w.start(chip_cnt.at[h * SIDE + step(p1[h], by)], got_cnt.at[h, k], ring1[h](by))
        for h in range(2)
        for k, by in enumerate((1, -1, 2))
    ]
    direct(0)

    near2 = {0: [], 1: []}
    for h in range(2):
        small[h, 0] = finished(h, 2).astype(BF16)
        near2[h].append(w.start(small.at[h, 0], final2.at[h, 0], ring2[h](2)))
    combine(0)
    for copy in cnt1:
        copy.wait_recv()
    for h in range(2):
        ring_cnt[h] = chip_cnt[h * SIDE + step(p1[h], 0)] + got_cnt[h, 0] + got_cnt[h, 1] + got_cnt[h, 2]
    cnt2 = [
        w.start(ring_cnt.at[h], got_cnt2.at[h, k], ring2[h](by)) for h in range(2) for k, by in enumerate((1, -1, 2))
    ]
    for h in range(2):
        small[h, 1] = finished(h, 1).astype(BF16)
        near2[h].append(w.start(small.at[h, 1], final2.at[h, 1], ring2[h](1)))
        small[h, 2] = finished(h, -1).astype(BF16)
        near2[h].append(w.start(small.at[h, 2], final2.at[h, 2], ring2[h](-1)))
    for h in range(2):
        total[h] = finished(h, 0)

    for copy in own_copies:
        copy.wait()
    for copy in cnt2:
        copy.wait_recv()
    own_diag = lax.broadcasted_iota(jnp.int32, (seg, TILE), 0) == lax.broadcasted_iota(jnp.int32, (seg, TILE), 1)
    degrees = []
    for h in range(2):
        counts = ring_cnt[h] + got_cnt2[h, 0] + got_cnt2[h, 1] + got_cnt2[h, 2]
        own_row = lax.broadcasted_iota(jnp.int32, counts.shape, 0) == p2[h]
        degree = jnp.sum(jnp.where(own_row, counts, 0.0), axis=0, keepdims=True)
        degree = jnp.sum(jnp.where(own_diag, jnp.broadcast_to(degree, (seg, TILE)), 0.0), axis=1, keepdims=True)
        degrees.append(jnp.maximum(degree, 1.0))
    def send(h, k1, k2, start, size, device):
        there = users.at[rows_at(seg_at(h, k1, k2) + start, size, half2)]
        return w.start(there, there, device)

    c1, c2, c2f = {}, {}, {}

    def spread(h, k2):
        for s in (1, -1):
            c2[h, k2, s] = send(h, 0, k2, 0, seg, ring1[h](s))
        if k2 == 2:
            c2f[h, k2, 0] = send(h, 0, k2, 0, seg, ring1[h](2))

    def relay(h, k2):
        c2[h, k2, 1].wait_recv()
        c2f[h, k2, 1] = send(h, -1, k2, 0, half2, ring1[h](1))
        c2[h, k2, -1].wait_recv()
        c2f[h, k2, -1] = send(h, 1, k2, half2, half2, ring1[h](-1))

    for h in range(2):
        for copy in near2[h]:
            copy.wait_recv()
        summed = total[h] + up(final2[h, 0]) + up(final2[h, 1]) + up(final2[h, 2])
        average = (summed / degrees[h]).astype(BF16)
        v = jnp.dot(average, weight[...], preferred_element_type=F32)
        fresh = up(own_rows[h]) + v / (1.0 + jnp.exp(-v))
        users[rows_at(seg_at(h, 0, 0), seg, seg), :] = fresh.astype(BF16)
        for s in (1, -1, 2):
            c1[h, s] = send(h, 0, 0, 0, seg, ring2[h](s))
        spread(h, 0)
    for h in range(2):
        for s in (1, -1):
            c1[h, s].wait_recv()
            spread(h, -s)
    for h in range(2):
        c1[h, 2].wait_recv()
        spread(h, 2)
    for k2 in (0, -1, 1):
        for h in range(2):
            relay(h, k2)
    for h in range(2):
        for s in (1, -1):
            c2[h, 2, s].wait_recv()
    for copy in c2f.values():
        copy.wait_recv()
    w.finish()
    assert len(w.made) == PLANE_COPIES, len(w.made)


DEPTH = 8
PARTS = 4
COLUMN_COPIES = 8 + 7 * PARTS + 8


def column_kernel(
    part, hits, items, up_weight, down_weight, out, to_core, from_core, sums, got_up, got_down, chip_hits, got_hits, own_rows, arrived,
    up_v, down_v, local_sem, send_sem, recv_sem,
):
    u, e = lax.axis_index("user"), lax.axis_index("edge")
    share = out.shape[0]
    half = share // PARTS

    def step(by):
        return lax.rem(u + (by + DEPTH), DEPTH)

    other = {"edge": 1 - e}
    place = {1: {"user": step(1)}, -1: {"user": step(-1)}}

    peers = [place[1], place[-1], other]
    greet(peers)

    def chunk(k, core):
        return (step(k) * 2 + core) * share

    local = [
        pltpu.make_async_copy(items.at[rows_at(chunk(0, e), share, share)], own_rows, local_sem.at[0]),
        pltpu.make_async_copy(up_weight, up_v, local_sem.at[1]),
        pltpu.make_async_copy(down_weight, down_v, local_sem.at[2]),
    ]
    for copy in local:
        copy.start()
    def round_off(k):
        to_core[k % DEPTH] = part[rows_at(chunk(k, 1 - e), share, share), :].astype(BF16)

    round_off(4)
    meet(peers)
    w = Wires(send_sem, recv_sem)
    core = {}
    for k in (4, 3, -3, 2, -2, 1, -1, 0):
        if k != 4:
            round_off(k)
        core[k] = w.start(to_core.at[k % DEPTH], from_core.at[k % DEPTH], other)
    core_hits = w.start(hits, got_hits.at[0], other)

    def mine(k, q):
        return part[rows_at(chunk(k, e) + q * half, half, half), :] + up(from_core[k % DEPTH, pl.ds(q * half, half), :])

    got = {1: got_up, -1: got_down}
    wires = {}
    hit_wires = {}

    landed = set()

    def land(k):
        if k not in landed:
            landed.add(k)
            core[k].wait_recv()

    def pass_on(s, k, q):
        land(4 if k == 4 else s * k)
        value = mine(s * k, q)
        if (s, k + 1, q) in wires:
            wires[s, k + 1, q].wait_recv()
            value += up(got[s][k, q])
        running = (s * k) % DEPTH, pl.ds(q * half, half)
        sums[running] = value.astype(BF16)
        wires[s, k, q] = w.start(sums.at[running], got[s].at[k - 1, q], place[s])

    first = [(s, j if s == 1 else PARTS // 2 + j) for j in range(PARTS // 2) for s in (1, -1)]
    second = [(s, PARTS // 2 + j if s == 1 else j) for j in range(PARTS // 2) for s in (1, -1)]
    for s, q in first:
        pass_on(s, 4, q)
    for s, q in second:
        pass_on(s, 3, q)
    core_hits.wait_recv()
    chip_hits[...] = hits[...] + got_hits[0]
    for s in (1, -1):
        hit_wires[s, 1] = w.start(chip_hits, got_hits.at[1 if s == 1 else 5], place[s])
    for k in (3, 2, 1):
        for s, q in first:
            pass_on(s, k, q)
        far = 5 - k
        for s in (1, -1):
            hit_wires[s, far - 1].wait_recv()
            if s == 1 or far < 4:
                base = 1 if s == 1 else 5
                hit_wires[s, far] = w.start(got_hits.at[base + far - 2], got_hits.at[base + far - 1], place[s])
        if k > 1:
            for s, q in second:
                pass_on(s, k - 1, q)
    hit_wires[1, 4].wait_recv()
    land(0)
    degree = chip_hits[...]
    for k in range(1, DEPTH):
        degree += got_hits[k]
    lane = lax.broadcasted_iota(jnp.int32, degree.shape, 1)
    for copy in local:
        copy.wait()
    own = [jnp.sum(jnp.where(lane == (u * 2 + e) * 2 + k, degree, 0.0)[0:1, :], axis=1, keepdims=True) for k in range(2)]
    own = [jnp.maximum(count, 1.0) for count in own]
    for q in range(PARTS):
        arrived[pl.ds(q * half, half), :] = mine(0, q)
    for pair in ((0, PARTS // 2), (1, PARTS // 2 + 1)):
        merged = []
        for q in pair:
            wires[1, 1, q].wait_recv()
            wires[-1, 1, q].wait_recv()
            rows = pl.ds(q * half, half)
            summed = arrived[rows, :] + up(got_up[0, q]) + up(got_down[0, q])
            merged.append(up(own_rows[rows, :]) + summed / own[q * half // TILE])
        merged = jnp.concatenate(merged, axis=0)
        v = jnp.dot(merged.astype(BF16), up_v[...], preferred_element_type=F32)
        hidden = (v / (1.0 + jnp.exp(-v))).astype(BF16)
        fresh = (merged + jnp.dot(hidden, down_v[...], preferred_element_type=F32)).astype(BF16)
        for at, q in enumerate(pair):
            out[pl.ds(q * half, half), :] = fresh[at * half : (at + 1) * half]
    w.finish()
    assert len(w.made) <= COLUMN_COPIES, len(w.made)


def vmem():
    return pl.BlockSpec(memory_space=VM)


def smem():
    return pl.BlockSpec(memory_space=pltpu.SMEM)


def hbm():
    return pl.BlockSpec(memory_space=pltpu.HBM)


MIB = 2**20


def swap(bi, bu, count, links, items, half_tiles):
    slots = links.shape[0]
    assert items.shape[0] == ITEM_TILES * TILE and 2 * slots <= SLOTS
    return pl.pallas_call(
        functools.partial(swap_kernel, half_tiles),
        out_shape=(
            jax.ShapeDtypeStruct((16, TILE), jnp.int32),
            jax.ShapeDtypeStruct((2 * slots, TILE), jnp.int32),
            jax.ShapeDtypeStruct((slots, TILE), F32),
            jax.ShapeDtypeStruct((8, TILE), F32),
            jax.ShapeDtypeStruct(items.shape, BF16),
        ),
        in_specs=[hbm()] * 5,
        out_specs=(vmem(),) * 5,
        scratch_shapes=[
            VM((1, slots), jnp.int32),
            VM((1, slots), jnp.int32),
            pltpu.SMEM((1,), jnp.int32),
            VM((8, TILE), jnp.int32),
            pltpu.SemaphoreType.DMA((5,)),
            pltpu.SemaphoreType.DMA((2,)),
            pltpu.SemaphoreType.DMA((2,)),
        ],
        compiler_params=pltpu.CompilerParams(collective_id=2, has_side_effects=True, vmem_limit_bytes=16 * MIB),
        name="swap",
    )(bi, bu, count, links, items)


def hop(from_items, meta, links, source, rows):
    slots = links.shape[0]
    return pl.pallas_call(
        functools.partial(hop_kernel, from_items),
        out_shape=jax.ShapeDtypeStruct((rows, source.shape[1]), F32),
        in_specs=[vmem()] * 3,
        out_specs=vmem(),
        scratch_shapes=[
            pltpu.SMEM(meta.shape, jnp.int32),
            pltpu.SMEM((slots + GROUP,), jnp.int32),
            pltpu.SemaphoreType.DMA((1,)),
        ],
        compiler_params=pltpu.CompilerParams(vmem_limit_bytes=24 * MIB),
        name="hop1" if from_items else "hop2",
    )(meta, links, source)


def plane(part, meta, links, found, emb, weight):
    rows, channels = part.shape
    seg = rows // (2 * SIDE * SIDE)
    pieces = 4 * SIDE
    return pl.pallas_call(
        plane_kernel,
        out_shape=jax.ShapeDtypeStruct((rows, channels), BF16),
        in_specs=[vmem()] * 4 + [hbm()] * 2,
        out_specs=vmem(),
        scratch_shapes=[
            VM((2, SIDE, SIDE, seg, channels), BF16),
            VM((2, 2, SIDE, seg // 2, channels), BF16),
            VM((2, 2, SIDE, seg, channels), BF16),
            VM((2, seg, channels), F32),
            VM((2, 3, seg, channels), BF16),
            VM((2, 3, seg, channels), BF16),
            VM((pieces, 8, TILE), F32),
            VM((pieces // 2, 8, TILE), F32),
            VM((pieces // 2, 8, TILE), F32),
            VM((2, 3, 8, TILE), F32),
            VM((2, 8, TILE), F32),
            VM((2, 3, 8, TILE), F32),
            VM((2, seg, channels), BF16),
            VM(weight.shape, BF16),
            pltpu.SemaphoreType.DMA((3,)),
            pltpu.SemaphoreType.DMA((PLANE_COPIES,)),
            pltpu.SemaphoreType.DMA((PLANE_COPIES,)),
        ],
        compiler_params=pltpu.CompilerParams(collective_id=0, has_side_effects=True, vmem_limit_bytes=32 * MIB),
        name="plane",
    )(part, meta, links, found, emb, weight)


def column(part, hits, items, up_weight, down_weight):
    rows, channels = part.shape
    share = rows // (2 * DEPTH)
    return pl.pallas_call(
        column_kernel,
        out_shape=jax.ShapeDtypeStruct((share, channels), BF16),
        in_specs=[vmem(), vmem(), hbm(), hbm(), hbm()],
        out_specs=vmem(),
        scratch_shapes=[
            VM((DEPTH, share, channels), BF16),
            VM((DEPTH, share, channels), BF16),
            VM((DEPTH, share, channels), BF16),
            VM((4, PARTS, share // PARTS, channels), BF16),
            VM((4, PARTS, share // PARTS, channels), BF16),
            VM(hits.shape, F32),
            VM((DEPTH,) + hits.shape, F32),
            VM((share, channels), BF16),
            VM((share, channels), F32),
            VM(up_weight.shape, BF16),
            VM(down_weight.shape, BF16),
            pltpu.SemaphoreType.DMA((3,)),
            pltpu.SemaphoreType.DMA((COLUMN_COPIES,)),
            pltpu.SemaphoreType.DMA((COLUMN_COPIES,)),
        ],
        compiler_params=pltpu.CompilerParams(collective_id=1, has_side_effects=True, vmem_limit_bytes=40 * MIB),
        name="column",
    )(part, hits, items, up_weight, down_weight)


def pin(*xs):
    return [pltpu.with_memory_space_constraint(x, pltpu.HBM) for x in xs]


def body(item_emb, user_emb, block_item, block_user, block_rows, block_count, user_weight, up_weight, down_weight):
    bi, bu, count = block_item.reshape(1, -1), block_user.reshape(1, -1), block_count.reshape(-1)
    links = block_rows.reshape(-1, TILE)
    bi, bu, links, item_emb, user_emb, user_weight, up_weight, down_weight = pin(
        bi, bu, links, item_emb, user_emb, user_weight, up_weight, down_weight
    )
    half_rows = user_emb.shape[0] // 2
    meta, links, found, hits, items = swap(bi, bu, count, links, item_emb, half_rows // TILE)
    user_part = hop(True, meta, links, items, half_rows)
    users = plane(user_part, meta, links, found, user_emb, user_weight)
    item_part = hop(False, meta, links, users, item_emb.shape[0])
    return column(item_part, hits, item_emb, up_weight, down_weight)


def solution(mesh):
    return jax.shard_map(
        body,
        mesh=mesh,
        in_specs=(
            P("item", None),
            P("user", None),
            P("item", "user", "edge", None),
            P("item", "user", "edge", None),
            P("item", "user", "edge", None, None),
            P("item", "user", "edge"),
            P(),
            P(),
            P(),
        ),
        out_specs=P(("item", "user", "edge"), None),
        check_vma=False,
    )
```
